32 devices in a mesh: dp: 32 (over z, y, x, core).
Axes of the slice: x: 2, y: 2, z: 4, core: 2. Of those that a mesh axis runs over, the one named last changes fastest.
Arguments:
- g_mat: bfloat16 [32, 2457600], P('dp')
- g_vec: bfloat16 [32, 8320], P('dp')
- p_mat: float32 [2457600], P('dp')
- m_mat: float32 [2457600], P('dp')
- v_mat: float32 [2457600], P('dp')
- p_vec: float32 [8320], replicated
- m_vec: float32 [8320], replicated
- v_vec: float32 [8320], replicated
- learn_rate: float32 [], replicated
Outputs:
- output 1: float32 [2457600], P('dp')
- output 2: float32 [2457600], P('dp')
- output 3: float32 [2457600], P('dp')
- output 4: float32 [8320], replicated
- output 5: float32 [8320], replicated
- output 6: float32 [8320], replicated
- output 7: bfloat16 [2457600], replicated
All inputs are finite; a program needn't handle non-finite values.
Results may differ from the reference program's by a relative error of at most 0.001.
Values are sent between devices in bfloat16 or wider.
A program may use at most 1 GiB of HBM per device.

```python
import jax
import jax.numpy as jnp
from jax import lax

D = 320
FF = 1280
TP = 1
DP = 32
STEP = 10

N_MAT = (8 * D * D + 4 * D * FF) // TP
N_VEC = 2 * ((3 * D + FF) // TP) + 12 * D
N_ALL = N_MAT + N_VEC
ELEM_SCALE = N_ALL ** -0.5
NOISE_GAIN = 6.0 * DP ** 0.5
ADAM_BETA1 = 0.9
ADAM_BETA2 = 0.98
ADAM_EPS = 1e-8
WEIGHT_DECAY = 0.01
MAX_NORM = 1.0
NORM_EPS = 1e-6
BIAS_ONE = 1.0 - ADAM_BETA1 ** STEP
BIAS_TWO = 1.0 - ADAM_BETA2 ** STEP


def draw_local_grads(draw_key, elem_count):
    key_base, key_dev = jax.random.split(draw_key)
    base_part = 2.0 * jax.random.normal(key_base, (elem_count,), jnp.float32)
    dev_keys = jax.random.split(key_dev, DP)

    def one_device(dev_key):
        noise_part = jax.random.normal(dev_key, (elem_count,), jnp.float32)
        return ((base_part + NOISE_GAIN * noise_part) * ELEM_SCALE).astype(jnp.bfloat16)

    return lax.map(one_device, dev_keys)


def setup_inputs(seed: int = 0) -> dict:
    key_list = jax.random.split(jax.random.key(seed), 9)
    return dict(
        g_mat=draw_local_grads(key_list[0], N_MAT),
        g_vec=draw_local_grads(key_list[1], N_VEC),
        p_mat=0.02 * jax.random.normal(key_list[2], (N_MAT,), jnp.float32),
        m_mat=0.1 * ELEM_SCALE * jax.random.normal(key_list[3], (N_MAT,), jnp.float32),
        v_mat=0.05 * ELEM_SCALE * ELEM_SCALE * jax.random.uniform(key_list[4], (N_MAT,), jnp.float32, minval=0.25, maxval=1.75),
        p_vec=0.05 * jax.random.normal(key_list[5], (N_VEC,), jnp.float32),
        m_vec=0.1 * ELEM_SCALE * jax.random.normal(key_list[6], (N_VEC,), jnp.float32),
        v_vec=0.05 * ELEM_SCALE * ELEM_SCALE * jax.random.uniform(key_list[7], (N_VEC,), jnp.float32, minval=0.25, maxval=1.75),
        learn_rate=jax.random.uniform(key_list[8], (), jnp.float32, minval=0.002, maxval=0.008),
    )


def mean_over_devices(local_grads):
    def add_row(acc_sum, grad_row):
        return acc_sum + grad_row.astype(jnp.float32), None

    total_sum, _ = lax.scan(add_row, jnp.zeros(local_grads.shape[1:], jnp.float32), local_grads)
    return total_sum / local_grads.shape[0]


def adam_update(grad_vals, param_vals, moment_one, moment_two, learn_rate, decay_rate):
    new_one = ADAM_BETA1 * moment_one + (1.0 - ADAM_BETA1) * grad_vals
    new_two = ADAM_BETA2 * moment_two + (1.0 - ADAM_BETA2) * grad_vals * grad_vals
    direction = (new_one / BIAS_ONE) / (jnp.sqrt(new_two / BIAS_TWO) + ADAM_EPS)
    return param_vals - learn_rate * (direction + decay_rate * param_vals), new_one, new_two


def reference(g_mat, g_vec, p_mat, m_mat, v_mat, p_vec, m_vec, v_vec, learn_rate):
    grad_mat = mean_over_devices(g_mat)
    grad_vec = mean_over_devices(g_vec)
    norm_sq = jnp.sum(grad_mat * grad_mat) + jnp.sum(grad_vec * grad_vec)
    clip_scale = jnp.minimum(1.0, MAX_NORM / (jnp.sqrt(norm_sq) + NORM_EPS))
    new_p_mat, new_m_mat, new_v_mat = adam_update(grad_mat * clip_scale, p_mat, m_mat, v_mat, learn_rate, WEIGHT_DECAY)
    new_p_vec, new_m_vec, new_v_vec = adam_update(grad_vec * clip_scale, p_vec, m_vec, v_vec, learn_rate, 0.0)
    return (new_p_mat, new_m_mat, new_v_mat, new_p_vec, new_m_vec, new_v_vec, new_p_mat.astype(jnp.bfloat16))
```

```python
import jax
import jax.numpy as jnp
from jax import lax
from jax.experimental import pallas as pl
from jax.experimental.pallas import tpu as pltpu
from jax.sharding import PartitionSpec as P

STEP = 10
ADAM_BETA1 = 0.9
ADAM_BETA2 = 0.98
ADAM_EPS = 1e-8
WEIGHT_DECAY = 0.01
MAX_NORM = 1.0
NORM_EPS = 1e-6
BIAS_ONE = 1.0 - ADAM_BETA1 ** STEP
BIAS_TWO = 1.0 - ADAM_BETA2 ** STEP

MESH = pl.DeviceIdType.MESH
F32 = jnp.float32
BF16 = jnp.bfloat16
LANES = 128
CHUNK = 120


def adam_update(grad_vals, param_vals, moment_one, moment_two, learn_rate, decay_rate):
    new_one = ADAM_BETA1 * moment_one + (1.0 - ADAM_BETA1) * grad_vals
    new_two = ADAM_BETA2 * moment_two + (1.0 - ADAM_BETA2) * grad_vals * grad_vals
    direction = (new_one / BIAS_ONE) / (jnp.sqrt(new_two / BIAS_TWO) + ADAM_EPS)
    return param_vals - learn_rate * (direction + decay_rate * param_vals), new_one, new_two


def step_kernel(group, rows, vrows, axis_name):
    inv_group = 1.0 / group

    def body(g_ref, gv_ref, p_ref, m_ref, v_ref, pv_ref, mv_ref, vv_ref, lr_ref,
             pb_out, p_out, m_out, v_out, pv_out, mv_out, vv_out,
             own, pair, send_a, recv_a, send_b, recv_b, send_z, recv_z, grad, norm_rows,
             p_in, m_in, v_in, gv_own, gv_pair, gv_x, gv_xr, gv_y, gv_yr, gv_z, gv_zr, gv_sum,
             pv_in, mv_in, vv_in,
             own_sem, pair_s, pair_r, a_s, a_r, b_s, b_r, z_s, z_r, load_sem,
             vc_s, vc_r, vx_s, vx_r, vy_s, vy_r, vz_s, vz_r, n_s, n_r,
             gz_s, gz_r, gb_s, gb_r, ga_s, ga_r, gc_s, gc_r):
        me = lax.axis_index(axis_name)
        core = me % 2
        x = (me // 2) % 2
        y = (me // 4) % 2
        z = me // 8
        str_a = 2 + 2 * core
        str_b = 4 - 2 * core
        a = x + core * (y - x)
        b = y + core * (x - y)
        dev_c = me + 1 - 2 * core
        dev_a = me + (1 - 2 * a) * str_a
        dev_b = me + (1 - 2 * b) * str_b
        dev_x = me + (1 - 2 * x) * 2
        dev_y = me + (1 - 2 * y) * 4
        high = z // 2
        order = [3 - 3 * high, 2 - high, 1 - z + 4 * high, z]

        def dev_z(zq):
            return me + (zq - z) * 8

        def piece(zq, flip_a, flip_b):
            aq = 1 - a if flip_a else a
            bq = 1 - b if flip_b else b
            return zq * 8 + aq * str_a + bq * str_b + core

        def partner_piece(zq, flip_a, flip_b):
            aq = 1 - b if flip_a else b
            bq = 1 - a if flip_b else a
            return zq * 8 + aq * str_b + bq * str_a + 1 - core

        def remote(src, dst, s_sem, r_sem, dev):
            return pltpu.make_async_remote_copy(
                src_ref=src, dst_ref=dst, send_sem=s_sem, recv_sem=r_sem, device_id=(dev,), device_id_type=MESH)

        flips = [(True, True), (True, False), (False, True), (False, False)]
        own_copies = []
        for j in range(4):
            for k, (fa, fb) in enumerate(flips):
                src = g_ref.at[pl.ds(piece(order[j], fa, fb) * rows, rows)]
                own_copies.append(pltpu.make_async_copy(src, own.at[j * 4 + k], own_sem.at[j * 4 + k]))
        for copy in own_copies[:4]:
            copy.start()
        loads = [pltpu.make_async_copy(s, d, load_sem.at[i]) for i, (s, d) in enumerate([
            (gv_ref, gv_own), (p_ref, p_in), (m_ref, m_in), (v_ref, v_in),
            (pv_ref, pv_in), (mv_ref, mv_in), (vv_ref, vv_in)])]

        barrier = pltpu.get_barrier_semaphore()
        for i in range(group):
            @pl.when(i != me)
            def _():
                pl.semaphore_signal(barrier, inc=1, device_id=(i,), device_id_type=MESH)
        pl.semaphore_wait(barrier, group - 1)

        pair_copies = []
        for j in range(4):
            for k, (fa, fb) in enumerate(flips):
                src = g_ref.at[pl.ds(partner_piece(order[j], fa, fb) * rows, rows)]
                pair_copies.append(remote(src, pair.at[j * 4 + k], pair_s.at[j * 4 + k], pair_r.at[j * 4 + k], dev_c))
        for i in range(16):
            pair_copies[i].start()
            if i >= 4:
                own_copies[i].start()
        vec_pair = remote(gv_ref, gv_pair, vc_s.at[0], vc_r.at[0], dev_c)
        vec_pair.start()
        for load in loads:
            load.start()

        def chunks(fn):
            @pl.loop(0, rows // CHUNK)
            def _(i):
                fn(pl.ds(pl.multiple_of(i * CHUNK, 8), CHUNK))

        def pair_sum(i, s):
            return own[i, s, 0, :].astype(F32) + pair[i, s, 0, :].astype(F32)

        a_copies = [remote(send_a.at[i], recv_a.at[i], a_s.at[i], a_r.at[i], dev_a) for i in range(8)]
        for i in range(8):
            slot = (i // 2) * 4 + i % 2
            own_copies[slot].wait()
            pair_copies[slot].wait_recv()

            def add_pair(s, i=i, slot=slot):
                send_a[i, s, :] = pair_sum(slot, s)

            chunks(add_pair)
            a_copies[i].start()

        loads[0].wait()
        vec_pair.wait_recv()
        gv_x[...] = gv_own[:, 0, :].astype(F32) + gv_pair[:, 0, :].astype(F32)
        vec_x = remote(gv_x, gv_xr, vx_s.at[0], vx_r.at[0], dev_x)
        vec_x.start()

        b_copies = [remote(send_b.at[j], recv_b.at[j], b_s.at[j], b_r.at[j], dev_b) for j in range(4)]
        z_copies = [remote(send_z.at[j], recv_z.at[z], z_s.at[j], z_r.at[z], dev_z(order[j])) for j in range(3)]

        def do_b(j):
            slot = j * 4 + 2
            own_copies[slot].wait()
            pair_copies[slot].wait_recv()
            a_copies[j * 2].wait_recv()

            def add_a(s):
                send_b[j, s, :] = pair_sum(slot, s) + recv_a[j * 2, s, :]

            chunks(add_a)
            b_copies[j].start()

        def do_z(j):
            slot = j * 4 + 3
            own_copies[slot].wait()
            pair_copies[slot].wait_recv()
            a_copies[j * 2 + 1].wait_recv()
            b_copies[j].wait_recv()

            def add_ab(s):
                send_z[j, s, :] = pair_sum(slot, s) + recv_a[j * 2 + 1, s, :] + recv_b[j, s, :]

            chunks(add_ab)
            if j < 3:
                z_copies[j].start()

        do_b(0)
        vec_x.wait_recv()
        gv_y[...] = gv_x[...] + gv_xr[...]
        vec_y = remote(gv_y, gv_yr, vy_s.at[0], vy_r.at[0], dev_y)
        vec_y.start()
        do_b(1)
        do_z(0)
        do_b(2)
        vec_y.wait_recv()
        gv_z[...] = gv_y[...] + gv_yr[...]
        vec_z = [remote(gv_z, gv_zr.at[z], vz_s.at[j], vz_r.at[z], dev_z(order[j])) for j in range(3)]
        for copy in vec_z:
            copy.start()
        gv_zr[z] = gv_z[...]
        do_z(1)
        do_b(3)
        do_z(2)
        do_z(3)

        for j in range(3):
            remote(gv_z, gv_zr.at[order[j]], vz_s.at[j], vz_r.at[order[j]], dev_z(order[j])).wait_recv()
        gv_sum[...] = (((gv_zr[0] + gv_zr[1]) + gv_zr[2]) + gv_zr[3]) * inv_group
        vec_sq = jnp.sum(gv_sum[...] * gv_sum[...])

        for j in range(3):
            remote(send_z.at[j], recv_z.at[order[j]], z_s.at[j], z_r.at[order[j]], dev_z(order[j])).wait_recv()

        def final_sum(i, acc):
            s = pl.ds(pl.multiple_of(i * CHUNK, 8), CHUNK)
            g = send_z[3, s, :]
            for j in range(3):
                g = g + recv_z[order[j], s, :]
            g = g * inv_group
            grad[s, :] = g
            return acc + jnp.sum((g * g).reshape(CHUNK // 8, 8, LANES), axis=0)

        sq = lax.fori_loop(0, rows // CHUNK, final_sum, jnp.zeros((8, LANES), F32))
        norm_rows[me] = jnp.sum(sq, axis=0, keepdims=True)

        for d in range(1, group):
            to = (me + d) % group
            remote(norm_rows.at[me], norm_rows.at[me], n_s.at[d], n_r.at[d], to).start()
        for load in loads[1:]:
            load.wait()
        for d in range(1, group):
            frm = (me - d + group) % group
            remote(norm_rows.at[frm], norm_rows.at[frm], n_s.at[d], n_r.at[d], frm).wait_recv()
        norm_sq = jnp.sum(norm_rows[...]) + vec_sq
        norm = jnp.sqrt(jnp.full((8, LANES), norm_sq, F32))
        scale = jnp.minimum(1.0, MAX_NORM / (norm + NORM_EPS))[0:1, :]
        lr = lr_ref[0]

        def adam(s):
            new_p, new_m, new_v = adam_update(grad[s, :] * scale, p_in[s, :], m_in[s, :], v_in[s, :], lr, WEIGHT_DECAY)
            p_out[s, :] = new_p
            m_out[s, :] = new_m
            v_out[s, :] = new_v
            p_in[s, :] = new_p

        chunks(adam)
        pb_out[me] = p_in[...].astype(BF16)

        def move(idx, s_sem, r_sem, dev):
            return remote(pb_out.at[idx], pb_out.at[idx], s_sem, r_sem, dev)

        near = [z, order[2], order[1], order[0]]
        z_sends = [move(me, gz_s.at[q], gz_r.at[z], dev_z(near[q])) for q in range(1, 4)]
        b_idx = [piece(near[q], False, False) for q in range(4)]
        a_idx = [piece(near[i // 2], False, i % 2 == 1) for i in range(8)]
        c_idx = a_idx + [piece(near[i // 2], True, i % 2 == 1) for i in range(8)]
        b_sends = [move(b_idx[q], gb_s.at[q], gb_r.at[q], dev_b) for q in range(4)]
        a_sends = [move(a_idx[i], ga_s.at[i], ga_r.at[i], dev_a) for i in range(8)]
        c_sends = [move(c_idx[i], gc_s.at[i], gc_r.at[i], dev_c) for i in range(16)]

        def wait_z(q):
            idx = piece(near[q], False, False)
            move(idx, gz_s.at[q], gz_r.at[near[q]], dev_z(near[q])).wait_recv()

        def wait_b(q):
            move(piece(near[q], False, True), gb_s.at[q], gb_r.at[q], dev_b).wait_recv()

        def wait_a(i):
            move(c_idx[8 + i], ga_s.at[i], ga_r.at[i], dev_a).wait_recv()

        def wait_c(i):
            idx = partner_piece(near[(i % 8) // 2], i >= 8, i % 2 == 1)
            move(idx, gc_s.at[i], gc_r.at[i], dev_c).wait_recv()

        for q in range(3):
            z_sends[q].start()
        b_sends[0].start()
        a_sends[0].start()
        c_sends[0].start()

        pv_new, mv_new, vv_new = adam_update(gv_sum[...] * scale, pv_in[...], mv_in[...], vv_in[...], lr, 0.0)
        pv_out[...] = pv_new
        mv_out[...] = mv_new
        vv_out[...] = vv_new

        for q in range(4):
            if q > 0:
                wait_z(q)
                b_sends[q].start()
                a_sends[2 * q].start()
                c_sends[2 * q].start()
                for i in (2 * q - 2, 2 * q - 1):
                    wait_a(i)
                    c_sends[8 + i].start()
            wait_b(q)
            a_sends[2 * q + 1].start()
            c_sends[2 * q + 1].start()
        for i in (6, 7):
            wait_a(i)
            c_sends[8 + i].start()
        for i in range(16):
            wait_c(i)

        for copy in pair_copies + [vec_pair] + a_copies + [vec_x, vec_y] + b_copies + z_copies + vec_z:
            copy.wait_send()
        for d in range(1, group):
            remote(norm_rows.at[me], norm_rows.at[me], n_s.at[d], n_r.at[d], (me + d) % group).wait_send()
        for copy in z_sends + b_sends + a_sends + c_sends:
            copy.wait_send()

    vmem = pl.BlockSpec(memory_space=pltpu.VMEM)
    hbm = pl.BlockSpec(memory_space=pl.ANY)
    sems = pltpu.SemaphoreType.DMA
    return pl.pallas_call(
        body,
        name="adam_step",
        out_shape=(
            jax.ShapeDtypeStruct((group, rows, LANES), BF16),
            *[jax.ShapeDtypeStruct((rows, LANES), F32)] * 3,
            *[jax.ShapeDtypeStruct((vrows, LANES), F32)] * 3,
        ),
        in_specs=[hbm] * 8 + [pl.BlockSpec(memory_space=pltpu.SMEM)],
        out_specs=(vmem,) * 7,
        scratch_shapes=[
            pltpu.VMEM((16, rows, 1, LANES), BF16),
            pltpu.VMEM((16, rows, 1, LANES), BF16),
            pltpu.VMEM((8, rows, LANES), F32),
            pltpu.VMEM((8, rows, LANES), F32),
            pltpu.VMEM((4, rows, LANES), F32),
            pltpu.VMEM((4, rows, LANES), F32),
            pltpu.VMEM((4, rows, LANES), F32),
            pltpu.VMEM((4, rows, LANES), F32),
            pltpu.VMEM((rows, LANES), F32),
            pltpu.VMEM((group, 1, LANES), F32),
            *[pltpu.VMEM((rows, LANES), F32)] * 3,
            *[pltpu.VMEM((vrows, 1, LANES), BF16)] * 2,
            *[pltpu.VMEM((vrows, LANES), F32)] * 5,
            pltpu.VMEM((4, vrows, LANES), F32),
            *[pltpu.VMEM((vrows, LANES), F32)] * 4,
            sems((16,)), sems((16,)), sems((16,)),
            sems((8,)), sems((8,)), sems((4,)), sems((4,)), sems((4,)), sems((4,)), sems((7,)),
            sems((1,)), sems((1,)), sems((1,)), sems((1,)), sems((1,)), sems((1,)), sems((4,)), sems((4,)),
            sems((group,)), sems((group,)),
            sems((4,)), sems((4,)), sems((4,)), sems((4,)), sems((8,)), sems((8,)), sems((16,)), sems((16,)),
        ],
        compiler_params=pltpu.CompilerParams(
            collective_id=0, has_side_effects=True, vmem_limit_bytes=56 * 1024 * 1024),
    )


def store_kernel(shapes):
    def body(*refs):
        n = len(shapes)
        ins, outs, sem = refs[:n], refs[n:2 * n], refs[2 * n]
        copies = [pltpu.make_async_copy(ins[i], outs[i], sem.at[i]) for i in range(n)]
        for copy in copies:
            copy.start()
        for copy in copies:
            copy.wait()

    return pl.pallas_call(
        body,
        name="store_results",
        out_shape=tuple(shapes),
        in_specs=[pl.BlockSpec(memory_space=pltpu.VMEM)] * len(shapes),
        out_specs=tuple([pl.BlockSpec(memory_space=pl.ANY)] * len(shapes)),
        scratch_shapes=[pltpu.SemaphoreType.DMA((len(shapes),))],
    )


def solution(mesh):
    axis_name = mesh.axis_names[0]
    group = mesh.shape[axis_name]

    def local_step(g_mat, g_vec, p_mat, m_mat, v_mat, p_vec, m_vec, v_vec, learn_rate):
        rows = p_mat.shape[0] // LANES
        vrows = p_vec.shape[0] // LANES
        results = step_kernel(group, rows, vrows, axis_name)(
            g_mat.reshape(group * rows, 1, LANES), g_vec.reshape(vrows, 1, LANES),
            *[t.reshape(rows, LANES) for t in (p_mat, m_mat, v_mat)],
            *[t.reshape(vrows, LANES) for t in (p_vec, m_vec, v_vec)],
            learn_rate.reshape(1))
        results = store_kernel([jax.ShapeDtypeStruct(r.shape, r.dtype) for r in results])(*results)
        full, new_p, new_m, new_v, new_pv, new_mv, new_vv = results
        return (*[t.reshape(-1) for t in (new_p, new_m, new_v, new_pv, new_mv, new_vv)], full.reshape(-1))

    return jax.shard_map(
        local_step,
        mesh=mesh,
        in_specs=(P(axis_name, None), P(axis_name, None), P(axis_name), P(axis_name), P(axis_name), P(), P(), P(), P()),
        out_specs=(P(axis_name), P(axis_name), P(axis_name), P(), P(), P(), P()),
        check_vma=False,
    )
```

```python
import jax
import jax.numpy as jnp
from jax import lax
from jax.experimental import pallas as pl
from jax.experimental.pallas import tpu as pltpu
from jax.sharding import PartitionSpec as P

STEP = 10
ADAM_BETA1 = 0.9
ADAM_BETA2 = 0.98
ADAM_EPS = 1e-8
WEIGHT_DECAY = 0.01
MAX_NORM = 1.0
NORM_EPS = 1e-6
BIAS_ONE = 1.0 - ADAM_BETA1 ** STEP
BIAS_TWO = 1.0 - ADAM_BETA2 ** STEP

MESH = pl.DeviceIdType.MESH
F32 = jnp.float32
BF16 = jnp.bfloat16
LANES = 128
CHUNK = 120


def adam_update(grad_vals, param_vals, moment_one, moment_two, learn_rate, decay_rate):
    new_one = ADAM_BETA1 * moment_one + (1.0 - ADAM_BETA1) * grad_vals
    new_two = ADAM_BETA2 * moment_two + (1.0 - ADAM_BETA2) * grad_vals * grad_vals
    direction = (new_one / BIAS_ONE) / (jnp.sqrt(new_two / BIAS_TWO) + ADAM_EPS)
    return param_vals - learn_rate * (direction + decay_rate * param_vals), new_one, new_two


def step_kernel(group, rows, vrows, axis_name):
    inv_group = 1.0 / group
    vstep = vrows // 16 * 8
    vhalf = vrows - vstep

    def body(g_ref, gv_ref, p_ref, m_ref, v_ref, pv_ref, mv_ref, vv_ref, lr_ref,
             pb_out, p_out, m_out, v_out, pv_out, mv_out, vv_out,
             own, pair, send_a, recv_a, send_b, recv_b, send_z, recv_z, grad, norm_rows,
             p_in, m_in, v_in, gv_own, gv_pair, gv_plane, gv_line, gv_half, gv_other, gv_sum,
             pv_in, mv_in, vv_in,
             own_sem, pair_s, pair_r, a_s, a_r, b_s, b_r, z_s, z_r, load_sem,
             vc_s, vc_r, vp_s, vp_r, vz_s, vz_r, ve_s, ve_r, n_s, n_r,
             gz_s, gz_r, gb_s, gb_r, ga_s, ga_r, gc_s, gc_r):
        me = lax.axis_index(axis_name)
        core = me % 2
        x = (me // 2) % 2
        y = (me // 4) % 2
        z = me // 8
        str_a = 2 + 2 * core
        str_b = 4 - 2 * core
        a = x + core * (y - x)
        b = y + core * (x - y)
        dev_c = me + 1 - 2 * core
        dev_a = me + (1 - 2 * a) * str_a
        dev_b = me + (1 - 2 * b) * str_b
        dev_x = me + (1 - 2 * x) * 2
        dev_y = me + (1 - 2 * y) * 4
        spot = y * 2 + x
        high = z // 2
        order = [3 - 3 * high, 2 - high, 1 - z + 4 * high, z]

        def dev_z(zq):
            return me + (zq - z) * 8

        def piece(zq, flip_a, flip_b):
            aq = 1 - a if flip_a else a
            bq = 1 - b if flip_b else b
            return zq * 8 + aq * str_a + bq * str_b + core

        def partner_piece(zq, flip_a, flip_b):
            aq = 1 - b if flip_a else b
            bq = 1 - a if flip_b else a
            return zq * 8 + aq * str_b + bq * str_a + 1 - core

        def remote(src, dst, s_sem, r_sem, dev):
            return pltpu.make_async_remote_copy(
                src_ref=src, dst_ref=dst, send_sem=s_sem, recv_sem=r_sem, device_id=(dev,), device_id_type=MESH)

        flips = [(True, True), (True, False), (False, True), (False, False)]
        own_copies = []
        for j in range(4):
            for k, (fa, fb) in enumerate(flips):
                src = g_ref.at[pl.ds(piece(order[j], fa, fb) * rows, rows)]
                own_copies.append(pltpu.make_async_copy(src, own.at[j * 4 + k], own_sem.at[j * 4 + k]))
        use_order = [j * 4 + k for ks in ((0, 1), (2, 3)) for j in range(4) for k in ks]
        for i in use_order[:4]:
            own_copies[i].start()
        loads = [pltpu.make_async_copy(s, d, load_sem.at[i]) for i, (s, d) in enumerate([
            (gv_ref.at[pl.ds(core * vstep, vhalf)], gv_own), (p_ref, p_in), (m_ref, m_in), (v_ref, v_in),
            (pv_ref, pv_in), (mv_ref, mv_in), (vv_ref, vv_in)])]

        barrier = pltpu.get_barrier_semaphore()
        plane = [dev_x, dev_y, dev_x + dev_y - me]
        partners = [dev_c] + plane + [dev_z(order[j]) for j in range(3)]
        for partner in partners:
            pl.semaphore_signal(barrier, inc=1, device_id=(partner,), device_id_type=MESH)
        pl.semaphore_wait(barrier, len(partners))

        pair_copies = []
        for j in range(4):
            for k, (fa, fb) in enumerate(flips):
                src = g_ref.at[pl.ds(partner_piece(order[j], fa, fb) * rows, rows)]
                pair_copies.append(remote(src, pair.at[j * 4 + k], pair_s.at[j * 4 + k], pair_r.at[j * 4 + k], dev_c))
        vec_pair = remote(gv_ref.at[pl.ds((1 - core) * vstep, vhalf)], gv_pair, vc_s.at[0], vc_r.at[0], dev_c)
        loads[0].start()
        vec_pair.start()
        for n, i in enumerate(use_order):
            pair_copies[i].start()
            if n >= 4:
                own_copies[i].start()
        for load in loads[1:]:
            load.start()

        def chunks(fn):
            @pl.loop(0, rows // CHUNK)
            def _(i):
                fn(pl.ds(pl.multiple_of(i * CHUNK, 8), CHUNK))

        def pair_sum(i, s):
            return own[i, s, 0, :].astype(F32) + pair[i, s, 0, :].astype(F32)

        loads[0].wait()
        vec_pair.wait_recv()
        gv_plane[spot] = gv_own[:, 0, :].astype(F32) + gv_pair[:, 0, :].astype(F32)
        vec_plane = [remote(gv_plane.at[spot], gv_plane.at[spot], vp_s.at[i], vp_r.at[i], dev)
                     for i, dev in enumerate(plane)]
        for copy in vec_plane:
            copy.start()

        a_copies = [remote(send_a.at[i], recv_a.at[i], a_s.at[i], a_r.at[i], dev_a) for i in range(8)]
        for i in range(8):
            slot = (i // 2) * 4 + i % 2
            own_copies[slot].wait()
            pair_copies[slot].wait_recv()

            def add_pair(s, i=i, slot=slot):
                send_a[i, s, :] = pair_sum(slot, s)

            chunks(add_pair)
            a_copies[i].start()

        for i, other in enumerate((spot + 1 - 2 * x, spot + 2 - 4 * y, 3 - spot)):
            remote(gv_plane.at[other], gv_plane.at[other], vp_s.at[i], vp_r.at[i], plane[i]).wait_recv()
        gv_line[z] = ((gv_plane[0] + gv_plane[1]) + gv_plane[2]) + gv_plane[3]
        vec_line = [remote(gv_line.at[z], gv_line.at[z], vz_s.at[j], vz_r.at[z], dev_z(order[j])) for j in range(3)]
        for copy in vec_line:
            copy.start()

        b_copies = [remote(send_b.at[j], recv_b.at[j], b_s.at[j], b_r.at[j], dev_b) for j in range(4)]
        z_copies = [remote(send_z.at[j], recv_z.at[z], z_s.at[j], z_r.at[z], dev_z(order[j])) for j in range(3)]

        def do_b(j):
            slot = j * 4 + 2
            own_copies[slot].wait()
            pair_copies[slot].wait_recv()
            a_copies[j * 2].wait_recv()

            def add_a(s):
                send_b[j, s, :] = pair_sum(slot, s) + recv_a[j * 2, s, :]

            chunks(add_a)
            b_copies[j].start()

        def do_z(j):
            slot = j * 4 + 3
            own_copies[slot].wait()
            pair_copies[slot].wait_recv()
            a_copies[j * 2 + 1].wait_recv()
            b_copies[j].wait_recv()

            def add_ab(s):
                send_z[j, s, :] = pair_sum(slot, s) + recv_a[j * 2 + 1, s, :] + recv_b[j, s, :]

            chunks(add_ab)
            if j < 3:
                z_copies[j].start()

        do_b(0)
        for j in range(3):
            remote(gv_line.at[order[j]], gv_line.at[order[j]], vz_s.at[j], vz_r.at[order[j]], dev_z(order[j])).wait_recv()
        gv_half[...] = (((gv_line[0] + gv_line[1]) + gv_line[2]) + gv_line[3]) * inv_group
        vec_end = remote(gv_half, gv_other, ve_s.at[0], ve_r.at[0], dev_c)
        vec_end.start()
        do_b(1)
        vec_end.wait_recv()
        gv_sum[pl.ds(pl.multiple_of(core * vstep, 8), vhalf), :] = gv_half[...]
        gv_sum[pl.ds(pl.multiple_of((1 - core) * vstep, 8), vhalf), :] = gv_other[...]
        vec_sq = jnp.sum(gv_sum[...] * gv_sum[...])
        do_z(0)
        do_b(2)
        do_z(1)
        do_b(3)
        do_z(2)
        do_z(3)

        for j in range(3):
            remote(send_z.at[j], recv_z.at[order[j]], z_s.at[j], z_r.at[order[j]], dev_z(order[j])).wait_recv()

        def final_sum(i, acc):
            s = pl.ds(pl.multiple_of(i * CHUNK, 8), CHUNK)
            g = send_z[3, s, :]
            for j in range(3):
                g = g + recv_z[order[j], s, :]
            g = g * inv_group
            grad[s, :] = g
            return acc + jnp.sum((g * g).reshape(CHUNK // 8, 8, LANES), axis=0)

        sq = lax.fori_loop(0, rows // CHUNK, final_sum, jnp.zeros((8, LANES), F32))
        norm_rows[me] = jnp.sum(sq, axis=0, keepdims=True)

        for d in range(1, group):
            to = (me + d) % group
            remote(norm_rows.at[me], norm_rows.at[me], n_s.at[d], n_r.at[d], to).start()
        for load in loads[1:]:
            load.wait()
        for d in range(1, group):
            frm = (me - d + group) % group
            remote(norm_rows.at[frm], norm_rows.at[frm], n_s.at[d], n_r.at[d], frm).wait_recv()
        norm_sq = jnp.sum(norm_rows[...]) + vec_sq
        norm = jnp.sqrt(jnp.full((8, LANES), norm_sq, F32))
        scale = jnp.minimum(1.0, MAX_NORM / (norm + NORM_EPS))[0:1, :]
        lr = lr_ref[0]

        def adam(s):
            new_p, new_m, new_v = adam_update(grad[s, :] * scale, p_in[s, :], m_in[s, :], v_in[s, :], lr, WEIGHT_DECAY)
            p_out[s, :] = new_p
            m_out[s, :] = new_m
            v_out[s, :] = new_v
            p_in[s, :] = new_p

        chunks(adam)
        pb_out[me] = p_in[...].astype(BF16)

        def move(idx, s_sem, r_sem, dev):
            return remote(pb_out.at[idx], pb_out.at[idx], s_sem, r_sem, dev)

        near = [z, order[2], order[1], order[0]]
        z_sends = [move(me, gz_s.at[q], gz_r.at[z], dev_z(near[q])) for q in range(1, 4)]
        b_idx = [piece(near[q], False, False) for q in range(4)]
        a_idx = [piece(near[i // 2], False, i % 2 == 1) for i in range(8)]
        c_idx = a_idx + [piece(near[i // 2], True, i % 2 == 1) for i in range(8)]
        b_sends = [move(b_idx[q], gb_s.at[q], gb_r.at[q], dev_b) for q in range(4)]
        a_sends = [move(a_idx[i], ga_s.at[i], ga_r.at[i], dev_a) for i in range(8)]
        c_sends = [move(c_idx[i], gc_s.at[i], gc_r.at[i], dev_c) for i in range(16)]

        def wait_z(q):
            idx = piece(near[q], False, False)
            move(idx, gz_s.at[q], gz_r.at[near[q]], dev_z(near[q])).wait_recv()

        def wait_b(q):
            move(piece(near[q], False, True), gb_s.at[q], gb_r.at[q], dev_b).wait_recv()

        def wait_a(i):
            move(c_idx[8 + i], ga_s.at[i], ga_r.at[i], dev_a).wait_recv()

        def wait_c(i):
            idx = partner_piece(near[(i % 8) // 2], i >= 8, i % 2 == 1)
            move(idx, gc_s.at[i], gc_r.at[i], dev_c).wait_recv()

        for q in range(3):
            z_sends[q].start()
        b_sends[0].start()
        a_sends[0].start()
        c_sends[0].start()

        pv_new, mv_new, vv_new = adam_update(gv_sum[...] * scale, pv_in[...], mv_in[...], vv_in[...], lr, 0.0)
        pv_out[...] = pv_new
        mv_out[...] = mv_new
        vv_out[...] = vv_new

        for q in range(4):
            if q > 0:
                wait_z(q)
                b_sends[q].start()
                a_sends[2 * q].start()
                c_sends[2 * q].start()
                for i in (2 * q - 2, 2 * q - 1):
                    wait_a(i)
                    c_sends[8 + i].start()
            wait_b(q)
            a_sends[2 * q + 1].start()
            c_sends[2 * q + 1].start()
        for i in (6, 7):
            wait_a(i)
            c_sends[8 + i].start()
        for i in range(16):
            wait_c(i)

        for copy in pair_copies + [vec_pair, vec_end] + vec_plane + vec_line + a_copies + b_copies + z_copies:
            copy.wait_send()
        for d in range(1, group):
            remote(norm_rows.at[me], norm_rows.at[me], n_s.at[d], n_r.at[d], (me + d) % group).wait_send()
        for copy in z_sends + b_sends + a_sends + c_sends:
            copy.wait_send()

    vmem = pl.BlockSpec(memory_space=pltpu.VMEM)
    hbm = pl.BlockSpec(memory_space=pltpu.HBM)
    sems = pltpu.SemaphoreType.DMA
    return pl.pallas_call(
        body,
        name="adam_step",
        out_shape=(
            jax.ShapeDtypeStruct((group, rows, LANES), BF16),
            *[jax.ShapeDtypeStruct((rows, LANES), F32)] * 3,
            *[jax.ShapeDtypeStruct((vrows, LANES), F32)] * 3,
        ),
        in_specs=[hbm] * 8 + [pl.BlockSpec(memory_space=pltpu.SMEM)],
        out_specs=(vmem,) * 7,
        scratch_shapes=[
            pltpu.VMEM((16, rows, 1, LANES), BF16),
            pltpu.VMEM((16, rows, 1, LANES), BF16),
            pltpu.VMEM((8, rows, LANES), F32),
            pltpu.VMEM((8, rows, LANES), F32),
            pltpu.VMEM((4, rows, LANES), F32),
            pltpu.VMEM((4, rows, LANES), F32),
            pltpu.VMEM((4, rows, LANES), F32),
            pltpu.VMEM((4, rows, LANES), F32),
            pltpu.VMEM((rows, LANES), F32),
            pltpu.VMEM((group, 1, LANES), F32),
            *[pltpu.VMEM((rows, LANES), F32)] * 3,
            *[pltpu.VMEM((vhalf, 1, LANES), BF16)] * 2,
            *[pltpu.VMEM((4, vhalf, LANES), F32)] * 2,
            *[pltpu.VMEM((vhalf, LANES), F32)] * 2,
            *[pltpu.VMEM((vrows, LANES), F32)] * 4,
            sems((16,)), sems((16,)), sems((16,)),
            sems((8,)), sems((8,)), sems((4,)), sems((4,)), sems((4,)), sems((4,)), sems((7,)),
            sems((1,)), sems((1,)), sems((3,)), sems((3,)), sems((4,)), sems((4,)), sems((1,)), sems((1,)),
            sems((group,)), sems((group,)),
            sems((4,)), sems((4,)), sems((4,)), sems((4,)), sems((8,)), sems((8,)), sems((16,)), sems((16,)),
        ],
        compiler_params=pltpu.CompilerParams(
            collective_id=0, has_side_effects=True, vmem_limit_bytes=30 * 1024 * 1024),
    )


def store_kernel(shapes):
    def body(*refs):
        n = len(shapes)
        ins, outs, sem = refs[:n], refs[n:2 * n], refs[2 * n]
        copies = [pltpu.make_async_copy(ins[i], outs[i], sem.at[i]) for i in range(n)]
        for copy in copies:
            copy.start()
        for copy in copies:
            copy.wait()

    return pl.pallas_call(
        body,
        name="store_results",
        out_shape=tuple(shapes),
        in_specs=[pl.BlockSpec(memory_space=pltpu.VMEM)] * len(shapes),
        out_specs=tuple([pl.BlockSpec(memory_space=pltpu.HBM)] * len(shapes)),
        scratch_shapes=[pltpu.SemaphoreType.DMA((len(shapes),))],
        compiler_params=pltpu.CompilerParams(vmem_limit_bytes=16 * 1024 * 1024),
    )


def solution(mesh):
    axis_name = mesh.axis_names[0]
    group = mesh.shape[axis_name]

    def local_step(g_mat, g_vec, p_mat, m_mat, v_mat, p_vec, m_vec, v_vec, learn_rate):
        rows = p_mat.shape[0] // LANES
        vrows = p_vec.shape[0] // LANES
        operands = [
            g_mat.reshape(group * rows, 1, LANES), g_vec.reshape(vrows, 1, LANES),
            *[t.reshape(rows, LANES) for t in (p_mat, m_mat, v_mat)],
            *[t.reshape(vrows, LANES) for t in (p_vec, m_vec, v_vec)]]
        operands = [pltpu.with_memory_space_constraint(t, pltpu.HBM) for t in operands]
        results = step_kernel(group, rows, vrows, axis_name)(*operands, learn_rate.reshape(1))
        results = store_kernel([jax.ShapeDtypeStruct(r.shape, r.dtype) for r in results])(*results)
        full, new_p, new_m, new_v, new_pv, new_mv, new_vv = results
        return (*[t.reshape(-1) for t in (new_p, new_m, new_v, new_pv, new_mv, new_vv)], full.reshape(-1))

    return jax.shard_map(
        local_step,
        mesh=mesh,
        in_specs=(P(axis_name, None), P(axis_name, None), P(axis_name), P(axis_name), P(axis_name), P(), P(), P(), P()),
        out_specs=(P(axis_name), P(axis_name), P(axis_name), P(), P(), P(), P()),
        check_vma=False,
    )
```

```python
import jax
import jax.numpy as jnp
from jax import lax
from jax.experimental import pallas as pl
from jax.experimental.pallas import tpu as pltpu
from jax.sharding import PartitionSpec as P

STEP = 10
ADAM_BETA1 = 0.9
ADAM_BETA2 = 0.98
ADAM_EPS = 1e-8
WEIGHT_DECAY = 0.01
MAX_NORM = 1.0
NORM_EPS = 1e-6
BIAS_ONE = 1.0 - ADAM_BETA1 ** STEP
BIAS_TWO = 1.0 - ADAM_BETA2 ** STEP

MESH = pl.DeviceIdType.MESH
F32 = jnp.float32
BF16 = jnp.bfloat16
LANES = 128
CHUNK = 120


def adam_update(grad_vals, param_vals, moment_one, moment_two, learn_rate, decay_rate):
    new_one = ADAM_BETA1 * moment_one + (1.0 - ADAM_BETA1) * grad_vals
    new_two = ADAM_BETA2 * moment_two + (1.0 - ADAM_BETA2) * grad_vals * grad_vals
    direction = (new_one / BIAS_ONE) / (jnp.sqrt(new_two / BIAS_TWO) + ADAM_EPS)
    return param_vals - learn_rate * (direction + decay_rate * param_vals), new_one, new_two


def step_kernel(group, rows, vrows, axis_name):
    inv_group = 1.0 / group
    vstep = vrows // 16 * 8
    vhalf = vrows - vstep
    cut = (rows // 2 + 15) // 16 * 16
    halves = [pl.ds(0, cut), pl.ds(cut, rows - cut)]
    steps = []
    for lo, hi in ((0, cut), (cut, rows)):
        mid = lo + ((hi - lo) // 2 + 15) // 16 * 16
        steps.append([(lo, mid - lo), (mid, hi - mid)])

    def body(g_ref, gv_ref, p_ref, m_ref, v_ref, pv_ref, mv_ref, vv_ref, lr_ref,
             pb_out, p_out, m_out, v_out, pv_out, mv_out, vv_out,
             own, pair, send_a, recv_a, send_b, recv_b, send_z, recv_z, grad, norm_rows,
             state, gv_own, gv_pair, gv_plane, gv_line, gv_half, gv_other, gv_sum, vec_state,
             own_sem, pair_s, pair_r, a_s, a_r, b_s, b_r, z_s, z_r, load_sem,
             vc_s, vc_r, vp_s, vp_r, vz_s, vz_r, ve_s, ve_r, n_s, n_r,
             gz_s, gz_r, gb_s, gb_r, ga_s, ga_r, gc_s, gc_r):
        me = lax.axis_index(axis_name)
        core = me % 2
        x = (me // 2) % 2
        y = (me // 4) % 2
        z = me // 8
        str_a = 2 + 2 * core
        str_b = 4 - 2 * core
        a = x + core * (y - x)
        b = y + core * (x - y)
        dev_c = me + 1 - 2 * core
        dev_a = me + (1 - 2 * a) * str_a
        dev_b = me + (1 - 2 * b) * str_b
        dev_x = me + (1 - 2 * x) * 2
        dev_y = me + (1 - 2 * y) * 4
        spot = y * 2 + x
        high = z // 2
        order = [3 - 3 * high, 2 - high, 1 - z + 4 * high, z]

        def dev_z(zq):
            return me + (zq - z) * 8

        def piece(zq, flip_a, flip_b):
            aq = 1 - a if flip_a else a
            bq = 1 - b if flip_b else b
            return zq * 8 + aq * str_a + bq * str_b + core

        def partner_piece(zq, flip_a, flip_b):
            aq = 1 - b if flip_a else b
            bq = 1 - a if flip_b else a
            return zq * 8 + aq * str_b + bq * str_a + 1 - core

        def remote(src, dst, s_sem, r_sem, dev):
            return pltpu.make_async_remote_copy(
                src_ref=src, dst_ref=dst, send_sem=s_sem, recv_sem=r_sem, device_id=(dev,), device_id_type=MESH)

        flips = [(True, True), (True, False), (False, True), (False, False)]
        own_copies = []
        for j in range(4):
            for k, (fa, fb) in enumerate(flips):
                src = g_ref.at[pl.ds(piece(order[j], fa, fb) * rows, rows)]
                own_copies.append(pltpu.make_async_copy(src, own.at[j * 4 + k], own_sem.at[j * 4 + k]))
        use_order = [j * 4 + k for ks in ((0, 1), (2, 3)) for j in range(4) for k in ks]
        for i in use_order[:4]:
            own_copies[i].start()
        vec_load = pltpu.make_async_copy(gv_ref.at[pl.ds(core * vstep, vhalf)], gv_own, load_sem.at[0])
        vec_load.start()

        def wait_all(ref, sem):
            remote(ref, ref, sem, sem, dev_c).wait_recv()

        barrier = pltpu.get_barrier_semaphore()
        plane = [dev_x, dev_y, dev_x + dev_y - me]
        partners = [dev_c] + plane + [dev_z(order[j]) for j in range(3)]
        for partner in partners:
            pl.semaphore_signal(barrier, inc=1, device_id=(partner,), device_id_type=MESH)
        pl.semaphore_wait(barrier, len(partners))

        pair_copies = []
        for j in range(4):
            for k, (fa, fb) in enumerate(flips):
                src = g_ref.at[pl.ds(partner_piece(order[j], fa, fb) * rows, rows)]
                pair_copies.append(remote(src, pair.at[j * 4 + k], pair_s, pair_r.at[j * 4 + k], dev_c))
        vec_pair = remote(gv_ref.at[pl.ds((1 - core) * vstep, vhalf)], gv_pair, vc_s, vc_r, dev_c)
        vec_pair.start()
        for n, i in enumerate(use_order):
            pair_copies[i].start()
            if n >= 4:
                own_copies[i].start()
        for i, ref in enumerate((p_ref, m_ref, v_ref)):
            pltpu.make_async_copy(ref, state.at[i], load_sem.at[1]).start()
        for i, ref in enumerate((pv_ref, mv_ref, vv_ref)):
            pltpu.make_async_copy(ref, vec_state.at[i], load_sem.at[2]).start()

        def chunks(fn):
            @pl.loop(0, rows // CHUNK)
            def _(i):
                fn(pl.ds(pl.multiple_of(i * CHUNK, 8), CHUNK))

        def pair_sum(i, s):
            return own[i, s, 0, :].astype(F32) + pair[i, s, 0, :].astype(F32)

        vec_load.wait()
        vec_pair.wait_recv()
        gv_plane[spot] = gv_own[:, 0, :].astype(F32) + gv_pair[:, 0, :].astype(F32)
        vec_plane = [remote(gv_plane.at[spot], gv_plane.at[spot], vp_s, vp_r, dev) for dev in plane]
        for copy in vec_plane:
            copy.start()

        a_copies = [remote(send_a.at[i], recv_a.at[i], a_s, a_r.at[i], dev_a) for i in range(8)]
        for i in range(8):
            slot = (i // 2) * 4 + i % 2
            own_copies[slot].wait()
            pair_copies[slot].wait_recv()

            def add_pair(s, i=i, slot=slot):
                send_a[i, s, :] = pair_sum(slot, s)

            chunks(add_pair)
            a_copies[i].start()

        wait_all(gv_plane.at[pl.ds(0, 3)], vp_r)
        gv_line[z] = ((gv_plane[0] + gv_plane[1]) + gv_plane[2]) + gv_plane[3]
        vec_line = [remote(gv_line.at[z], gv_line.at[z], vz_s, vz_r, dev_z(order[j])) for j in range(3)]
        for copy in vec_line:
            copy.start()

        b_copies = [remote(send_b.at[j], recv_b.at[j], b_s, b_r.at[j], dev_b) for j in range(4)]
        z_copies = [remote(send_z.at[j], recv_z.at[z], z_s, z_r, dev_z(order[j])) for j in range(3)]

        def do_b(j):
            slot = j * 4 + 2
            own_copies[slot].wait()
            pair_copies[slot].wait_recv()
            a_copies[j * 2].wait_recv()

            def add_a(s):
                send_b[j, s, :] = pair_sum(slot, s) + recv_a[j * 2, s, :]

            chunks(add_a)
            b_copies[j].start()

        def do_z(j):
            slot = j * 4 + 3
            own_copies[slot].wait()
            pair_copies[slot].wait_recv()
            a_copies[j * 2 + 1].wait_recv()
            b_copies[j].wait_recv()

            def add_ab(s):
                send_z[j, s, :] = pair_sum(slot, s) + recv_a[j * 2 + 1, s, :] + recv_b[j, s, :]

            chunks(add_ab)
            if j < 3:
                z_copies[j].start()

        do_b(0)
        wait_all(gv_line.at[pl.ds(0, 3)], vz_r)
        gv_half[...] = (((gv_line[0] + gv_line[1]) + gv_line[2]) + gv_line[3]) * inv_group
        vec_end = remote(gv_half, gv_other, ve_s, ve_r, dev_c)
        vec_end.start()
        do_z(0)
        vec_end.wait_recv()
        gv_sum[pl.ds(pl.multiple_of(core * vstep, 8), vhalf), :] = gv_half[...]
        gv_sum[pl.ds(pl.multiple_of((1 - core) * vstep, 8), vhalf), :] = gv_other[...]
        vec_sq = jnp.sum(gv_sum[...] * gv_sum[...])
        for j in range(1, 4):
            do_b(j)
            do_z(j)

        wait_all(recv_z.at[pl.ds(0, 3)], z_r)

        def final_sum(i, acc):
            s = pl.ds(pl.multiple_of(i * CHUNK, 8), CHUNK)
            g = send_z[3, s, :]
            for j in range(3):
                g = g + recv_z[order[j], s, :]
            g = g * inv_group
            grad[s, :] = g
            return acc + jnp.sum((g * g).reshape(CHUNK // 8, 8, LANES), axis=0)

        sq = lax.fori_loop(0, rows // CHUNK, final_sum, jnp.zeros((8, LANES), F32))
        norm_rows[me] = jnp.sum(sq, axis=0, keepdims=True)

        for d in range(1, group):
            to = (me + d) % group
            remote(norm_rows.at[me], norm_rows.at[me], n_s, n_r, to).start()
        wait_all(state, load_sem.at[1])
        wait_all(vec_state, load_sem.at[2])
        wait_all(norm_rows.at[pl.ds(0, group - 1)], n_r)
        norm_sq = jnp.sum(norm_rows[...]) + vec_sq
        norm = jnp.sqrt(jnp.full((8, LANES), norm_sq, F32))
        scale = jnp.minimum(1.0, MAX_NORM / (norm + NORM_EPS))[0:1, :]
        lr = lr_ref[0]

        def adam(start, size):
            s = pl.ds(start, size)
            new_p, new_m, new_v = adam_update(grad[s, :] * scale, state[0, s, :], state[1, s, :], state[2, s, :], lr, WEIGHT_DECAY)
            p_out[s, :] = new_p
            m_out[s, :] = new_m
            v_out[s, :] = new_v
            pb_out[me, s, :] = new_p.astype(BF16)

        def plane_at(r):
            return r + high * (3 - 2 * r)

        def move(idx, h, s_sem, r_sem, dev):
            ref = pb_out.at[idx, halves[h]]
            return remote(ref, ref, s_sem, r_sem, dev)

        def send_line(r, h, to):
            zq = plane_at(r)
            move(piece(zq, False, False), h, gz_s, gz_r.at[zq * 2 + h], dev_z(plane_at(to))).start()

        def move_b(zq, flip, h):
            return move(piece(zq, False, flip), h, gb_s, gb_r.at[zq * 2 + h], dev_b)

        def move_a(zq, flip_a, fb, h):
            i = (zq * 2 + fb) * 2 + h
            return move(piece(zq, flip_a, fb == 1), h, ga_s, ga_r.at[i], dev_a)

        def move_c(zq, fa, fb, h):
            return move(piece(zq, fa == 1, fb == 1), h, gc_s, gc_r, dev_c)

        def from_line(r, h, onward_to=None):
            zq = plane_at(r)
            move(piece(zq, False, False), h, gz_s, gz_r.at[zq * 2 + h], dev_z(zq)).wait_recv()
            if onward_to is not None:
                send_line(r, h, onward_to)
            share(r, h)

        def share(r, h):
            zq = plane_at(r)
            move_b(zq, False, h).start()
            move_a(zq, False, 0, h).start()
            move_c(zq, 0, 0, h).start()

        def from_b(r, h):
            zq = plane_at(r)
            move_b(zq, True, h).wait_recv()
            move_a(zq, False, 1, h).start()
            move_c(zq, 0, 1, h).start()

        def from_a(r, fb, h):
            zq = plane_at(r)
            move_a(zq, True, fb, h).wait_recv()
            move_c(zq, 1, fb, h).start()

        def finish(line_pieces):
            wait_all(pb_out.at[pl.ds(0, group // 2)], gc_r)
            wait_all(pb_out.at[pl.ds(0, line_pieces)], gz_s)

        def update_vector():
            pv_new, mv_new, vv_new = adam_update(gv_sum[...] * scale, vec_state[0], vec_state[1], vec_state[2], lr, 0.0)
            pv_out[...] = pv_new
            mv_out[...] = mv_new
            vv_out[...] = vv_new

        inner = z + high * (3 - 2 * z)

        @pl.when(inner == 0)
        def _():
            for h in range(2):
                for start, size in steps[h]:
                    adam(start, size)
                send_line(0, h, 1)
                send_line(0, h, 2)
                share(0, h)
            update_vector()
            for h in range(2):
                from_line(1, h)
                from_b(0, h)
            for h in range(2):
                from_a(0, 0, h)
            for r in (1, 2):
                for h in range(2):
                    from_line(r + 1, h)
                    from_b(r, h)
                for h in range(2):
                    from_a(r - 1, 1, h)
                    from_a(r, 0, h)
            for h in range(2):
                from_b(3, h)
                from_a(2, 1, h)
                from_a(3, 0, h)
            for h in range(2):
                from_a(3, 1, h)
            finish(2)

        @pl.when(inner == 1)
        def _():
            for h in range(2):
                for start, size in steps[h]:
                    adam(start, size)
                send_line(1, h, 2)
                send_line(1, h, 0)
                share(1, h)
            update_vector()
            for h in range(2):
                from_line(2, h, 0)
                from_line(0, h)
                from_b(1, h)
            for h in range(2):
                from_a(1, 0, h)
            for h in range(2):
                from_line(3, h, 0)
                from_b(2, h)
                from_b(0, h)
            for h in range(2):
                from_a(1, 1, h)
                from_a(2, 0, h)
                from_a(0, 0, h)
            for h in range(2):
                from_b(3, h)
                from_a(2, 1, h)
                from_a(0, 1, h)
                from_a(3, 0, h)
            for h in range(2):
                from_a(3, 1, h)
            finish(4)

        for ref, sem in ((pair, pair_s), (gv_pair, vc_s), (gv_plane.at[pl.ds(0, 3)], vp_s),
                         (gv_line.at[pl.ds(0, 3)], vz_s), (gv_half, ve_s), (send_a, a_s), (send_b, b_s),
                         (send_z.at[pl.ds(0, 3)], z_s), (norm_rows.at[pl.ds(0, group - 1)], n_s),
                         (pb_out.at[pl.ds(0, 4)], gb_s), (pb_out.at[pl.ds(0, 8)], ga_s),
                         (pb_out.at[pl.ds(0, group // 2)], gc_s)):
            wait_all(ref, sem)

    vmem = pl.BlockSpec(memory_space=pltpu.VMEM)
    hbm = pl.BlockSpec(memory_space=pltpu.HBM)
    sem = sems = pltpu.SemaphoreType.DMA
    return pl.pallas_call(
        body,
        name="adam_step",
        out_shape=(
            jax.ShapeDtypeStruct((group, rows, LANES), BF16),
            *[jax.ShapeDtypeStruct((rows, LANES), F32)] * 3,
            *[jax.ShapeDtypeStruct((vrows, LANES), F32)] * 3,
        ),
        in_specs=[hbm] * 8 + [pl.BlockSpec(memory_space=pltpu.SMEM)],
        out_specs=(vmem,) * 7,
        scratch_shapes=[
            pltpu.VMEM((16, rows, 1, LANES), BF16),
            pltpu.VMEM((16, rows, 1, LANES), BF16),
            pltpu.VMEM((8, rows, LANES), F32),
            pltpu.VMEM((8, rows, LANES), F32),
            pltpu.VMEM((4, rows, LANES), F32),
            pltpu.VMEM((4, rows, LANES), F32),
            pltpu.VMEM((4, rows, LANES), F32),
            pltpu.VMEM((4, rows, LANES), F32),
            pltpu.VMEM((rows, LANES), F32),
            pltpu.VMEM((group, 1, LANES), F32),
            pltpu.VMEM((3, rows, LANES), F32),
            *[pltpu.VMEM((vhalf, 1, LANES), BF16)] * 2,
            *[pltpu.VMEM((4, vhalf, LANES), F32)] * 2,
            *[pltpu.VMEM((vhalf, LANES), F32)] * 2,
            pltpu.VMEM((vrows, LANES), F32),
            pltpu.VMEM((3, vrows, LANES), F32),
            sems((16,)), sem, sems((16,)), sem, sems((8,)), sem, sems((4,)), sem, sem, sems((3,)),
            *[sem] * 8, sem, sem,
            sem, sems((8,)), sem, sems((8,)), sem, sems((16,)), sem, sem,
        ],
        compiler_params=pltpu.CompilerParams(
            collective_id=0, has_side_effects=True, vmem_limit_bytes=30 * 1024 * 1024),
    )


def store_kernel(shapes):
    def body(*refs):
        n = len(shapes)
        ins, outs, sem = refs[:n], refs[n:2 * n], refs[2 * n]
        copies = [pltpu.make_async_copy(ins[i], outs[i], sem.at[i]) for i in range(n)]
        for copy in copies:
            copy.start()
        for copy in copies:
            copy.wait()

    return pl.pallas_call(
        body,
        name="store_results",
        out_shape=tuple(shapes),
        in_specs=[pl.BlockSpec(memory_space=pltpu.VMEM)] * len(shapes),
        out_specs=tuple([pl.BlockSpec(memory_space=pltpu.HBM)] * len(shapes)),
        scratch_shapes=[pltpu.SemaphoreType.DMA((len(shapes),))],
        compiler_params=pltpu.CompilerParams(vmem_limit_bytes=16 * 1024 * 1024),
    )


def solution(mesh):
    axis_name = mesh.axis_names[0]
    group = mesh.shape[axis_name]

    def local_step(g_mat, g_vec, p_mat, m_mat, v_mat, p_vec, m_vec, v_vec, learn_rate):
        rows = p_mat.shape[0] // LANES
        vrows = p_vec.shape[0] // LANES
        operands = [
            g_mat.reshape(group * rows, 1, LANES), g_vec.reshape(vrows, 1, LANES),
            *[t.reshape(rows, LANES) for t in (p_mat, m_mat, v_mat)],
            *[t.reshape(vrows, LANES) for t in (p_vec, m_vec, v_vec)]]
        operands = [pltpu.with_memory_space_constraint(t, pltpu.HBM) for t in operands]
        results = step_kernel(group, rows, vrows, axis_name)(*operands, learn_rate.reshape(1))
        results = store_kernel([jax.ShapeDtypeStruct(r.shape, r.dtype) for r in results])(*results)
        full, new_p, new_m, new_v, new_pv, new_mv, new_vv = results
        return (*[t.reshape(-1) for t in (new_p, new_m, new_v, new_pv, new_mv, new_vv)], full.reshape(-1))

    return jax.shard_map(
        local_step,
        mesh=mesh,
        in_specs=(P(axis_name, None), P(axis_name, None), P(axis_name), P(axis_name), P(axis_name), P(), P(), P(), P()),
        out_specs=(P(axis_name), P(axis_name), P(axis_name), P(), P(), P(), P()),
        check_vma=False,
    )
```

```python
import jax
import jax.numpy as jnp
from jax import lax
from jax.experimental import pallas as pl
from jax.experimental.pallas import tpu as pltpu
from jax.sharding import PartitionSpec as P

STEP = 10
ADAM_BETA1 = 0.9
ADAM_BETA2 = 0.98
ADAM_EPS = 1e-8
WEIGHT_DECAY = 0.01
MAX_NORM = 1.0
NORM_EPS = 1e-6
BIAS_ONE = 1.0 - ADAM_BETA1 ** STEP
BIAS_TWO = 1.0 - ADAM_BETA2 ** STEP

MESH = pl.DeviceIdType.MESH
F32 = jnp.float32
BF16 = jnp.bfloat16
LANES = 128
CHUNK = 120


def adam_update(grad_vals, param_vals, moment_one, moment_two, learn_rate, decay_rate):
    new_one = ADAM_BETA1 * moment_one + (1.0 - ADAM_BETA1) * grad_vals
    new_two = ADAM_BETA2 * moment_two + (1.0 - ADAM_BETA2) * grad_vals * grad_vals
    direction = (new_one / BIAS_ONE) / (jnp.sqrt(new_two / BIAS_TWO) + ADAM_EPS)
    return param_vals - learn_rate * (direction + decay_rate * param_vals), new_one, new_two


def step_kernel(group, rows, vrows, axis_name):
    inv_group = 1.0 / group
    vstep = vrows // 16 * 8
    vhalf = vrows - vstep
    last = rows * 3 // 5 // CHUNK * CHUNK
    cut = (rows // 2 + 15) // 16 * 16
    halves = [pl.ds(0, cut), pl.ds(cut, rows - cut)]
    steps = []
    for lo, hi in ((0, cut), (cut, rows)):
        mid = lo + ((hi - lo) // 2 + 15) // 16 * 16
        steps.append([(lo, mid - lo), (mid, hi - mid)])

    def body(g_ref, gv_ref, p_ref, m_ref, v_ref, pv_ref, mv_ref, vv_ref, lr_ref,
             pb_out, p_out, m_out, v_out, pv_out, mv_out, vv_out,
             own, pair, send_a, recv_a, send_b, recv_b, send_z, recv_z, mid, mid_recv, mid_b, mid_b_recv, grad, norm_rows,
             state, gv_own, gv_pair, gv_plane, gv_line, gv_half, gv_other, gv_sum, vec_state,
             own_sem, pair_s, pair_r, a_s, a_r, b_s, b_r, z_s, z_r, m_s, m_r, mb_s, mb_r, load_sem,
             vc_s, vc_r, vp_s, vp_r, vz_s, vz_r, ve_s, ve_r, n_s, n_r,
             gz_s, gz_r, gb_s, gb_r, ga_s, ga_r, gc_s, gc_r):
        me = lax.axis_index(axis_name)
        core = me % 2
        x = (me // 2) % 2
        y = (me // 4) % 2
        z = me // 8
        str_a = 2 + 2 * core
        str_b = 4 - 2 * core
        a = x + core * (y - x)
        b = y + core * (x - y)
        dev_c = me + 1 - 2 * core
        dev_a = me + (1 - 2 * a) * str_a
        dev_b = me + (1 - 2 * b) * str_b
        dev_x = me + (1 - 2 * x) * 2
        dev_y = me + (1 - 2 * y) * 4
        spot = y * 2 + x
        high = z // 2
        order = [3 - 3 * high, 2 - high, 1 - z + 4 * high, z]

        place = z + high * (3 - 2 * z)

        def plane_at(r):
            return r + high * (3 - 2 * r)

        def dev_z(zq):
            return me + (zq - z) * 8

        def piece(zq, flip_a, flip_b):
            aq = 1 - a if flip_a else a
            bq = 1 - b if flip_b else b
            return zq * 8 + aq * str_a + bq * str_b + core

        def partner_piece(zq, flip_a, flip_b):
            aq = 1 - b if flip_a else b
            bq = 1 - a if flip_b else a
            return zq * 8 + aq * str_b + bq * str_a + 1 - core

        def remote(src, dst, s_sem, r_sem, dev):
            return pltpu.make_async_remote_copy(
                src_ref=src, dst_ref=dst, send_sem=s_sem, recv_sem=r_sem, device_id=(dev,), device_id_type=MESH)

        flips = [(True, True), (True, False), (False, True), (False, False)]
        own_copies = []
        for j in range(4):
            for k, (fa, fb) in enumerate(flips):
                src = g_ref.at[pl.ds(piece(order[j], fa, fb) * rows, rows)]
                own_copies.append(pltpu.make_async_copy(src, own.at[j * 4 + k], own_sem.at[j * 4 + k]))
        use_order = [j * 4 + k for ks in ((0, 1), (2, 3)) for j in range(4) for k in ks]
        for i in use_order[:4]:
            own_copies[i].start()
        vec_load = pltpu.make_async_copy(gv_ref.at[pl.ds(core * vstep, vhalf)], gv_own, load_sem.at[0])
        vec_load.start()

        def wait_all(ref, sem):
            remote(ref, ref, sem, sem, dev_c).wait_recv()

        barrier = pltpu.get_barrier_semaphore()
        plane = [dev_x, dev_y, dev_x + dev_y - me]
        partners = [dev_c] + plane + [dev_z(order[j]) for j in range(3)]
        for partner in partners:
            pl.semaphore_signal(barrier, inc=1, device_id=(partner,), device_id_type=MESH)
        pl.semaphore_wait(barrier, len(partners))

        pair_copies = []
        for j in range(4):
            for k, (fa, fb) in enumerate(flips):
                src = g_ref.at[pl.ds(partner_piece(order[j], fa, fb) * rows, rows)]
                pair_copies.append(remote(src, pair.at[j * 4 + k], pair_s, pair_r.at[j * 4 + k], dev_c))
        vec_pair = remote(gv_ref.at[pl.ds((1 - core) * vstep, vhalf)], gv_pair, vc_s, vc_r, dev_c)
        for n, i in enumerate(use_order):
            pair_copies[i].start()
            if n == 1:
                vec_pair.start()
            if n >= 4:
                own_copies[i].start()
        for i, ref in enumerate((p_ref, m_ref, v_ref)):
            pltpu.make_async_copy(ref, state.at[i], load_sem.at[1]).start()
        for i, ref in enumerate((pv_ref, mv_ref, vv_ref)):
            pltpu.make_async_copy(ref, vec_state.at[i], load_sem.at[2]).start()

        def chunks(start, stop, fn):
            @pl.loop(0, (stop - start) // CHUNK)
            def _(i):
                fn(pl.ds(pl.multiple_of(start + i * CHUNK, 8), CHUNK), pl.ds(pl.multiple_of(i * CHUNK, 8), CHUNK))

        def pair_sum(i, s):
            return own[i, s, 0, :].astype(F32) + pair[i, s, 0, :].astype(F32)

        def move_a_sum(i, first):
            part = pl.ds(0, last) if first else pl.ds(last, rows - last)
            return remote(send_a.at[i, part], recv_a.at[i, part], a_s, a_r.at[i * 2 + first], dev_a)

        def do_a(i, first):
            slot = (i // 2) * 4 + i % 2
            if not first:
                own_copies[slot].wait()
                pair_copies[slot].wait_recv()

            def add_pair(s, _):
                send_a[i, s, :] = pair_sum(slot, s)

            chunks(*((0, last) if first else (last, rows)), add_pair)
            move_a_sum(i, first).start()

        do_a(0, 0)

        vec_load.wait()
        vec_pair.wait_recv()
        gv_plane[spot] = gv_own[:, 0, :].astype(F32) + gv_pair[:, 0, :].astype(F32)
        vec_plane = [remote(gv_plane.at[spot], gv_plane.at[spot], vp_s, vp_r, dev) for dev in plane]
        for copy in vec_plane:
            copy.start()

        for i in range(1, 8):
            do_a(i, 0)
        for i in (0, 2, 1, 4, 3, 5, 6, 7):
            do_a(i, 1)

        wait_all(gv_plane.at[pl.ds(0, 3)], vp_r)
        gv_line[z] = ((gv_plane[0] + gv_plane[1]) + gv_plane[2]) + gv_plane[3]
        vec_line = [remote(gv_line.at[z], gv_line.at[z], vz_s, vz_r, dev_z(order[j])) for j in range(3)]
        for copy in vec_line:
            copy.start()

        def move_mid(j, kind, slot, r):
            at = slot * 2 + kind
            return remote(mid.at[j, kind], mid_recv.at[slot, kind], m_s, m_r.at[at], dev_z(plane_at(r)))

        def do_mid(j):
            for kind in (1, 0):
                slot = j * 4 + 3 - kind
                i = j * 2 + 1 - kind
                own_copies[slot].wait()
                pair_copies[slot].wait_recv()
                move_a_sum(i, 0).wait_recv()

                def add_a(s, t, kind=kind, slot=slot, i=i):
                    mid[j, kind, t, :] = pair_sum(slot, s) + recv_a[i, s, :]

                chunks(last, rows, add_a)
                if j < 3:
                    @pl.when(place == 0)
                    def _(kind=kind):
                        move_mid(j, kind, (2, 3, 0)[j], 1).start()
                if j == 2:
                    @pl.when(place == 1)
                    def _(kind=kind):
                        move_mid(j, kind, 0, 0).start()

        def merge_mid(j):
            @pl.when(place == 1)
            def _():
                for kind in (1, 0):
                    move_mid(j, kind, 2 + j, 0).wait_recv()

                    def add_end(_, t, kind=kind):
                        mid[j, kind, t, :] = mid[j, kind, t, :] + mid_recv[2 + j, kind, t, :]

                    chunks(last, rows, add_end)
                    move_mid(j, kind, 1, 3 - j).start()

        def mid_total(kind, t):
            return mid[3, kind, t, :] + mid_recv[0, kind, t, :] + mid_recv[1, kind, t, :]

        def wait_mid(kind):
            for slot in range(2):
                move_mid(3, kind, slot, 2).wait_recv()

        mid_b_copy = remote(mid_b, mid_b_recv, mb_s, mb_r, dev_b)

        def mid_second():
            wait_mid(1)

            def add_mid(_, t):
                mid_b[t, :] = mid_total(1, t)

            chunks(last, rows, add_mid)
            mid_b_copy.start()

        b_copies = [remote(send_b.at[j], recv_b.at[j], b_s, b_r.at[j], dev_b) for j in range(4)]
        z_copies = [remote(send_z.at[j], recv_z.at[z], z_s, z_r, dev_z(order[j])) for j in range(3)]

        def do_b(j):
            move_a_sum(j * 2, 1).wait_recv()

            def add_a(s, _):
                send_b[j, s, :] = pair_sum(j * 4 + 2, s) + recv_a[j * 2, s, :]

            chunks(0, last, add_a)
            b_copies[j].start()

        def plane_total(j, s):
            return pair_sum(j * 4 + 3, s) + recv_a[j * 2 + 1, s, :] + recv_b[j, s, :]

        def do_z(j):
            move_a_sum(j * 2 + 1, 1).wait_recv()
            b_copies[j].wait_recv()

            def add_ab(s, _):
                send_z[j, s, :] = plane_total(j, s)

            if j < 3:
                chunks(0, last, add_ab)
                z_copies[j].start()

        do_mid(0)
        do_mid(1)
        wait_all(gv_line.at[pl.ds(0, 3)], vz_r)
        gv_half[...] = (((gv_line[0] + gv_line[1]) + gv_line[2]) + gv_line[3]) * inv_group
        vec_end = remote(gv_half, gv_other, ve_s, ve_r, dev_c)
        vec_end.start()
        do_mid(2)
        merge_mid(0)
        do_mid(3)
        vec_end.wait_recv()
        gv_sum[pl.ds(pl.multiple_of(core * vstep, 8), vhalf), :] = gv_half[...]
        gv_sum[pl.ds(pl.multiple_of((1 - core) * vstep, 8), vhalf), :] = gv_other[...]
        vec_sq = jnp.sum(gv_sum[...] * gv_sum[...])
        do_b(0)
        merge_mid(1)
        do_b(1)
        do_z(0)
        do_b(2)
        do_z(1)
        do_z(2)
        do_b(3)
        mid_second()
        wait_mid(0)
        mid_b_copy.wait_recv()

        def squares(acc, g):
            return acc + jnp.sum((g * g).reshape(CHUNK // 8, 8, LANES), axis=0)

        def final_mid(i, acc):
            t = pl.ds(pl.multiple_of(i * CHUNK, 8), CHUNK)
            g = (mid_total(0, t) + mid_b_recv[t, :]) * inv_group
            grad[pl.ds(pl.multiple_of(last + i * CHUNK, 8), CHUNK), :] = g
            return squares(acc, g)

        def final_last(i, acc):
            s = pl.ds(pl.multiple_of(i * CHUNK, 8), CHUNK)
            g = plane_total(3, s)
            for j in range(3):
                g = g + recv_z[order[j], s, :]
            g = g * inv_group
            grad[s, :] = g
            return squares(acc, g)

        sq = lax.fori_loop(0, (rows - last) // CHUNK, final_mid, jnp.zeros((8, LANES), F32))
        do_z(3)
        wait_all(recv_z.at[pl.ds(0, 3)], z_r)
        sq = lax.fori_loop(0, last // CHUNK, final_last, sq)
        norm_rows[me] = jnp.sum(sq, axis=0, keepdims=True)

        for d in range(1, group):
            to = (me + d) % group
            remote(norm_rows.at[me], norm_rows.at[me], n_s, n_r, to).start()
        wait_all(state, load_sem.at[1])
        wait_all(vec_state, load_sem.at[2])
        wait_all(norm_rows.at[pl.ds(0, group - 1)], n_r)
        norm_sq = jnp.sum(norm_rows[...]) + vec_sq
        norm = jnp.sqrt(jnp.full((8, LANES), norm_sq, F32))
        scale = jnp.minimum(1.0, MAX_NORM / (norm + NORM_EPS))[0:1, :]
        lr = lr_ref[0]

        def adam(start, size):
            s = pl.ds(start, size)
            new_p, new_m, new_v = adam_update(grad[s, :] * scale, state[0, s, :], state[1, s, :], state[2, s, :], lr, WEIGHT_DECAY)
            p_out[s, :] = new_p
            m_out[s, :] = new_m
            v_out[s, :] = new_v
            pb_out[me, s, :] = new_p.astype(BF16)

        def move(idx, h, s_sem, r_sem, dev):
            ref = pb_out.at[idx, halves[h]]
            return remote(ref, ref, s_sem, r_sem, dev)

        def send_line(r, h, to):
            zq = plane_at(r)
            move(piece(zq, False, False), h, gz_s, gz_r.at[zq * 2 + h], dev_z(plane_at(to))).start()

        def move_b(zq, flip, h):
            return move(piece(zq, False, flip), h, gb_s, gb_r.at[zq * 2 + h], dev_b)

        def move_a(zq, flip_a, fb, h):
            i = (zq * 2 + fb) * 2 + h
            return move(piece(zq, flip_a, fb == 1), h, ga_s, ga_r.at[i], dev_a)

        def move_c(zq, fa, fb, h):
            return move(piece(zq, fa == 1, fb == 1), h, gc_s, gc_r, dev_c)

        def from_line(r, h, onward_to=None):
            zq = plane_at(r)
            move(piece(zq, False, False), h, gz_s, gz_r.at[zq * 2 + h], dev_z(zq)).wait_recv()
            if onward_to is not None:
                send_line(r, h, onward_to)
            share(r, h)

        def share(r, h):
            zq = plane_at(r)
            move_b(zq, False, h).start()
            move_a(zq, False, 0, h).start()
            move_c(zq, 0, 0, h).start()

        def from_b(r, h):
            zq = plane_at(r)
            move_b(zq, True, h).wait_recv()
            move_a(zq, False, 1, h).start()
            move_c(zq, 0, 1, h).start()

        def from_a(r, fb, h):
            zq = plane_at(r)
            move_a(zq, True, fb, h).wait_recv()
            move_c(zq, 1, fb, h).start()

        def finish(line_pieces):
            wait_all(pb_out.at[pl.ds(0, group // 2)], gc_r)
            wait_all(pb_out.at[pl.ds(0, line_pieces)], gz_s)

        def update_vector():
            pv_new, mv_new, vv_new = adam_update(gv_sum[...] * scale, vec_state[0], vec_state[1], vec_state[2], lr, 0.0)
            pv_out[...] = pv_new
            mv_out[...] = mv_new
            vv_out[...] = vv_new

        @pl.when(place == 0)
        def _():
            for h in range(2):
                for start, size in steps[h]:
                    adam(start, size)
                send_line(0, h, 1)
                send_line(0, h, 2)
                share(0, h)
            update_vector()
            for h in range(2):
                from_line(1, h)
                from_b(0, h)
            for h in range(2):
                from_a(0, 0, h)
            for r in (1, 2):
                for h in range(2):
                    from_line(r + 1, h)
                    from_b(r, h)
                for h in range(2):
                    from_a(r - 1, 1, h)
                    from_a(r, 0, h)
            for h in range(2):
                from_b(3, h)
                from_a(2, 1, h)
                from_a(3, 0, h)
            for h in range(2):
                from_a(3, 1, h)
            finish(2)

        @pl.when(place == 1)
        def _():
            for h in range(2):
                for start, size in steps[h]:
                    adam(start, size)
                send_line(1, h, 2)
                send_line(1, h, 0)
                share(1, h)
            update_vector()
            for h in range(2):
                from_line(2, h, 0)
                from_line(0, h)
                from_b(1, h)
            for h in range(2):
                from_a(1, 0, h)
            for h in range(2):
                from_line(3, h, 0)
                from_b(2, h)
                from_b(0, h)
            for h in range(2):
                from_a(1, 1, h)
                from_a(2, 0, h)
                from_a(0, 0, h)
            for h in range(2):
                from_b(3, h)
                from_a(2, 1, h)
                from_a(0, 1, h)
                from_a(3, 0, h)
            for h in range(2):
                from_a(3, 1, h)
            finish(4)

        for ref, sem in ((pair, pair_s), (gv_pair, vc_s), (gv_plane.at[pl.ds(0, 3)], vp_s),
                         (gv_line.at[pl.ds(0, 3)], vz_s), (gv_half, ve_s), (send_a, a_s), (send_b, b_s),
                         (send_z.at[pl.ds(0, 3)], z_s), (mid.at[pl.ds(0, 3)], m_s), (mid_b, mb_s), (norm_rows.at[pl.ds(0, group - 1)], n_s),
                         (pb_out.at[pl.ds(0, 4)], gb_s), (pb_out.at[pl.ds(0, 8)], ga_s),
                         (pb_out.at[pl.ds(0, group // 2)], gc_s)):
            wait_all(ref, sem)

    vmem = pl.BlockSpec(memory_space=pltpu.VMEM)
    hbm = pl.BlockSpec(memory_space=pltpu.HBM)
    sem = sems = pltpu.SemaphoreType.DMA
    return pl.pallas_call(
        body,
        name="adam_step",
        out_shape=(
            jax.ShapeDtypeStruct((group, rows, LANES), BF16),
            *[jax.ShapeDtypeStruct((rows, LANES), F32)] * 3,
            *[jax.ShapeDtypeStruct((vrows, LANES), F32)] * 3,
        ),
        in_specs=[hbm] * 8 + [pl.BlockSpec(memory_space=pltpu.SMEM)],
        out_specs=(vmem,) * 7,
        scratch_shapes=[
            pltpu.VMEM((16, rows, 1, LANES), BF16),
            pltpu.VMEM((16, rows, 1, LANES), BF16),
            *[pltpu.VMEM((8, rows, LANES), F32)] * 2,
            *[pltpu.VMEM((4, last, LANES), F32)] * 4,
            *[pltpu.VMEM((4, 2, rows - last, LANES), F32)] * 2,
            *[pltpu.VMEM((rows - last, LANES), F32)] * 2,
            pltpu.VMEM((rows, LANES), F32),
            pltpu.VMEM((group, 1, LANES), F32),
            pltpu.VMEM((3, rows, LANES), F32),
            *[pltpu.VMEM((vhalf, 1, LANES), BF16)] * 2,
            *[pltpu.VMEM((4, vhalf, LANES), F32)] * 2,
            *[pltpu.VMEM((vhalf, LANES), F32)] * 2,
            pltpu.VMEM((vrows, LANES), F32),
            pltpu.VMEM((3, vrows, LANES), F32),
            sems((16,)), sem, sems((16,)), sem, sems((16,)), sem, sems((4,)), sem, sem, sem, sems((8,)), sem, sem, sems((3,)),
            *[sem] * 8, sem, sem,
            sem, sems((8,)), sem, sems((8,)), sem, sems((16,)), sem, sem,
        ],
        compiler_params=pltpu.CompilerParams(
            collective_id=0, has_side_effects=True, vmem_limit_bytes=32 * 1024 * 1024),
    )


def store_kernel(shapes):
    def body(*refs):
        n = len(shapes)
        ins, outs, sem = refs[:n], refs[n:2 * n], refs[2 * n]
        copies = [pltpu.make_async_copy(ins[i], outs[i], sem.at[i]) for i in range(n)]
        for copy in copies:
            copy.start()
        for copy in copies:
            copy.wait()

    return pl.pallas_call(
        body,
        name="store_results",
        out_shape=tuple(shapes),
        in_specs=[pl.BlockSpec(memory_space=pltpu.VMEM)] * len(shapes),
        out_specs=tuple([pl.BlockSpec(memory_space=pltpu.HBM)] * len(shapes)),
        scratch_shapes=[pltpu.SemaphoreType.DMA((len(shapes),))],
        compiler_params=pltpu.CompilerParams(vmem_limit_bytes=16 * 1024 * 1024),
    )


def solution(mesh):
    axis_name = mesh.axis_names[0]
    group = mesh.shape[axis_name]

    def local_step(g_mat, g_vec, p_mat, m_mat, v_mat, p_vec, m_vec, v_vec, learn_rate):
        rows = p_mat.shape[0] // LANES
        vrows = p_vec.shape[0] // LANES
        operands = [
            g_mat.reshape(group * rows, 1, LANES), g_vec.reshape(vrows, 1, LANES),
            *[t.reshape(rows, LANES) for t in (p_mat, m_mat, v_mat)],
            *[t.reshape(vrows, LANES) for t in (p_vec, m_vec, v_vec)]]
        operands = [pltpu.with_memory_space_constraint(t, pltpu.HBM) for t in operands]
        results = step_kernel(group, rows, vrows, axis_name)(*operands, learn_rate.reshape(1))
        results = store_kernel([jax.ShapeDtypeStruct(r.shape, r.dtype) for r in results])(*results)
        full, new_p, new_m, new_v, new_pv, new_mv, new_vv = results
        return (*[t.reshape(-1) for t in (new_p, new_m, new_v, new_pv, new_mv, new_vv)], full.reshape(-1))

    return jax.shard_map(
        local_step,
        mesh=mesh,
        in_specs=(P(axis_name, None), P(axis_name, None), P(axis_name), P(axis_name), P(axis_name), P(), P(), P(), P()),
        out_specs=(P(axis_name), P(axis_name), P(axis_name), P(), P(), P(), P()),
        check_vma=False,
    )
```

```python
import jax
import jax.numpy as jnp
from jax import lax
from jax.experimental import pallas as pl
from jax.experimental.pallas import tpu as pltpu
from jax.sharding import PartitionSpec as P

STEP = 10
ADAM_BETA1 = 0.9
ADAM_BETA2 = 0.98
ADAM_EPS = 1e-8
WEIGHT_DECAY = 0.01
MAX_NORM = 1.0
NORM_EPS = 1e-6
BIAS_ONE = 1.0 - ADAM_BETA1 ** STEP
BIAS_TWO = 1.0 - ADAM_BETA2 ** STEP

MESH = pl.DeviceIdType.MESH
F32 = jnp.float32
BF16 = jnp.bfloat16
LANES = 128
STEPS = 3


END_PLAN = [
    "z100", "b00", "z110", "b01", "b02", "z120", "a00", "z200", "b10", "z210", "b11", "z220",
    "z121", "a01", "a10", "z300", "b20", "z310", "b21", "z320", "z221", "a11", "a20", "z321",
    "b30", "b31", "a21", "a30", "a31",
]
INNER_PLAN = [
    "z200", "z000", "b10", "z210", "z010", "b11", "b12", "z220", "z020", "a10", "z300", "b20",
    "b00", "z310", "b21", "b01", "z320", "z221", "z021", "a11", "a20", "a00", "z321", "b30",
    "b31", "a21", "a01", "a30", "a31",
]


def adam_update(grad_vals, param_vals, moment_one, moment_two, learn_rate, decay_rate):
    new_one = ADAM_BETA1 * moment_one + (1.0 - ADAM_BETA1) * grad_vals
    new_two = ADAM_BETA2 * moment_two + (1.0 - ADAM_BETA2) * grad_vals * grad_vals
    direction = (new_one / BIAS_ONE) / (jnp.sqrt(new_two / BIAS_TWO) + ADAM_EPS)
    return param_vals - learn_rate * (direction + decay_rate * param_vals), new_one, new_two


def step_kernel(group, rows, vrows, axis_name):
    inv_group = 1.0 / group
    vstep = vrows // 16 * 8
    vhalf = vrows - vstep
    last = rows * 3 // 5 // (8 * STEPS) * (8 * STEPS)
    early, late = 176, 352
    bounds = (0, early, late, rows)
    parts = [pl.ds(lo, hi - lo) for lo, hi in zip(bounds, bounds[1:])]
    steps = []
    for lo, hi in zip(bounds, bounds[1:]):
        half = lo + ((hi - lo) // 2 + 15) // 16 * 16
        steps.append([(lo, half - lo), (half, hi - half)])

    def body(g_ref, gv_ref, p_ref, m_ref, v_ref, pv_ref, mv_ref, vv_ref, lr_ref,
             pb_out, p_out, m_out, v_out, pv_out, mv_out, vv_out,
             own, pair, send_a, recv_a, send_b, recv_b, send_z, recv_z, mid, mid_recv, mid_b, mid_b_recv, grad, norm_rows,
             state, gv_own, gv_pair, gv_plane, gv_line, gv_half, gv_other, gv_sum, vec_state,
             own_sem, pool, pair_s, a_s, b_s, z_s, z_r, m_s, mb_s, mb_r, load_sem,
             vc_s, vc_r, vp_s, vp_r, vz_s, vz_r, ve_s, ve_r, n_s, n_r,
             gz_s, gb_s, ga_s, gc_s, gc_r):
        me = lax.axis_index(axis_name)
        core = me % 2
        x = (me // 2) % 2
        y = (me // 4) % 2
        z = me // 8
        str_a = 2 + 2 * core
        str_b = 4 - 2 * core
        a = x + core * (y - x)
        b = y + core * (x - y)
        dev_c = me + 1 - 2 * core
        dev_a = me + (1 - 2 * a) * str_a
        dev_b = me + (1 - 2 * b) * str_b
        dev_x = me + (1 - 2 * x) * 2
        dev_y = me + (1 - 2 * y) * 4
        spot = y * 2 + x
        high = z // 2
        order = [3 - 3 * high, 2 - high, 1 - z + 4 * high, z]

        place = z + high * (3 - 2 * z)

        def plane_at(r):
            return r + high * (3 - 2 * r)

        def dev_z(zq):
            return me + (zq - z) * 8

        def piece(zq, flip_a, flip_b):
            aq = 1 - a if flip_a else a
            bq = 1 - b if flip_b else b
            return zq * 8 + aq * str_a + bq * str_b + core

        def partner_piece(zq, flip_a, flip_b):
            aq = 1 - b if flip_a else b
            bq = 1 - a if flip_b else a
            return zq * 8 + aq * str_b + bq * str_a + 1 - core

        def remote(src, dst, s_sem, r_sem, dev):
            return pltpu.make_async_remote_copy(
                src_ref=src, dst_ref=dst, send_sem=s_sem, recv_sem=r_sem, device_id=(dev,), device_id_type=MESH)

        flips = [(True, True), (True, False), (False, True), (False, False)]
        own_copies = []
        for j in range(4):
            for k, (fa, fb) in enumerate(flips):
                src = g_ref.at[pl.ds(piece(order[j], fa, fb) * rows, rows)]
                group_of = 0 if j + k == 0 else 1 + k // 2
                own_copies.append(pltpu.make_async_copy(src, own.at[j * 4 + k], own_sem.at[group_of]))
        use_order = [j * 4 + k for ks in ((0, 1), (2, 3)) for j in range(4) for k in ks]
        for i in use_order[:4]:
            own_copies[i].start()
        vec_load = pltpu.make_async_copy(gv_ref.at[pl.ds(core * vstep, vhalf)], gv_own, load_sem.at[0])
        vec_load.start()

        def wait_all(ref, sem):
            remote(ref, ref, sem, sem, dev_c).wait_recv()

        barrier = pltpu.get_barrier_semaphore()
        plane = [dev_x, dev_y, dev_x + dev_y - me]
        partners = [dev_c] + plane + [dev_z(order[j]) for j in range(3)]
        for partner in partners:
            pl.semaphore_signal(barrier, inc=1, device_id=(partner,), device_id_type=MESH)
        pl.semaphore_wait(barrier, len(partners))

        pair_copies = []
        for j in range(4):
            for k, (fa, fb) in enumerate(flips):
                src = g_ref.at[pl.ds(partner_piece(order[j], fa, fb) * rows, rows)]
                arrival = pool.at[j * 2 + k if k < 2 else 8 + j // 2]
                pair_copies.append(remote(src, pair.at[j * 4 + k], pair_s, arrival, dev_c))
        vec_pair = remote(gv_ref.at[pl.ds((1 - core) * vstep, vhalf)], gv_pair, vc_s, vc_r, dev_c)
        for n, i in enumerate(use_order):
            pair_copies[i].start()
            if n == 1:
                vec_pair.start()
            if n >= 4:
                own_copies[i].start()
        for i, ref in enumerate((p_ref, m_ref, v_ref)):
            pltpu.make_async_copy(ref, state.at[i], load_sem.at[1]).start()
        for i, ref in enumerate((pv_ref, mv_ref, vv_ref)):
            pltpu.make_async_copy(ref, vec_state.at[i], load_sem.at[2]).start()

        def chunks(start, stop, fn):
            size = (stop - start) // STEPS

            @pl.loop(0, STEPS)
            def _(i):
                fn(pl.ds(pl.multiple_of(start + i * size, 8), size), pl.ds(pl.multiple_of(i * size, 8), size))

        def pair_sum(i, s):
            return own[i, s, 0, :].astype(F32) + pair[i, s, 0, :].astype(F32)

        def move_a_sum(i, first):
            part = pl.ds(0, last) if first else pl.ds(last, rows - last)
            return remote(send_a.at[i, part], recv_a.at[i, part], a_s, pool.at[10 + i * 2 + first], dev_a)

        loaded = set()

        def do_a(i, first):
            slot = (i // 2) * 4 + i % 2
            if slot not in loaded:
                loaded.add(slot)
                if len(loaded) == 1:
                    own_copies[0].wait()
                if len(loaded) == 2:
                    wait_all(own.at[pl.ds(0, 7)], own_sem.at[1])
                pair_copies[slot].wait_recv()

            def add_pair(s, _):
                send_a[i, s, :] = pair_sum(slot, s)

            chunks(*((0, last) if first else (last, rows)), add_pair)
            move_a_sum(i, first).start()

        do_a(0, 0)

        vec_load.wait()
        vec_pair.wait_recv()
        gv_plane[spot] = gv_own[:, 0, :].astype(F32) + gv_pair[:, 0, :].astype(F32)
        vec_plane = [remote(gv_plane.at[spot], gv_plane.at[spot], vp_s, vp_r, dev) for dev in plane]
        for copy in vec_plane:
            copy.start()

        for i, first in [(1, 0), (2, 0), (3, 0), (4, 0), (5, 0), (0, 1), (2, 1), (6, 0), (7, 0), (1, 1), (4, 1), (3, 1), (5, 1), (6, 1), (7, 1)]:
            do_a(i, first)

        wait_all(gv_plane.at[pl.ds(0, 3)], vp_r)
        gv_line[z] = ((gv_plane[0] + gv_plane[1]) + gv_plane[2]) + gv_plane[3]
        vec_line = [remote(gv_line.at[z], gv_line.at[z], vz_s, vz_r, dev_z(order[j])) for j in range(3)]
        for copy in vec_line:
            copy.start()

        def move_mid(j, kind, slot, r):
            at = slot * 2 + kind
            return remote(mid.at[j, kind], mid_recv.at[slot, kind], m_s, pool.at[30 + at], dev_z(plane_at(r)))

        def do_mid(j):
            for kind in (1, 0):
                slot = j * 4 + 3 - kind
                i = j * 2 + 1 - kind
                if j == 0 and kind == 1:
                    wait_all(own.at[pl.ds(0, 8)], own_sem.at[2])
                if j % 2 == 0 and kind == 1:
                    wait_all(pair.at[pl.ds(0, 4)], pool.at[8 + j // 2])
                move_a_sum(i, 0).wait_recv()

                def add_a(s, t, kind=kind, slot=slot, i=i):
                    mid[j, kind, t, :] = pair_sum(slot, s) + recv_a[i, s, :]

                chunks(last, rows, add_a)
                if j < 3:
                    @pl.when(place == 0)
                    def _(kind=kind):
                        move_mid(j, kind, (2, 3, 0)[j], 1).start()
                if j == 2:
                    @pl.when(place == 1)
                    def _(kind=kind):
                        move_mid(j, kind, 0, 0).start()

        def merge_mid(j):
            @pl.when(place == 1)
            def _():
                for kind in (1, 0):
                    move_mid(j, kind, 2 + j, 0).wait_recv()

                    def add_end(_, t, kind=kind):
                        mid[j, kind, t, :] = mid[j, kind, t, :] + mid_recv[2 + j, kind, t, :]

                    chunks(last, rows, add_end)
                    move_mid(j, kind, 1, 3 - j).start()

        def mid_total(kind, t):
            return mid[3, kind, t, :] + mid_recv[0, kind, t, :] + mid_recv[1, kind, t, :]

        def wait_mid(kind):
            for slot in range(2):
                move_mid(3, kind, slot, 2).wait_recv()

        mid_b_copy = remote(mid_b, mid_b_recv, mb_s, mb_r, dev_b)

        def mid_second():
            wait_mid(1)

            def add_mid(_, t):
                mid_b[t, :] = mid_total(1, t)

            chunks(last, rows, add_mid)
            mid_b_copy.start()

        b_copies = [remote(send_b.at[j], recv_b.at[j], b_s, pool.at[26 + j], dev_b) for j in range(4)]
        z_copies = [remote(send_z.at[j], recv_z.at[z], z_s, z_r, dev_z(order[j])) for j in range(3)]

        def do_b(j):
            move_a_sum(j * 2, 1).wait_recv()

            def add_a(s, _):
                send_b[j, s, :] = pair_sum(j * 4 + 2, s) + recv_a[j * 2, s, :]

            chunks(0, last, add_a)
            b_copies[j].start()

        def plane_total(j, s):
            return pair_sum(j * 4 + 3, s) + recv_a[j * 2 + 1, s, :] + recv_b[j, s, :]

        def do_z(j):
            move_a_sum(j * 2 + 1, 1).wait_recv()
            b_copies[j].wait_recv()

            def add_ab(s, _):
                send_z[j, s, :] = plane_total(j, s)

            if j < 3:
                chunks(0, last, add_ab)
                z_copies[j].start()

        do_mid(0)
        do_mid(1)
        wait_all(gv_line.at[pl.ds(0, 3)], vz_r)
        gv_half[...] = (((gv_line[0] + gv_line[1]) + gv_line[2]) + gv_line[3]) * inv_group
        vec_end = remote(gv_half, gv_other, ve_s, ve_r, dev_c)
        vec_end.start()
        do_mid(2)
        merge_mid(0)
        vec_end.wait_recv()
        gv_sum[pl.ds(pl.multiple_of(core * vstep, 8), vhalf), :] = gv_half[...]
        gv_sum[pl.ds(pl.multiple_of((1 - core) * vstep, 8), vhalf), :] = gv_other[...]
        vec_sq = jnp.sum(gv_sum[...] * gv_sum[...])
        do_b(0)
        merge_mid(1)
        do_b(1)
        do_mid(3)
        do_z(0)
        do_b(2)
        do_z(1)
        do_z(2)
        do_b(3)
        mid_second()
        wait_mid(0)
        mid_b_copy.wait_recv()

        def squares(size, total):
            def add(i, acc):
                g = total(pl.ds(pl.multiple_of(i * size, 8), size), i)
                return acc + jnp.sum((g * g).reshape(size // 8, 8, LANES), axis=0)

            return add

        mid_step = (rows - last) // STEPS
        last_step = last // STEPS

        def final_mid(t, i):
            g = (mid_total(0, t) + mid_b_recv[t, :]) * inv_group
            grad[pl.ds(pl.multiple_of(last + i * mid_step, 8), mid_step), :] = g
            return g

        def final_last(s, i):
            g = plane_total(3, s)
            for j in range(3):
                g = g + recv_z[order[j], s, :]
            g = g * inv_group
            grad[s, :] = g
            return g

        sq = lax.fori_loop(0, STEPS, squares(mid_step, final_mid), jnp.zeros((8, LANES), F32))
        do_z(3)
        wait_all(recv_z.at[pl.ds(0, 3)], z_r)
        sq = lax.fori_loop(0, STEPS, squares(last_step, final_last), sq)
        norm_rows[me] = jnp.sum(sq, axis=0, keepdims=True)

        for d in range(1, group):
            to = (me + d) % group
            remote(norm_rows.at[me], norm_rows.at[me], n_s, n_r, to).start()
        wait_all(state, load_sem.at[1])
        wait_all(vec_state, load_sem.at[2])
        wait_all(norm_rows.at[pl.ds(0, group - 1)], n_r)
        norm_sq = jnp.sum(norm_rows[...]) + vec_sq
        norm = jnp.sqrt(jnp.full((8, LANES), norm_sq, F32))
        scale = jnp.minimum(1.0, MAX_NORM / (norm + NORM_EPS))[0:1, :]
        lr = lr_ref[0]

        def adam(start, size):
            s = pl.ds(start, size)
            new_p, new_m, new_v = adam_update(grad[s, :] * scale, state[0, s, :], state[1, s, :], state[2, s, :], lr, WEIGHT_DECAY)
            p_out[s, :] = new_p
            m_out[s, :] = new_m
            v_out[s, :] = new_v
            pb_out[me, s, :] = new_p.astype(BF16)

        def move(idx, p, s_sem, r_sem, dev):
            ref = pb_out.at[idx, parts[p]]
            return remote(ref, ref, s_sem, r_sem, dev)

        def move_line(r, p, kind, to):
            zq = plane_at(r)
            return move(piece(zq, False, kind == 1), p, gz_s.at[kind], pool.at[zq * 4 + p + kind], dev_z(plane_at(to)))

        def move_b(zq, flip, p):
            return move(piece(zq, False, flip), p, gb_s.at[p // 2], pool.at[24 if p == 2 else 16 + zq * 2 + p], dev_b)

        def move_a(zq, kind, p):
            return move(piece(zq, False, kind == 1), p, ga_s, pool.at[25 + zq * 2 + kind], dev_a)

        def move_c(zq, kind, p):
            return move(piece(zq, False, kind == 1), p, gc_s, gc_r, dev_c)

        def pass_on(r, kind, p):
            zq = plane_at(r)
            move_a(zq, kind, p).start()
            move_c(zq, kind, p).start()

        def gather(own_place, to, plan):
            def from_line(r, p, kind=0):
                move_line(r, p, kind, r).wait_recv()
                if own_place == 1 and r > 1:
                    move_line(r, p, kind, 0).start()
                if p < 2:
                    move_b(plane_at(r), False, p).start()
                pass_on(r, kind, p)

            def from_b(r, p):
                move_b(plane_at(r), True, p).wait_recv()
                if p == 2:
                    for other in to:
                        move_line(r, p, 1, other).start()
                pass_on(r, 1, p)

            def from_a(r, kind):
                zq = plane_at(r)
                ref = pb_out.at[piece(zq, True, kind == 1)]
                wait_all(ref, pool.at[25 + zq * 2 + kind])
                remote(ref, ref, gc_s, gc_r, dev_c).start()

            for p in range(3):
                for start, size in steps[p]:
                    adam(start, size)
                for other in to:
                    move_line(own_place, p, 0, other).start()
                move_b(plane_at(own_place), False, p).start()
                pass_on(own_place, 0, p)
            pv_new, mv_new, vv_new = adam_update(gv_sum[...] * scale, vec_state[0], vec_state[1], vec_state[2], lr, 0.0)
            pv_out[...] = pv_new
            mv_out[...] = mv_new
            vv_out[...] = vv_new
            takers = {"z": from_line, "b": from_b, "a": from_a}
            for item in plan:
                takers[item[0]](*[int(digit) for digit in item[1:]])
            wait_all(pb_out.at[pl.ds(0, group // 2)], gc_r)
            lines = 2 + 2 * own_place
            wait_all(pb_out.at[pl.ds(0, lines)], gz_s.at[0])
            wait_all(pb_out.at[pl.ds(0, lines), parts[2]], gz_s.at[1])

        @pl.when(place == 0)
        def _():
            gather(0, (1, 2), END_PLAN)

        @pl.when(place == 1)
        def _():
            gather(1, (2, 0), INNER_PLAN)

        for ref, sem in ((pair, pair_s), (gv_pair, vc_s), (gv_plane.at[pl.ds(0, 3)], vp_s),
                         (gv_line.at[pl.ds(0, 3)], vz_s), (gv_half, ve_s), (send_a, a_s), (send_b, b_s),
                         (send_z.at[pl.ds(0, 3)], z_s), (mid.at[pl.ds(0, 3)], m_s), (mid_b, mb_s), (norm_rows.at[pl.ds(0, group - 1)], n_s),
                         (pb_out.at[pl.ds(0, 4), pl.ds(0, late)], gb_s.at[0]),
                         (pb_out.at[0, parts[2]], gb_s.at[1]), (pb_out.at[pl.ds(0, 8)], ga_s),
                         (pb_out.at[pl.ds(0, group // 2)], gc_s)):
            wait_all(ref, sem)

    vmem = pl.BlockSpec(memory_space=pltpu.VMEM)
    hbm = pl.BlockSpec(memory_space=pltpu.HBM)
    sem = sems = pltpu.SemaphoreType.DMA
    return pl.pallas_call(
        body,
        name="adam_step",
        out_shape=(
            jax.ShapeDtypeStruct((group, rows, LANES), BF16),
            *[jax.ShapeDtypeStruct((rows, LANES), F32)] * 3,
            *[jax.ShapeDtypeStruct((vrows, LANES), F32)] * 3,
        ),
        in_specs=[hbm] * 8 + [pl.BlockSpec(memory_space=pltpu.SMEM)],
        out_specs=(vmem,) * 7,
        scratch_shapes=[
            pltpu.VMEM((16, rows, 1, LANES), BF16),
            pltpu.VMEM((16, rows, 1, LANES), BF16),
            *[pltpu.VMEM((8, rows, LANES), F32)] * 2,
            *[pltpu.VMEM((4, last, LANES), F32)] * 4,
            *[pltpu.VMEM((4, 2, rows - last, LANES), F32)] * 2,
            *[pltpu.VMEM((rows - last, LANES), F32)] * 2,
            pltpu.VMEM((rows, LANES), F32),
            pltpu.VMEM((group, 1, LANES), F32),
            pltpu.VMEM((3, rows, LANES), F32),
            *[pltpu.VMEM((vhalf, 1, LANES), BF16)] * 2,
            *[pltpu.VMEM((4, vhalf, LANES), F32)] * 2,
            *[pltpu.VMEM((vhalf, LANES), F32)] * 2,
            pltpu.VMEM((vrows, LANES), F32),
            pltpu.VMEM((3, vrows, LANES), F32),
            sems((3,)), sems((38,)), *[sem] * 8, sems((3,)),
            *[sem] * 10,
            sems((2,)), sems((2,)), sem, sem, sem,
        ],
        compiler_params=pltpu.CompilerParams(
            collective_id=0, has_side_effects=True, vmem_limit_bytes=32 * 1024 * 1024),
    )


def store_kernel(shapes):
    def body(*refs):
        n = len(shapes)
        ins, outs, sem = refs[:n], refs[n:2 * n], refs[2 * n]
        copies = [pltpu.make_async_copy(ins[i], outs[i], sem.at[i]) for i in range(n)]
        for copy in copies:
            copy.start()
        for copy in copies:
            copy.wait()

    return pl.pallas_call(
        body,
        name="store_results",
        out_shape=tuple(shapes),
        in_specs=[pl.BlockSpec(memory_space=pltpu.VMEM)] * len(shapes),
        out_specs=tuple([pl.BlockSpec(memory_space=pltpu.HBM)] * len(shapes)),
        scratch_shapes=[pltpu.SemaphoreType.DMA((len(shapes),))],
        compiler_params=pltpu.CompilerParams(vmem_limit_bytes=16 * 1024 * 1024),
    )


def solution(mesh):
    axis_name = mesh.axis_names[0]
    group = mesh.shape[axis_name]

    def local_step(g_mat, g_vec, p_mat, m_mat, v_mat, p_vec, m_vec, v_vec, learn_rate):
        rows = p_mat.shape[0] // LANES
        vrows = p_vec.shape[0] // LANES
        operands = [
            g_mat.reshape(group * rows, 1, LANES), g_vec.reshape(vrows, 1, LANES),
            *[t.reshape(rows, LANES) for t in (p_mat, m_mat, v_mat)],
            *[t.reshape(vrows, LANES) for t in (p_vec, m_vec, v_vec)]]
        operands = [pltpu.with_memory_space_constraint(t, pltpu.HBM) for t in operands]
        results = step_kernel(group, rows, vrows, axis_name)(*operands, learn_rate.reshape(1))
        results = store_kernel([jax.ShapeDtypeStruct(r.shape, r.dtype) for r in results])(*results)
        full, new_p, new_m, new_v, new_pv, new_mv, new_vv = results
        return (*[t.reshape(-1) for t in (new_p, new_m, new_v, new_pv, new_mv, new_vv)], full.reshape(-1))

    return jax.shard_map(
        local_step,
        mesh=mesh,
        in_specs=(P(axis_name, None), P(axis_name, None), P(axis_name), P(axis_name), P(axis_name), P(), P(), P(), P()),
        out_specs=(P(axis_name), P(axis_name), P(axis_name), P(), P(), P(), P()),
        check_vma=False,
    )
```

```python
import jax
import jax.numpy as jnp
from jax import lax
from jax.experimental import pallas as pl
from jax.experimental.pallas import tpu as pltpu
from jax.sharding import PartitionSpec as P

STEP = 10
ADAM_BETA1 = 0.9
ADAM_BETA2 = 0.98
ADAM_EPS = 1e-8
WEIGHT_DECAY = 0.01
MAX_NORM = 1.0
NORM_EPS = 1e-6
BIAS_ONE = 1.0 - ADAM_BETA1 ** STEP
BIAS_TWO = 1.0 - ADAM_BETA2 ** STEP

MESH = pl.DeviceIdType.MESH
F32 = jnp.float32
BF16 = jnp.bfloat16
LANES = 128
STEPS = 3


END_PLAN = [
    "z100", "b00", "z110", "b01", "b02", "z120", "a00", "z200", "b10", "z210", "b11", "z220",
    "z121", "a01", "a10", "z300", "b20", "z310", "b21", "z320", "z221", "a11", "a20", "z321",
    "b30", "b31", "a21", "a30", "a31",
]
INNER_PLAN = [
    "z200", "z000", "b10", "z210", "z010", "b11", "b12", "z220", "z020", "a10", "z300", "b20",
    "b00", "z310", "b21", "b01", "z320", "z221", "z021", "a11", "a20", "a00", "z321", "b30",
    "b31", "a21", "a01", "a30", "a31",
]


def adam_update(grad_vals, param_vals, moment_one, moment_two, learn_rate, decay_rate):
    new_one = ADAM_BETA1 * moment_one + (1.0 - ADAM_BETA1) * grad_vals
    new_two = ADAM_BETA2 * moment_two + (1.0 - ADAM_BETA2) * grad_vals * grad_vals
    direction = (new_one / BIAS_ONE) / (jnp.sqrt(new_two / BIAS_TWO) + ADAM_EPS)
    return param_vals - learn_rate * (direction + decay_rate * param_vals), new_one, new_two


def step_kernel(group, rows, vrows, axis_name):
    inv_group = 1.0 / group
    vstep = vrows // 16 * 8
    vhalf = vrows - vstep
    last = rows * 3 // 5 // (8 * STEPS) * (8 * STEPS)
    early, late = 176, 352
    bounds = (0, early, late, rows)
    parts = [pl.ds(lo, hi - lo) for lo, hi in zip(bounds, bounds[1:])]
    steps = []
    for lo, hi in zip(bounds, bounds[1:]):
        half = lo + ((hi - lo) // 2 + 15) // 16 * 16
        steps.append([(lo, half - lo), (half, hi - half)])

    def body(g_ref, gv_ref, p_ref, m_ref, v_ref, pv_ref, mv_ref, vv_ref, lr_ref,
             pb_out, p_out, m_out, v_out, pv_out, mv_out, vv_out,
             own, pair, send_a, recv_a, send_b, recv_b, send_z, recv_z, mid, mid_recv, mid_b, mid_b_recv, grad, norm_rows,
             state, gv_own, gv_pair, gv_plane, gv_line, gv_half, gv_other, gv_sum, vec_state,
             own_sem, pool, pair_s, a_s, b_s, z_s, z_r, m_s, mb_s, mb_r, load_sem,
             vc_s, vc_r, vp_s, vp_r, vz_s, vz_r, ve_s, ve_r, n_s, n_r):
        me = lax.axis_index(axis_name)
        core = me % 2
        x = (me // 2) % 2
        y = (me // 4) % 2
        z = me // 8
        str_a = 2 + 2 * core
        str_b = 4 - 2 * core
        a = x + core * (y - x)
        b = y + core * (x - y)
        dev_c = me + 1 - 2 * core
        dev_a = me + (1 - 2 * a) * str_a
        dev_b = me + (1 - 2 * b) * str_b
        dev_x = me + (1 - 2 * x) * 2
        dev_y = me + (1 - 2 * y) * 4
        spot = y * 2 + x
        high = z // 2
        order = [3 - 3 * high, 2 - high, 1 - z + 4 * high, z]

        place = z + high * (3 - 2 * z)

        def plane_at(r):
            return r + high * (3 - 2 * r)

        def dev_z(zq):
            return me + (zq - z) * 8

        def piece(zq, flip_a, flip_b):
            aq = 1 - a if flip_a else a
            bq = 1 - b if flip_b else b
            return zq * 8 + aq * str_a + bq * str_b + core

        def partner_piece(zq, flip_a, flip_b):
            aq = 1 - b if flip_a else b
            bq = 1 - a if flip_b else a
            return zq * 8 + aq * str_b + bq * str_a + 1 - core

        def remote(src, dst, s_sem, r_sem, dev):
            return pltpu.make_async_remote_copy(
                src_ref=src, dst_ref=dst, send_sem=s_sem, recv_sem=r_sem, device_id=(dev,), device_id_type=MESH)

        flips = [(True, True), (True, False), (False, True), (False, False)]
        own_copies = []
        for j in range(4):
            for k, (fa, fb) in enumerate(flips):
                src = g_ref.at[pl.ds(piece(order[j], fa, fb) * rows, rows)]
                group_of = 0 if j + k == 0 else 1 + k // 2
                own_copies.append(pltpu.make_async_copy(src, own.at[j * 4 + k], own_sem.at[group_of]))
        use_order = [j * 4 + k for ks in ((0, 1), (2, 3)) for j in range(4) for k in ks]
        for i in use_order[:4]:
            own_copies[i].start()
        vec_load = pltpu.make_async_copy(gv_ref.at[pl.ds(core * vstep, vhalf)], gv_own, load_sem.at[0])
        vec_load.start()

        def wait_all(ref, sem):
            remote(ref, ref, sem, sem, dev_c).wait_recv()

        barrier = pltpu.get_barrier_semaphore()
        plane = [dev_x, dev_y, dev_x + dev_y - me]
        partners = [dev_c] + plane + [dev_z(order[j]) for j in range(3)]
        for partner in partners:
            pl.semaphore_signal(barrier, inc=1, device_id=(partner,), device_id_type=MESH)
        pl.semaphore_wait(barrier, len(partners))

        pair_copies = []
        for j in range(4):
            for k, (fa, fb) in enumerate(flips):
                src = g_ref.at[pl.ds(partner_piece(order[j], fa, fb) * rows, rows)]
                arrival = pool.at[j * 2 + k if k < 2 else 8 + j // 2]
                pair_copies.append(remote(src, pair.at[j * 4 + k], pair_s, arrival, dev_c))
        vec_pair = remote(gv_ref.at[pl.ds((1 - core) * vstep, vhalf)], gv_pair, vc_s, vc_r, dev_c)
        src = g_ref.at[pl.ds(partner_piece(order[0], True, True) * rows + last, rows - last)]
        pair_head = remote(src, pair.at[0, pl.ds(last, rows - last)], pair_s, pool.at[0], dev_c)
        src = g_ref.at[pl.ds(partner_piece(order[0], True, True) * rows, last)]
        pair_rest = remote(src, pair.at[0, pl.ds(0, last)], pair_s, pool.at[38], dev_c)
        pair_head.start()
        for n, i in enumerate(use_order):
            if i > 0:
                pair_copies[i].start()
            if n == 1:
                vec_pair.start()
                pair_rest.start()
            if n >= 4:
                own_copies[i].start()
        for i, ref in enumerate((p_ref, m_ref, v_ref)):
            pltpu.make_async_copy(ref, state.at[i], load_sem.at[1]).start()
        for i, ref in enumerate((pv_ref, mv_ref, vv_ref)):
            pltpu.make_async_copy(ref, vec_state.at[i], load_sem.at[2]).start()

        def chunks(start, stop, fn):
            size = (stop - start) // STEPS

            @pl.loop(0, STEPS)
            def _(i):
                fn(pl.ds(pl.multiple_of(start + i * size, 8), size), pl.ds(pl.multiple_of(i * size, 8), size))

        def pair_sum(i, s):
            return own[i, s, 0, :].astype(F32) + pair[i, s, 0, :].astype(F32)

        def move_a_sum(i, first):
            part = pl.ds(0, last) if first else pl.ds(last, rows - last)
            return remote(send_a.at[i, part], recv_a.at[i, part], a_s, pool.at[10 + i * 2 + first], dev_a)

        loaded = set()

        def do_a(i, first):
            slot = (i // 2) * 4 + i % 2
            if slot not in loaded:
                take(slot)
            if slot == 0 and first:
                pair_rest.wait_recv()

            def add_pair(s, _):
                send_a[i, s, :] = pair_sum(slot, s)

            chunks(*((0, last) if first else (last, rows)), add_pair)
            move_a_sum(i, first).start()

        def take(slot):
            loaded.add(slot)
            if slot == 0:
                own_copies[0].wait()
                pair_head.wait_recv()
            else:
                if len(loaded) == 2:
                    wait_all(own.at[pl.ds(0, 7)], own_sem.at[1])
                pair_copies[slot].wait_recv()

        do_a(0, 0)

        vec_load.wait()
        vec_pair.wait_recv()
        gv_plane[spot] = gv_own[:, 0, :].astype(F32) + gv_pair[:, 0, :].astype(F32)
        vec_plane = [remote(gv_plane.at[spot], gv_plane.at[spot], vp_s, vp_r, dev) for dev in plane]
        for copy in vec_plane:
            copy.start()

        for i, first in [(1, 0), (2, 0), (3, 0), (4, 0), (5, 0), (0, 1), (2, 1), (6, 0), (7, 0), (1, 1), (4, 1), (3, 1), (5, 1), (6, 1), (7, 1)]:
            do_a(i, first)

        wait_all(gv_plane.at[pl.ds(0, 3)], vp_r)
        gv_line[z] = ((gv_plane[0] + gv_plane[1]) + gv_plane[2]) + gv_plane[3]
        vec_line = [remote(gv_line.at[z], gv_line.at[z], vz_s, vz_r, dev_z(order[j])) for j in range(3)]
        for copy in vec_line:
            copy.start()

        def move_mid(j, kind, slot, r):
            at = slot * 2 + kind
            return remote(mid.at[j, kind], mid_recv.at[slot, kind], m_s, pool.at[30 + at], dev_z(plane_at(r)))

        def do_mid(j):
            for kind in (1, 0):
                slot = j * 4 + 3 - kind
                i = j * 2 + 1 - kind
                if j == 0 and kind == 1:
                    wait_all(own.at[pl.ds(0, 8)], own_sem.at[2])
                if j % 2 == 0 and kind == 1:
                    wait_all(pair.at[pl.ds(0, 4)], pool.at[8 + j // 2])
                move_a_sum(i, 0).wait_recv()

                def add_a(s, t, kind=kind, slot=slot, i=i):
                    mid[j, kind, t, :] = pair_sum(slot, s) + recv_a[i, s, :]

                chunks(last, rows, add_a)
                if j < 3:
                    @pl.when(place == 0)
                    def _(kind=kind):
                        move_mid(j, kind, (2, 3, 0)[j], 1).start()
                if j == 2:
                    @pl.when(place == 1)
                    def _(kind=kind):
                        move_mid(j, kind, 0, 0).start()

        def merge_mid(j):
            @pl.when(place == 1)
            def _():
                for kind in (1, 0):
                    move_mid(j, kind, 2 + j, 0).wait_recv()

                    def add_end(_, t, kind=kind):
                        mid[j, kind, t, :] = mid[j, kind, t, :] + mid_recv[2 + j, kind, t, :]

                    chunks(last, rows, add_end)
                    move_mid(j, kind, 1, 3 - j).start()

        def mid_total(kind, t):
            return mid[3, kind, t, :] + mid_recv[0, kind, t, :] + mid_recv[1, kind, t, :]

        def wait_mid(kind):
            for slot in range(2):
                move_mid(3, kind, slot, 2).wait_recv()

        mid_b_copy = remote(mid_b, mid_b_recv, mb_s, mb_r, dev_b)

        def mid_second():
            wait_mid(1)

            def add_mid(_, t):
                mid_b[t, :] = mid_total(1, t)

            chunks(last, rows, add_mid)
            mid_b_copy.start()

        b_copies = [remote(send_b.at[j], recv_b.at[j], b_s, pool.at[26 + j], dev_b) for j in range(4)]
        z_copies = [remote(send_z.at[j], recv_z.at[z], z_s, z_r, dev_z(order[j])) for j in range(3)]

        def do_b(j):
            move_a_sum(j * 2, 1).wait_recv()

            def add_a(s, _):
                send_b[j, s, :] = pair_sum(j * 4 + 2, s) + recv_a[j * 2, s, :]

            chunks(0, last, add_a)
            b_copies[j].start()

        def plane_total(j, s):
            return pair_sum(j * 4 + 3, s) + recv_a[j * 2 + 1, s, :] + recv_b[j, s, :]

        def do_z(j):
            move_a_sum(j * 2 + 1, 1).wait_recv()
            b_copies[j].wait_recv()

            def add_ab(s, _):
                send_z[j, s, :] = plane_total(j, s)

            if j < 3:
                chunks(0, last, add_ab)
                z_copies[j].start()

        do_mid(0)
        do_mid(1)
        wait_all(gv_line.at[pl.ds(0, 3)], vz_r)
        gv_half[...] = (((gv_line[0] + gv_line[1]) + gv_line[2]) + gv_line[3]) * inv_group
        vec_end = remote(gv_half, gv_other, ve_s, ve_r, dev_c)
        vec_end.start()
        do_mid(2)
        merge_mid(0)
        vec_end.wait_recv()
        gv_sum[pl.ds(pl.multiple_of(core * vstep, 8), vhalf), :] = gv_half[...]
        gv_sum[pl.ds(pl.multiple_of((1 - core) * vstep, 8), vhalf), :] = gv_other[...]
        vec_sq = jnp.sum(gv_sum[...] * gv_sum[...])
        do_b(0)
        merge_mid(1)
        do_b(1)
        do_mid(3)
        do_z(0)
        do_b(2)
        do_z(1)
        do_z(2)
        do_b(3)
        mid_second()
        def squares(size, total):
            def add(i, acc):
                g = total(pl.ds(pl.multiple_of(i * size, 8), size), i)
                return acc + jnp.sum((g * g).reshape(size // 8, 8, LANES), axis=0)

            return add

        mid_step = (rows - last) // STEPS
        last_step = last // STEPS

        def final_mid(t, i):
            g = (mid_total(0, t) + mid_b_recv[t, :]) * inv_group
            grad[pl.ds(pl.multiple_of(last + i * mid_step, 8), mid_step), :] = g
            return g

        def last_plane(s, _):
            send_z[3, s, :] = plane_total(3, s)

        def final_last(s, i):
            g = send_z[3, s, :]
            for j in range(3):
                g = g + recv_z[order[j], s, :]
            g = g * inv_group
            grad[s, :] = g
            return g

        do_z(3)
        chunks(0, last, last_plane)
        wait_mid(0)
        mid_b_copy.wait_recv()
        sq = lax.fori_loop(0, STEPS, squares(mid_step, final_mid), jnp.zeros((8, LANES), F32))
        wait_all(recv_z.at[pl.ds(0, 3)], z_r)
        sq = lax.fori_loop(0, STEPS, squares(last_step, final_last), sq)
        norm_rows[me] = jnp.sum(sq, axis=0, keepdims=True)

        for d in range(1, group):
            to = (me + d) % group
            remote(norm_rows.at[me], norm_rows.at[me], n_s, n_r, to).start()
        wait_all(state, load_sem.at[1])
        wait_all(vec_state, load_sem.at[2])
        for ref, sem in ((pair, pair_s), (gv_pair, vc_s), (gv_plane.at[pl.ds(0, 3)], vp_s),
                         (gv_line.at[pl.ds(0, 3)], vz_s), (gv_half, ve_s), (send_a, a_s), (send_b, b_s),
                         (send_z.at[pl.ds(0, 3)], z_s), (mid.at[pl.ds(0, 3)], m_s), (mid_b, mb_s),
                         (norm_rows.at[pl.ds(0, group - 1)], n_s)):
            wait_all(ref, sem)
        wait_all(norm_rows.at[pl.ds(0, group - 1)], n_r)
        norm_sq = jnp.sum(norm_rows[...]) + vec_sq
        norm = jnp.sqrt(jnp.full((8, LANES), norm_sq, F32))
        scale = jnp.minimum(1.0, MAX_NORM / (norm + NORM_EPS))[0:1, :]
        lr = lr_ref[0]

        def adam(start, size):
            s = pl.ds(start, size)
            new_p, new_m, new_v = adam_update(grad[s, :] * scale, state[0, s, :], state[1, s, :], state[2, s, :], lr, WEIGHT_DECAY)
            p_out[s, :] = new_p
            m_out[s, :] = new_m
            v_out[s, :] = new_v
            pb_out[me, s, :] = new_p.astype(BF16)

        def move(idx, p, s_sem, r_sem, dev):
            ref = pb_out.at[idx, parts[p]]
            return remote(ref, ref, s_sem, r_sem, dev)

        def move_line(r, p, kind, to):
            zq = plane_at(r)
            return move(piece(zq, False, kind == 1), p, (m_s if kind else z_s), pool.at[zq * 4 + p + kind], dev_z(plane_at(to)))

        def move_b(zq, flip, p):
            return move(piece(zq, False, flip), p, (mb_s if p == 2 else b_s), pool.at[24 if p == 2 else 16 + zq * 2 + p], dev_b)

        def move_a(zq, kind, p):
            return move(piece(zq, False, kind == 1), p, a_s, pool.at[25 + zq * 2 + kind], dev_a)

        def move_c(zq, kind, p):
            return move(piece(zq, False, kind == 1), p, pair_s, z_r, dev_c)

        def pass_on(r, kind, p):
            zq = plane_at(r)
            move_a(zq, kind, p).start()
            move_c(zq, kind, p).start()

        def gather(own_place, to, plan):
            def from_line(r, p, kind=0):
                move_line(r, p, kind, r).wait_recv()
                if own_place == 1 and r > 1:
                    move_line(r, p, kind, 0).start()
                if p < 2:
                    move_b(plane_at(r), False, p).start()
                pass_on(r, kind, p)

            def from_b(r, p):
                move_b(plane_at(r), True, p).wait_recv()
                if p == 2:
                    for other in to:
                        move_line(r, p, 1, other).start()
                pass_on(r, 1, p)

            def from_a(r, kind):
                zq = plane_at(r)
                ref = pb_out.at[piece(zq, True, kind == 1)]
                wait_all(ref, pool.at[25 + zq * 2 + kind])
                remote(ref, ref, pair_s, z_r, dev_c).start()

            for p in range(3):
                for start, size in steps[p]:
                    adam(start, size)
                for other in to:
                    move_line(own_place, p, 0, other).start()
                move_b(plane_at(own_place), False, p).start()
                pass_on(own_place, 0, p)
            pv_new, mv_new, vv_new = adam_update(gv_sum[...] * scale, vec_state[0], vec_state[1], vec_state[2], lr, 0.0)
            pv_out[...] = pv_new
            mv_out[...] = mv_new
            vv_out[...] = vv_new
            takers = {"z": from_line, "b": from_b, "a": from_a}
            for item in plan:
                takers[item[0]](*[int(digit) for digit in item[1:]])
            wait_all(pb_out.at[pl.ds(0, group // 2)], z_r)
            lines = 2 + 2 * own_place
            wait_all(pb_out.at[pl.ds(0, lines)], z_s)
            wait_all(pb_out.at[pl.ds(0, lines), parts[2]], m_s)

        @pl.when(place == 0)
        def _():
            gather(0, (1, 2), END_PLAN)

        @pl.when(place == 1)
        def _():
            gather(1, (2, 0), INNER_PLAN)

        for ref, sem in ((pb_out.at[pl.ds(0, 4), pl.ds(0, late)], b_s), (pb_out.at[0, parts[2]], mb_s),
                         (pb_out.at[pl.ds(0, 8)], a_s), (pb_out.at[pl.ds(0, group // 2)], pair_s)):
            wait_all(ref, sem)

    vmem = pl.BlockSpec(memory_space=pltpu.VMEM)
    hbm = pl.BlockSpec(memory_space=pltpu.HBM)
    sem = sems = pltpu.SemaphoreType.DMA
    return pl.pallas_call(
        body,
        name="adam_step",
        out_shape=(
            jax.ShapeDtypeStruct((group, rows, LANES), BF16),
            *[jax.ShapeDtypeStruct((rows, LANES), F32)] * 3,
            *[jax.ShapeDtypeStruct((vrows, LANES), F32)] * 3,
        ),
        in_specs=[hbm] * 8 + [pl.BlockSpec(memory_space=pltpu.SMEM)],
        out_specs=(vmem,) * 7,
        scratch_shapes=[
            pltpu.VMEM((16, rows, 1, LANES), BF16),
            pltpu.VMEM((16, rows, 1, LANES), BF16),
            *[pltpu.VMEM((8, rows, LANES), F32)] * 2,
            *[pltpu.VMEM((4, last, LANES), F32)] * 4,
            *[pltpu.VMEM((4, 2, rows - last, LANES), F32)] * 2,
            *[pltpu.VMEM((rows - last, LANES), F32)] * 2,
            pltpu.VMEM((rows, LANES), F32),
            pltpu.VMEM((group, 1, LANES), F32),
            pltpu.VMEM((3, rows, LANES), F32),
            *[pltpu.VMEM((vhalf, 1, LANES), BF16)] * 2,
            *[pltpu.VMEM((4, vhalf, LANES), F32)] * 2,
            *[pltpu.VMEM((vhalf, LANES), F32)] * 2,
            pltpu.VMEM((vrows, LANES), F32),
            pltpu.VMEM((3, vrows, LANES), F32),
            sems((3,)), sems((39,)), *[sem] * 8, sems((3,)),
            *[sem] * 10,
        ],
        compiler_params=pltpu.CompilerParams(
            collective_id=0, has_side_effects=True, vmem_limit_bytes=32 * 1024 * 1024),
    )


def store_kernel(shapes):
    def body(*refs):
        n = len(shapes)
        ins, outs, sem = refs[:n], refs[n:2 * n], refs[2 * n]
        copies = [pltpu.make_async_copy(ins[i], outs[i], sem.at[i]) for i in range(n)]
        for copy in copies:
            copy.start()
        for copy in copies:
            copy.wait()

    return pl.pallas_call(
        body,
        name="store_results",
        out_shape=tuple(shapes),
        in_specs=[pl.BlockSpec(memory_space=pltpu.VMEM)] * len(shapes),
        out_specs=tuple([pl.BlockSpec(memory_space=pltpu.HBM)] * len(shapes)),
        scratch_shapes=[pltpu.SemaphoreType.DMA((len(shapes),))],
        compiler_params=pltpu.CompilerParams(vmem_limit_bytes=16 * 1024 * 1024),
    )


def solution(mesh):
    axis_name = mesh.axis_names[0]
    group = mesh.shape[axis_name]

    def local_step(g_mat, g_vec, p_mat, m_mat, v_mat, p_vec, m_vec, v_vec, learn_rate):
        rows = p_mat.shape[0] // LANES
        vrows = p_vec.shape[0] // LANES
        operands = [
            g_mat.reshape(group * rows, 1, LANES), g_vec.reshape(vrows, 1, LANES),
            *[t.reshape(rows, LANES) for t in (p_mat, m_mat, v_mat)],
            *[t.reshape(vrows, LANES) for t in (p_vec, m_vec, v_vec)]]
        operands = [pltpu.with_memory_space_constraint(t, pltpu.HBM) for t in operands]
        results = step_kernel(group, rows, vrows, axis_name)(*operands, learn_rate.reshape(1))
        results = store_kernel([jax.ShapeDtypeStruct(r.shape, r.dtype) for r in results])(*results)
        full, new_p, new_m, new_v, new_pv, new_mv, new_vv = results
        return (*[t.reshape(-1) for t in (new_p, new_m, new_v, new_pv, new_mv, new_vv)], full.reshape(-1))

    return jax.shard_map(
        local_step,
        mesh=mesh,
        in_specs=(P(axis_name, None), P(axis_name, None), P(axis_name), P(axis_name), P(axis_name), P(), P(), P(), P()),
        out_specs=(P(axis_name), P(axis_name), P(axis_name), P(), P(), P(), P()),
        check_vma=False,
    )
```

```python
import jax
import jax.numpy as jnp
from jax import lax
from jax.experimental import pallas as pl
from jax.experimental.pallas import tpu as pltpu
from jax.sharding import PartitionSpec as P

STEP = 10
ADAM_BETA1 = 0.9
ADAM_BETA2 = 0.98
ADAM_EPS = 1e-8
WEIGHT_DECAY = 0.01
MAX_NORM = 1.0
NORM_EPS = 1e-6
BIAS_ONE = 1.0 - ADAM_BETA1 ** STEP
BIAS_TWO = 1.0 - ADAM_BETA2 ** STEP

MESH = pl.DeviceIdType.MESH
F32 = jnp.float32
BF16 = jnp.bfloat16
LANES = 128
STEPS = 3


END_PLAN = [
    "b00", "z100", "z110", "b01", "b02", "b10", "z120", "z200", "z210", "a00", "b11", "z220",
    "z121", "b20", "a01", "a10", "z300", "z310", "b21", "z320", "a11", "z221", "z321", "b30",
    "b31", "a30", "a21", "a20", "a31",
]
INNER_PLAN = [
    "z200", "z000", "z210", "a10", "b11", "b12", "b10", "z010", "z220", "z020", "z300", "b20",
    "b00", "b21", "z021", "z310", "b01", "z320", "z221", "a11", "a20", "a00", "z321", "a01",
    "b30", "b31", "a31", "a30", "a21",
]


def adam_update(grad_vals, param_vals, moment_one, moment_two, learn_rate, decay_rate):
    new_one = ADAM_BETA1 * moment_one + (1.0 - ADAM_BETA1) * grad_vals
    new_two = ADAM_BETA2 * moment_two + (1.0 - ADAM_BETA2) * grad_vals * grad_vals
    direction = (new_one / BIAS_ONE) / (jnp.sqrt(new_two / BIAS_TWO) + ADAM_EPS)
    return param_vals - learn_rate * (direction + decay_rate * param_vals), new_one, new_two


def step_kernel(group, rows, vrows, axis_name):
    inv_group = 1.0 / group
    vstep = vrows // 16 * 8
    vhalf = vrows - vstep
    qstep = vhalf // 32 * 8
    quarter = vhalf - 3 * qstep
    last = rows * 16 // 25 // (8 * STEPS) * (8 * STEPS)
    early, late = 192, 352
    bounds = (0, early, late, rows)
    parts = [pl.ds(lo, hi - lo) for lo, hi in zip(bounds, bounds[1:])]
    steps = []
    for lo, hi in zip(bounds, bounds[1:]):
        half = lo + ((hi - lo) // 2 + 15) // 16 * 16
        steps.append([(lo, half - lo), (half, hi - half)])

    def body(g_ref, gv_ref, p_ref, m_ref, v_ref, pv_ref, mv_ref, vv_ref, lr_ref,
             pb_out, p_out, m_out, v_out, pv_out, mv_out, vv_out,
             own, pair, send_a, recv_a, send_b, recv_b, send_z, recv_z, mid, mid_recv, mid_b, mid_b_recv, grad, norm_rows,
             state, gv_own, gv_pair, gv_sums, gv_quarter, gv_plane, gv_line, gv_half, gv_other, gv_sum, vec_state,
             own_sem, pool, pair_s, a_s, b_s, z_s, z_r, m_s, mb_s, mb_r, load_sem,
             vc_s, vc_r, vq_s, vq_r, vp_s, vp_r, vz_s, vz_r, ve_s, ve_r, n_s, n_r):
        me = lax.axis_index(axis_name)
        core = me % 2
        x = (me // 2) % 2
        y = (me // 4) % 2
        z = me // 8
        str_a = 2 + 2 * core
        str_b = 4 - 2 * core
        a = x + core * (y - x)
        b = y + core * (x - y)
        dev_c = me + 1 - 2 * core
        dev_a = me + (1 - 2 * a) * str_a
        dev_b = me + (1 - 2 * b) * str_b
        dev_x = me + (1 - 2 * x) * 2
        dev_y = me + (1 - 2 * y) * 4
        spot = y * 2 + x
        high = z // 2
        order = [3 - 3 * high, 2 - high, 1 - z + 4 * high, z]

        place = z + high * (3 - 2 * z)

        def plane_at(r):
            return r + high * (3 - 2 * r)

        def dev_z(zq):
            return me + (zq - z) * 8

        def piece(zq, flip_a, flip_b):
            aq = 1 - a if flip_a else a
            bq = 1 - b if flip_b else b
            return zq * 8 + aq * str_a + bq * str_b + core

        def partner_piece(zq, flip_a, flip_b):
            aq = 1 - b if flip_a else b
            bq = 1 - a if flip_b else a
            return zq * 8 + aq * str_b + bq * str_a + 1 - core

        def remote(src, dst, s_sem, r_sem, dev):
            return pltpu.make_async_remote_copy(
                src_ref=src, dst_ref=dst, send_sem=s_sem, recv_sem=r_sem, device_id=(dev,), device_id_type=MESH)

        flips = [(True, True), (True, False), (False, True), (False, False)]
        own_copies = []
        for j in range(4):
            for k, (fa, fb) in enumerate(flips):
                src = g_ref.at[pl.ds(piece(order[j], fa, fb) * rows, rows)]
                group_of = 0 if j + k == 0 else 1 + k // 2
                own_copies.append(pltpu.make_async_copy(src, own.at[j * 4 + k], own_sem.at[group_of]))
        use_order = [j * 4 + k for ks in ((0, 1), (2, 3)) for j in range(4) for k in ks]
        for i in use_order[:4]:
            own_copies[i].start()
        vec_load = pltpu.make_async_copy(gv_ref.at[pl.ds(core * vstep, vhalf)], gv_own, load_sem.at[0])
        vec_load.start()

        def wait_all(ref, sem):
            remote(ref, ref, sem, sem, dev_c).wait_recv()

        barrier = pltpu.get_barrier_semaphore()
        plane = [dev_x, dev_y, dev_x + dev_y - me]
        partners = [dev_c] + plane + [dev_z(order[j]) for j in range(3)]
        for partner in partners:
            pl.semaphore_signal(barrier, inc=1, device_id=(partner,), device_id_type=MESH)
        pl.semaphore_wait(barrier, len(partners))

        pair_copies = []
        for j in range(4):
            for k, (fa, fb) in enumerate(flips):
                src = g_ref.at[pl.ds(partner_piece(order[j], fa, fb) * rows, rows)]
                arrival = pool.at[j * 2 + k if k < 2 else 8 + j // 2]
                pair_copies.append(remote(src, pair.at[j * 4 + k], pair_s, arrival, dev_c))
        vec_pair = remote(gv_ref.at[pl.ds((1 - core) * vstep, vhalf)], gv_pair, vc_s, vc_r, dev_c)
        src = g_ref.at[pl.ds(partner_piece(order[0], True, True) * rows + last, rows - last)]
        pair_head = remote(src, pair.at[0, pl.ds(last, rows - last)], pair_s, pool.at[0], dev_c)
        src = g_ref.at[pl.ds(partner_piece(order[0], True, True) * rows, last)]
        pair_rest = remote(src, pair.at[0, pl.ds(0, last)], pair_s, pool.at[38], dev_c)
        pair_head.start()
        for n, i in enumerate(use_order):
            if i > 0:
                pair_copies[i].start()
            if n == 1:
                vec_pair.start()
                pair_rest.start()
            if n >= 4:
                own_copies[i].start()
        for i, ref in enumerate((p_ref, m_ref, v_ref)):
            pltpu.make_async_copy(ref, state.at[i], load_sem.at[1]).start()
        for i, ref in enumerate((pv_ref, mv_ref, vv_ref)):
            pltpu.make_async_copy(ref, vec_state.at[i], load_sem.at[2]).start()

        def chunks(start, stop, fn):
            size = (stop - start) // STEPS

            @pl.loop(0, STEPS)
            def _(i):
                fn(pl.ds(pl.multiple_of(start + i * size, 8), size), pl.ds(pl.multiple_of(i * size, 8), size))

        def pair_sum(i, s):
            return own[i, s, 0, :].astype(F32) + pair[i, s, 0, :].astype(F32)

        def move_a_sum(i, first):
            part = pl.ds(0, last) if first else pl.ds(last, rows - last)
            return remote(send_a.at[i, part], recv_a.at[i, part], a_s, pool.at[10 + i * 2 + first], dev_a)

        loaded = set()

        def do_a(i, first):
            slot = (i // 2) * 4 + i % 2
            if slot not in loaded:
                take(slot)
            if slot == 0 and first:
                pair_rest.wait_recv()

            def add_pair(s, _):
                send_a[i, s, :] = pair_sum(slot, s)

            chunks(*((0, last) if first else (last, rows)), add_pair)
            move_a_sum(i, first).start()

        def take(slot):
            loaded.add(slot)
            if slot == 0:
                own_copies[0].wait()
                pair_head.wait_recv()
            else:
                if len(loaded) == 2:
                    wait_all(own.at[pl.ds(0, 7)], own_sem.at[1])
                pair_copies[slot].wait_recv()

        do_a(0, 0)

        vec_load.wait()
        vec_pair.wait_recv()
        gv_sums[...] = gv_own[:, 0, :].astype(F32) + gv_pair[:, 0, :].astype(F32)

        def quarter_at(zq):
            return pl.ds(pl.multiple_of(zq * qstep, 8), quarter)

        for zq in order[:3]:
            remote(gv_sums.at[quarter_at(zq)], gv_quarter.at[z], vq_s, vq_r, dev_z(zq)).start()
        gv_quarter[z] = gv_sums[quarter_at(z), :]

        def in_order(parts):
            return ((parts[0] + parts[1]) + parts[2]) + parts[3]

        for i in range(1, 6):
            do_a(i, 0)

        wait_all(gv_quarter.at[pl.ds(0, 3)], vq_r)
        gv_plane[spot] = in_order(gv_quarter)
        for dev in plane:
            remote(gv_plane.at[spot], gv_plane.at[spot], vp_s, vp_r, dev).start()

        for i, first in [(0, 1), (2, 1), (7, 0), (1, 1), (6, 0), (4, 1), (3, 1), (5, 1), (6, 1), (7, 1)]:
            do_a(i, first)

        def move_mid(j, kind, slot, r):
            at = slot * 2 + kind
            return remote(mid.at[j, kind], mid_recv.at[slot, kind], m_s, pool.at[30 + at], dev_z(plane_at(r)))

        def do_mid(j):
            for kind in (1, 0):
                slot = j * 4 + 3 - kind
                i = j * 2 + 1 - kind
                if j == 0 and kind == 1:
                    wait_all(own.at[pl.ds(0, 8)], own_sem.at[2])
                if j % 2 == 0 and kind == 1:
                    wait_all(pair.at[pl.ds(0, 4)], pool.at[8 + j // 2])
                move_a_sum(i, 0).wait_recv()

                def add_a(s, t, kind=kind, slot=slot, i=i):
                    mid[j, kind, t, :] = pair_sum(slot, s) + recv_a[i, s, :]

                chunks(last, rows, add_a)
                if j < 3:
                    @pl.when(place == 0)
                    def _(kind=kind):
                        move_mid(j, kind, (2, 3, 0)[j], 1).start()
                if j == 2:
                    @pl.when(place == 1)
                    def _(kind=kind):
                        move_mid(j, kind, 0, 0).start()

        def merge_mid(j):
            @pl.when(place == 1)
            def _():
                for kind in (1, 0):
                    move_mid(j, kind, 2 + j, 0).wait_recv()

                    def add_end(_, t, kind=kind):
                        mid[j, kind, t, :] = mid[j, kind, t, :] + mid_recv[2 + j, kind, t, :]

                    chunks(last, rows, add_end)
                    move_mid(j, kind, 1, 3 - j).start()

        def mid_total(kind, t):
            return mid[3, kind, t, :] + mid_recv[0, kind, t, :] + mid_recv[1, kind, t, :]

        def wait_mid(kind):
            for slot in range(2):
                move_mid(3, kind, slot, 2).wait_recv()

        mid_b_copy = remote(mid_b, mid_b_recv, mb_s, mb_r, dev_b)

        def mid_second():
            wait_mid(1)

            def add_mid(_, t):
                mid_b[t, :] = mid_total(1, t)

            chunks(last, rows, add_mid)
            mid_b_copy.start()

        b_copies = [remote(send_b.at[j], recv_b.at[j], b_s, pool.at[26 + j], dev_b) for j in range(4)]
        z_copies = [remote(send_z.at[j], recv_z.at[z], z_s, z_r, dev_z(order[j])) for j in range(3)]

        def do_b(j):
            move_a_sum(j * 2, 1).wait_recv()

            def add_a(s, _):
                send_b[j, s, :] = pair_sum(j * 4 + 2, s) + recv_a[j * 2, s, :]

            chunks(0, last, add_a)
            b_copies[j].start()

        def plane_total(j, s):
            return pair_sum(j * 4 + 3, s) + recv_a[j * 2 + 1, s, :] + recv_b[j, s, :]

        def do_z(j):
            move_a_sum(j * 2 + 1, 1).wait_recv()
            b_copies[j].wait_recv()

            def add_ab(s, _):
                send_z[j, s, :] = plane_total(j, s)

            if j < 3:
                chunks(0, last, add_ab)
                z_copies[j].start()

        do_mid(0)
        do_mid(1)
        do_mid(2)
        merge_mid(0)
        do_b(0)
        wait_all(gv_plane.at[pl.ds(0, 3)], vp_r)
        gv_line[z] = in_order(gv_plane) * inv_group
        for zq in order[:3]:
            remote(gv_line.at[z], gv_line.at[z], vz_s, vz_r, dev_z(zq)).start()
        merge_mid(1)
        do_b(1)
        do_mid(3)
        do_z(0)
        do_b(2)
        do_z(1)
        wait_all(gv_line.at[pl.ds(0, 3)], vz_r)
        for zq in range(4):
            gv_half[pl.ds(zq * qstep, quarter), :] = gv_line[zq]
        vec_end = remote(gv_half, gv_other, ve_s, ve_r, dev_c)
        vec_end.start()
        vec_end.wait_recv()
        gv_sum[pl.ds(pl.multiple_of(core * vstep, 8), vhalf), :] = gv_half[...]
        gv_sum[pl.ds(pl.multiple_of((1 - core) * vstep, 8), vhalf), :] = gv_other[...]
        vec_sq = jnp.sum(gv_sum[...] * gv_sum[...])
        mid_second()
        do_z(2)
        do_b(3)

        def squares(size, total):
            def add(i, acc):
                g = total(pl.ds(pl.multiple_of(i * size, 8), size), i)
                return acc + jnp.sum((g * g).reshape(size // 8, 8, LANES), axis=0)

            return add

        mid_step = (rows - last) // STEPS
        last_step = last // STEPS

        def final_mid(t, i):
            g = (mid_total(0, t) + mid_b_recv[t, :]) * inv_group
            grad[pl.ds(pl.multiple_of(last + i * mid_step, 8), mid_step), :] = g
            return g

        def last_plane(s, _):
            send_z[3, s, :] = plane_total(3, s)

        def final_last(s, i):
            g = send_z[3, s, :]
            for j in range(3):
                g = g + recv_z[order[j], s, :]
            g = g * inv_group
            grad[s, :] = g
            return g

        do_z(3)
        chunks(0, last, last_plane)
        wait_mid(0)
        mid_b_copy.wait_recv()
        sq = lax.fori_loop(0, STEPS, squares(mid_step, final_mid), jnp.zeros((8, LANES), F32))
        wait_all(recv_z.at[pl.ds(0, 3)], z_r)
        sq = lax.fori_loop(0, STEPS, squares(last_step, final_last), sq)
        norm_rows[me] = jnp.sum(sq, axis=0, keepdims=True)

        for d in range(1, group):
            to = (me + d) % group
            remote(norm_rows.at[me], norm_rows.at[me], n_s, n_r, to).start()
        wait_all(state, load_sem.at[1])
        wait_all(vec_state, load_sem.at[2])
        for ref, sem in ((pair, pair_s), (gv_pair, vc_s), (gv_quarter.at[pl.ds(0, 3)], vq_s), (gv_plane.at[pl.ds(0, 3)], vp_s),
                         (gv_line.at[pl.ds(0, 3)], vz_s), (gv_half, ve_s), (send_a, a_s), (send_b, b_s),
                         (send_z.at[pl.ds(0, 3)], z_s), (mid.at[pl.ds(0, 3)], m_s), (mid_b, mb_s),
                         (norm_rows.at[pl.ds(0, group - 1)], n_s)):
            wait_all(ref, sem)
        wait_all(norm_rows.at[pl.ds(0, group - 1)], n_r)
        norm_sq = jnp.sum(norm_rows[...]) + vec_sq
        norm = jnp.sqrt(jnp.full((8, LANES), norm_sq, F32))
        scale = jnp.minimum(1.0, MAX_NORM / (norm + NORM_EPS))[0:1, :]
        lr = lr_ref[0]

        def adam(start, size):
            s = pl.ds(start, size)
            new_p, new_m, new_v = adam_update(grad[s, :] * scale, state[0, s, :], state[1, s, :], state[2, s, :], lr, WEIGHT_DECAY)
            p_out[s, :] = new_p
            m_out[s, :] = new_m
            v_out[s, :] = new_v
            pb_out[me, s, :] = new_p.astype(BF16)

        def move(idx, p, s_sem, r_sem, dev):
            ref = pb_out.at[idx, parts[p]]
            return remote(ref, ref, s_sem, r_sem, dev)

        def move_line(r, p, kind, to):
            zq = plane_at(r)
            return move(piece(zq, False, kind == 1), p, (m_s if kind else z_s), pool.at[zq * 4 + p + kind], dev_z(plane_at(to)))

        def move_b(zq, flip, p):
            return move(piece(zq, False, flip), p, (mb_s if p == 2 else b_s), pool.at[24 if p == 2 else 16 + zq * 2 + p], dev_b)

        def move_a(r, kind, p):
            zq = plane_at(r)
            arrival = 33 + p if (r, kind) == (3, 1) else 25 + zq * 2 + kind
            return move(piece(zq, False, kind == 1), p, a_s, pool.at[arrival], dev_a)

        def move_c(zq, kind, p):
            return move(piece(zq, False, kind == 1), p, pair_s, z_r, dev_c)

        def pass_on(r, kind, p):
            move_a(r, kind, p).start()
            move_c(plane_at(r), kind, p).start()

        def gather(own_place, to, plan):
            def from_line(r, p, kind=0):
                move_line(r, p, kind, r).wait_recv()
                if own_place == 1 and r > 1:
                    move_line(r, p, kind, 0).start()
                if p < 2:
                    move_b(plane_at(r), False, p).start()
                pass_on(r, kind, p)

            def from_b(r, p):
                move_b(plane_at(r), True, p).wait_recv()
                if p == 2:
                    for other in to:
                        move_line(r, p, 1, other).start()
                pass_on(r, 1, p)

            def from_a(r, kind):
                zq = plane_at(r)
                idx = piece(zq, True, kind == 1)
                if (r, kind) == (3, 1):
                    for p in (0, 2, 1):
                        wait_all(pb_out.at[idx, parts[p]], pool.at[33 + p])
                        move(idx, p, pair_s, z_r, dev_c).start()
                    return
                ref = pb_out.at[idx]
                wait_all(ref, pool.at[25 + zq * 2 + kind])
                remote(ref, ref, pair_s, z_r, dev_c).start()

            for p in range(3):
                for start, size in steps[p]:
                    adam(start, size)
                for other in to:
                    move_line(own_place, p, 0, other).start()
                move_b(plane_at(own_place), False, p).start()
                pass_on(own_place, 0, p)
            pv_new, mv_new, vv_new = adam_update(gv_sum[...] * scale, vec_state[0], vec_state[1], vec_state[2], lr, 0.0)
            pv_out[...] = pv_new
            mv_out[...] = mv_new
            vv_out[...] = vv_new
            takers = {"z": from_line, "b": from_b, "a": from_a}
            for item in plan:
                takers[item[0]](*[int(digit) for digit in item[1:]])
            wait_all(pb_out.at[pl.ds(0, group // 2)], z_r)
            lines = 2 + 2 * own_place
            wait_all(pb_out.at[pl.ds(0, lines)], z_s)
            wait_all(pb_out.at[pl.ds(0, lines), parts[2]], m_s)

        @pl.when(place == 0)
        def _():
            gather(0, (1, 2), END_PLAN)

        @pl.when(place == 1)
        def _():
            gather(1, (2, 0), INNER_PLAN)

        for ref, sem in ((pb_out.at[pl.ds(0, 4), pl.ds(0, late)], b_s), (pb_out.at[0, parts[2]], mb_s),
                         (pb_out.at[pl.ds(0, 8)], a_s), (pb_out.at[pl.ds(0, group // 2)], pair_s)):
            wait_all(ref, sem)

    vmem = pl.BlockSpec(memory_space=pltpu.VMEM)
    hbm = pl.BlockSpec(memory_space=pltpu.HBM)
    sem = sems = pltpu.SemaphoreType.DMA
    return pl.pallas_call(
        body,
        name="adam_step",
        out_shape=(
            jax.ShapeDtypeStruct((group, rows, LANES), BF16),
            *[jax.ShapeDtypeStruct((rows, LANES), F32)] * 3,
            *[jax.ShapeDtypeStruct((vrows, LANES), F32)] * 3,
        ),
        in_specs=[hbm] * 8 + [pl.BlockSpec(memory_space=pltpu.SMEM)],
        out_specs=(vmem,) * 7,
        scratch_shapes=[
            pltpu.VMEM((16, rows, 1, LANES), BF16),
            pltpu.VMEM((16, rows, 1, LANES), BF16),
            *[pltpu.VMEM((8, rows, LANES), F32)] * 2,
            *[pltpu.VMEM((4, last, LANES), F32)] * 4,
            *[pltpu.VMEM((4, 2, rows - last, LANES), F32)] * 2,
            *[pltpu.VMEM((rows - last, LANES), F32)] * 2,
            pltpu.VMEM((rows, LANES), F32),
            pltpu.VMEM((group, 1, LANES), F32),
            pltpu.VMEM((3, rows, LANES), F32),
            *[pltpu.VMEM((vhalf, 1, LANES), BF16)] * 2,
            pltpu.VMEM((vhalf, LANES), F32),
            *[pltpu.VMEM((4, quarter, LANES), F32)] * 3,
            *[pltpu.VMEM((vhalf, LANES), F32)] * 2,
            pltpu.VMEM((vrows, LANES), F32),
            pltpu.VMEM((3, vrows, LANES), F32),
            sems((3,)), sems((39,)), *[sem] * 8, sems((3,)),
            *[sem] * 12,
        ],
        compiler_params=pltpu.CompilerParams(
            collective_id=0, has_side_effects=True, vmem_limit_bytes=32 * 1024 * 1024),
    )


def store_kernel(shapes):
    def body(*refs):
        n = len(shapes)
        ins, outs, sem = refs[:n], refs[n:2 * n], refs[2 * n]
        copies = [pltpu.make_async_copy(ins[i], outs[i], sem.at[i]) for i in range(n)]
        for copy in copies:
            copy.start()
        for copy in copies:
            copy.wait()

    return pl.pallas_call(
        body,
        name="store_results",
        out_shape=tuple(shapes),
        in_specs=[pl.BlockSpec(memory_space=pltpu.VMEM)] * len(shapes),
        out_specs=tuple([pl.BlockSpec(memory_space=pltpu.HBM)] * len(shapes)),
        scratch_shapes=[pltpu.SemaphoreType.DMA((len(shapes),))],
        compiler_params=pltpu.CompilerParams(vmem_limit_bytes=16 * 1024 * 1024),
    )


def solution(mesh):
    axis_name = mesh.axis_names[0]
    group = mesh.shape[axis_name]

    def local_step(g_mat, g_vec, p_mat, m_mat, v_mat, p_vec, m_vec, v_vec, learn_rate):
        rows = p_mat.shape[0] // LANES
        vrows = p_vec.shape[0] // LANES
        operands = [
            g_mat.reshape(group * rows, 1, LANES), g_vec.reshape(vrows, 1, LANES),
            *[t.reshape(rows, LANES) for t in (p_mat, m_mat, v_mat)],
            *[t.reshape(vrows, LANES) for t in (p_vec, m_vec, v_vec)]]
        operands = [pltpu.with_memory_space_constraint(t, pltpu.HBM) for t in operands]
        results = step_kernel(group, rows, vrows, axis_name)(*operands, learn_rate.reshape(1))
        results = store_kernel([jax.ShapeDtypeStruct(r.shape, r.dtype) for r in results])(*results)
        full, new_p, new_m, new_v, new_pv, new_mv, new_vv = results
        return (*[t.reshape(-1) for t in (new_p, new_m, new_v, new_pv, new_mv, new_vv)], full.reshape(-1))

    return jax.shard_map(
        local_step,
        mesh=mesh,
        in_specs=(P(axis_name, None), P(axis_name, None), P(axis_name), P(axis_name), P(axis_name), P(), P(), P(), P()),
        out_specs=(P(axis_name), P(axis_name), P(axis_name), P(), P(), P(), P()),
        check_vma=False,
    )
```

```python
import jax
import jax.numpy as jnp
from jax import lax
from jax.experimental import pallas as pl
from jax.experimental.pallas import tpu as pltpu
from jax.sharding import PartitionSpec as P

STEP = 10
ADAM_BETA1 = 0.9
ADAM_BETA2 = 0.98
ADAM_EPS = 1e-8
WEIGHT_DECAY = 0.01
MAX_NORM = 1.0
NORM_EPS = 1e-6
BIAS_ONE = 1.0 - ADAM_BETA1 ** STEP
BIAS_TWO = 1.0 - ADAM_BETA2 ** STEP

MESH = pl.DeviceIdType.MESH
F32 = jnp.float32
BF16 = jnp.bfloat16
LANES = 128
STEPS = 1


END_PLAN = [
    "b00", "z100", "z110", "b01", "b02", "b10", "z120", "z200", "z210", "a00", "b11", "z220",
    "z121", "b20", "a01", "a10", "z300", "z310", "b21", "z320", "a11", "z221", "z321", "b30",
    "b31", "a30", "a21", "a20", "a31",
]
INNER_PLAN = [
    "z200", "z000", "z210", "a10", "b11", "b12", "b10", "z010", "z220", "z020", "z300", "b20",
    "b00", "b21", "z021", "z310", "b01", "z320", "z221", "a11", "a20", "a00", "z321", "a01",
    "b30", "b31", "a31", "a30", "a21",
]


def adam_update(grad_vals, param_vals, moment_one, moment_two, learn_rate, decay_rate):
    new_one = ADAM_BETA1 * moment_one + (1.0 - ADAM_BETA1) * grad_vals
    new_two = ADAM_BETA2 * moment_two + (1.0 - ADAM_BETA2) * grad_vals * grad_vals
    direction = (new_one / BIAS_ONE) / (jnp.sqrt(new_two / BIAS_TWO) + ADAM_EPS)
    return param_vals - learn_rate * (direction + decay_rate * param_vals), new_one, new_two


def step_kernel(group, rows, vrows, axis_name):
    inv_group = 1.0 / group
    vstep = vrows // 16 * 8
    vhalf = vrows - vstep
    qstep = vhalf // 32 * 8
    quarter = vhalf - 3 * qstep
    last = rows * 16 // 25 // (8 * STEPS) * (8 * STEPS)
    early, late = 192, 352
    bounds = (0, early, late, rows)
    parts = [pl.ds(lo, hi - lo) for lo, hi in zip(bounds, bounds[1:])]
    steps = []
    for lo, hi in zip(bounds, bounds[1:]):
        half = lo + ((hi - lo) // 2 + 15) // 16 * 16
        steps.append([(lo, half - lo), (half, hi - half)])

    def body(g_ref, gv_ref, p_ref, m_ref, v_ref, pv_ref, mv_ref, vv_ref, lr_ref,
             pb_out, p_out, m_out, v_out, pv_out, mv_out, vv_out,
             own, pair, send_a, recv_a, send_b, recv_b, send_z, recv_z, mid, mid_recv, mid_b, mid_b_recv, grad, norm_rows,
             state, gv_own, gv_pair, gv_sums, gv_quarter, gv_plane, gv_line, gv_half, gv_other, gv_sum, vec_state,
             own_sem, pool, pair_s, a_s, b_s, z_s, z_r, m_s, mb_s, mb_r, load_sem,
             vc_s, vc_r, vq_s, vq_r, vp_s, vp_r, vz_s, vz_r, ve_s, ve_r, n_s, n_r):
        me = lax.axis_index(axis_name)
        core = me % 2
        x = (me // 2) % 2
        y = (me // 4) % 2
        z = me // 8
        str_a = 2 + 2 * core
        str_b = 4 - 2 * core
        a = x + core * (y - x)
        b = y + core * (x - y)
        dev_c = me + 1 - 2 * core
        dev_a = me + (1 - 2 * a) * str_a
        dev_b = me + (1 - 2 * b) * str_b
        dev_x = me + (1 - 2 * x) * 2
        dev_y = me + (1 - 2 * y) * 4
        spot = y * 2 + x
        high = z // 2
        order = [3 - 3 * high, 2 - high, 1 - z + 4 * high, z]

        place = z + high * (3 - 2 * z)

        def plane_at(r):
            return r + high * (3 - 2 * r)

        def dev_z(zq):
            return me + (zq - z) * 8

        def piece(zq, flip_a, flip_b):
            aq = 1 - a if flip_a else a
            bq = 1 - b if flip_b else b
            return zq * 8 + aq * str_a + bq * str_b + core

        def partner_piece(zq, flip_a, flip_b):
            aq = 1 - b if flip_a else b
            bq = 1 - a if flip_b else a
            return zq * 8 + aq * str_b + bq * str_a + 1 - core

        def remote(src, dst, s_sem, r_sem, dev):
            return pltpu.make_async_remote_copy(
                src_ref=src, dst_ref=dst, send_sem=s_sem, recv_sem=r_sem, device_id=(dev,), device_id_type=MESH)

        flips = [(True, True), (True, False), (False, True), (False, False)]
        own_copies = []
        for j in range(4):
            for k, (fa, fb) in enumerate(flips):
                src = g_ref.at[pl.ds(piece(order[j], fa, fb) * rows, rows)]
                group_of = 0 if j + k == 0 else 1 + k // 2
                own_copies.append(pltpu.make_async_copy(src, own.at[j * 4 + k], own_sem.at[group_of]))
        use_order = [j * 4 + k for ks in ((0, 1), (2, 3)) for j in range(4) for k in ks]
        for i in use_order[:4]:
            own_copies[i].start()
        vec_load = pltpu.make_async_copy(gv_ref.at[pl.ds(core * vstep, vhalf)], gv_own, load_sem.at[0])
        vec_load.start()

        def wait_all(ref, sem):
            remote(ref, ref, sem, sem, dev_c).wait_recv()

        barrier = pltpu.get_barrier_semaphore()
        plane = [dev_x, dev_y, dev_x + dev_y - me]
        partners = [dev_c] + plane + [dev_z(order[j]) for j in range(3)]
        for partner in partners:
            pl.semaphore_signal(barrier, inc=1, device_id=(partner,), device_id_type=MESH)
        pl.semaphore_wait(barrier, len(partners))

        pair_copies = []
        for j in range(4):
            for k, (fa, fb) in enumerate(flips):
                src = g_ref.at[pl.ds(partner_piece(order[j], fa, fb) * rows, rows)]
                arrival = pool.at[j * 2 + k if k < 2 else 8 + j // 2]
                pair_copies.append(remote(src, pair.at[j * 4 + k], pair_s, arrival, dev_c))
        vec_pair = remote(gv_ref.at[pl.ds((1 - core) * vstep, vhalf)], gv_pair, vc_s, vc_r, dev_c)
        src = g_ref.at[pl.ds(partner_piece(order[0], True, True) * rows + last, rows - last)]
        pair_head = remote(src, pair.at[0, pl.ds(last, rows - last)], pair_s, pool.at[0], dev_c)
        src = g_ref.at[pl.ds(partner_piece(order[0], True, True) * rows, last)]
        pair_rest = remote(src, pair.at[0, pl.ds(0, last)], pair_s, pool.at[38], dev_c)
        pair_head.start()
        for n, i in enumerate(use_order):
            if i > 0:
                pair_copies[i].start()
            if n == 1:
                vec_pair.start()
                pair_rest.start()
            if n >= 4:
                own_copies[i].start()
        for i, ref in enumerate((p_ref, m_ref, v_ref)):
            pltpu.make_async_copy(ref, state.at[i], load_sem.at[1]).start()
        for i, ref in enumerate((pv_ref, mv_ref, vv_ref)):
            pltpu.make_async_copy(ref, vec_state.at[i], load_sem.at[2]).start()

        def chunks(start, stop, fn):
            size = (stop - start) // STEPS

            @pl.loop(0, STEPS)
            def _(i):
                fn(pl.ds(pl.multiple_of(start + i * size, 8), size), pl.ds(pl.multiple_of(i * size, 8), size))

        def pair_sum(i, s):
            return own[i, s, 0, :].astype(F32) + pair[i, s, 0, :].astype(F32)

        def move_a_sum(i, first):
            part = pl.ds(0, last) if first else pl.ds(last, rows - last)
            return remote(send_a.at[i, part], recv_a.at[i, part], a_s, pool.at[10 + i * 2 + first], dev_a)

        loaded = set()

        def do_a(i, first):
            slot = (i // 2) * 4 + i % 2
            if slot not in loaded:
                take(slot)
            if slot == 0 and first:
                pair_rest.wait_recv()

            def add_pair(s, _):
                send_a[i, s, :] = pair_sum(slot, s)

            chunks(*((0, last) if first else (last, rows)), add_pair)
            move_a_sum(i, first).start()

        def take(slot):
            loaded.add(slot)
            if slot == 0:
                own_copies[0].wait()
                pair_head.wait_recv()
            else:
                if len(loaded) == 2:
                    wait_all(own.at[pl.ds(0, 7)], own_sem.at[1])
                pair_copies[slot].wait_recv()

        do_a(0, 0)

        vec_load.wait()
        vec_pair.wait_recv()
        gv_sums[...] = gv_own[:, 0, :].astype(F32) + gv_pair[:, 0, :].astype(F32)

        def quarter_at(zq):
            return pl.ds(pl.multiple_of(zq * qstep, 8), quarter)

        for zq in order[:3]:
            remote(gv_sums.at[quarter_at(zq)], gv_quarter.at[z], vq_s, vq_r, dev_z(zq)).start()
        gv_quarter[z] = gv_sums[quarter_at(z), :]

        def in_order(parts):
            return ((parts[0] + parts[1]) + parts[2]) + parts[3]

        for i in range(1, 6):
            do_a(i, 0)

        wait_all(gv_quarter.at[pl.ds(0, 3)], vq_r)
        gv_plane[spot] = in_order(gv_quarter)
        for dev in plane:
            remote(gv_plane.at[spot], gv_plane.at[spot], vp_s, vp_r, dev).start()

        for i, first in [(0, 1), (2, 1), (7, 0), (1, 1), (6, 0), (4, 1), (3, 1), (5, 1), (6, 1), (7, 1)]:
            do_a(i, first)

        def move_mid(j, kind, slot, r):
            at = slot * 2 + kind
            return remote(mid.at[j, kind], mid_recv.at[slot, kind], m_s, pool.at[30 + at], dev_z(plane_at(r)))

        def do_mid(j):
            for kind in (1, 0):
                slot = j * 4 + 3 - kind
                i = j * 2 + 1 - kind
                if j == 0 and kind == 1:
                    wait_all(own.at[pl.ds(0, 8)], own_sem.at[2])
                if j % 2 == 0 and kind == 1:
                    wait_all(pair.at[pl.ds(0, 4)], pool.at[8 + j // 2])
                move_a_sum(i, 0).wait_recv()

                def add_a(s, t, kind=kind, slot=slot, i=i):
                    mid[j, kind, t, :] = pair_sum(slot, s) + recv_a[i, s, :]

                chunks(last, rows, add_a)
                if j < 3:
                    @pl.when(place == 0)
                    def _(kind=kind):
                        move_mid(j, kind, (2, 3, 0)[j], 1).start()
                if j == 2:
                    @pl.when(place == 1)
                    def _(kind=kind):
                        move_mid(j, kind, 0, 0).start()

        def merge_mid(j):
            @pl.when(place == 1)
            def _():
                for kind in (1, 0):
                    move_mid(j, kind, 2 + j, 0).wait_recv()

                    def add_end(_, t, kind=kind):
                        mid[j, kind, t, :] = mid[j, kind, t, :] + mid_recv[2 + j, kind, t, :]

                    chunks(last, rows, add_end)
                    move_mid(j, kind, 1, 3 - j).start()

        def mid_total(kind, t):
            return mid[3, kind, t, :] + mid_recv[0, kind, t, :] + mid_recv[1, kind, t, :]

        def wait_mid(kind):
            for slot in range(2):
                move_mid(3, kind, slot, 2).wait_recv()

        mid_b_copy = remote(mid_b, mid_b_recv, mb_s, mb_r, dev_b)

        def mid_second():
            wait_mid(1)

            def add_mid(_, t):
                mid_b[t, :] = mid_total(1, t)

            chunks(last, rows, add_mid)
            mid_b_copy.start()

        b_copies = [remote(send_b.at[j], recv_b.at[j], b_s, pool.at[26 + j], dev_b) for j in range(4)]
        z_copies = [remote(send_z.at[j], recv_z.at[z], z_s, z_r, dev_z(order[j])) for j in range(3)]

        def do_b(j):
            move_a_sum(j * 2, 1).wait_recv()

            def add_a(s, _):
                send_b[j, s, :] = pair_sum(j * 4 + 2, s) + recv_a[j * 2, s, :]

            chunks(0, last, add_a)
            b_copies[j].start()

        def plane_total(j, s):
            return pair_sum(j * 4 + 3, s) + recv_a[j * 2 + 1, s, :] + recv_b[j, s, :]

        def do_z(j):
            move_a_sum(j * 2 + 1, 1).wait_recv()
            b_copies[j].wait_recv()

            def add_ab(s, _):
                send_z[j, s, :] = plane_total(j, s)

            if j < 3:
                chunks(0, last, add_ab)
                z_copies[j].start()

        do_mid(0)
        do_mid(1)
        do_mid(2)
        merge_mid(0)
        do_b(0)
        wait_all(gv_plane.at[pl.ds(0, 3)], vp_r)
        gv_line[z] = in_order(gv_plane) * inv_group
        for zq in order[:3]:
            remote(gv_line.at[z], gv_line.at[z], vz_s, vz_r, dev_z(zq)).start()
        merge_mid(1)
        do_b(1)
        do_mid(3)
        do_z(0)
        do_b(2)
        do_z(1)
        wait_all(gv_line.at[pl.ds(0, 3)], vz_r)
        for zq in range(4):
            gv_half[pl.ds(zq * qstep, quarter), :] = gv_line[zq]
        vec_end = remote(gv_half, gv_other, ve_s, ve_r, dev_c)
        vec_end.start()
        vec_end.wait_recv()
        gv_sum[pl.ds(pl.multiple_of(core * vstep, 8), vhalf), :] = gv_half[...]
        gv_sum[pl.ds(pl.multiple_of((1 - core) * vstep, 8), vhalf), :] = gv_other[...]
        vec_sq = jnp.sum(gv_sum[...] * gv_sum[...])
        mid_second()
        do_z(2)
        do_b(3)

        def squares(size, total):
            def add(i, acc):
                g = total(pl.ds(pl.multiple_of(i * size, 8), size), i)
                return acc + jnp.sum((g * g).reshape(size // 8, 8, LANES), axis=0)

            return add

        mid_step = (rows - last) // STEPS
        last_step = last // STEPS

        def final_mid(t, i):
            g = (mid_total(0, t) + mid_b_recv[t, :]) * inv_group
            grad[pl.ds(pl.multiple_of(last + i * mid_step, 8), mid_step), :] = g
            return g

        def last_plane(s, _):
            send_z[3, s, :] = plane_total(3, s)

        def final_last(s, i):
            g = send_z[3, s, :]
            for j in range(3):
                g = g + recv_z[order[j], s, :]
            g = g * inv_group
            grad[s, :] = g
            return g

        do_z(3)
        chunks(0, last, last_plane)
        wait_mid(0)
        mid_b_copy.wait_recv()
        sq = lax.fori_loop(0, STEPS, squares(mid_step, final_mid), jnp.zeros((8, LANES), F32))
        wait_all(recv_z.at[pl.ds(0, 3)], z_r)
        sq = lax.fori_loop(0, STEPS, squares(last_step, final_last), sq)
        norm_rows[me] = jnp.sum(sq, axis=0, keepdims=True)

        for d in range(1, group):
            to = (me + d) % group
            remote(norm_rows.at[me], norm_rows.at[me], n_s, n_r, to).start()
        wait_all(state, load_sem.at[1])
        wait_all(vec_state, load_sem.at[2])
        for ref, sem in ((pair, pair_s), (gv_pair, vc_s), (gv_quarter.at[pl.ds(0, 3)], vq_s), (gv_plane.at[pl.ds(0, 3)], vp_s),
                         (gv_line.at[pl.ds(0, 3)], vz_s), (gv_half, ve_s), (send_a, a_s), (send_b, b_s),
                         (send_z.at[pl.ds(0, 3)], z_s), (mid.at[pl.ds(0, 3)], m_s), (mid_b, mb_s),
                         (norm_rows.at[pl.ds(0, group - 1)], n_s)):
            wait_all(ref, sem)
        wait_all(norm_rows.at[pl.ds(0, group - 1)], n_r)
        norm_sq = jnp.sum(norm_rows[...]) + vec_sq
        norm = jnp.sqrt(jnp.full((8, LANES), norm_sq, F32))
        scale = jnp.minimum(1.0, MAX_NORM / (norm + NORM_EPS))[0:1, :]
        lr = lr_ref[0]

        def adam(start, size):
            s = pl.ds(start, size)
            new_p, new_m, new_v = adam_update(grad[s, :] * scale, state[0, s, :], state[1, s, :], state[2, s, :], lr, WEIGHT_DECAY)
            p_out[s, :] = new_p
            m_out[s, :] = new_m
            v_out[s, :] = new_v
            pb_out[me, s, :] = new_p.astype(BF16)

        def move(idx, p, s_sem, r_sem, dev):
            ref = pb_out.at[idx, parts[p]]
            return remote(ref, ref, s_sem, r_sem, dev)

        def move_line(r, p, kind, to):
            zq = plane_at(r)
            return move(piece(zq, False, kind == 1), p, (m_s if kind else z_s), pool.at[zq * 4 + p + kind], dev_z(plane_at(to)))

        def move_b(zq, flip, p):
            return move(piece(zq, False, flip), p, (mb_s if p == 2 else b_s), pool.at[24 if p == 2 else 16 + zq * 2 + p], dev_b)

        def move_a(r, kind, p):
            zq = plane_at(r)
            arrival = 33 + p if (r, kind) == (3, 1) else 25 + zq * 2 + kind
            return move(piece(zq, False, kind == 1), p, a_s, pool.at[arrival], dev_a)

        def move_c(zq, kind, p):
            return move(piece(zq, False, kind == 1), p, pair_s, z_r, dev_c)

        def pass_on(r, kind, p):
            move_a(r, kind, p).start()
            move_c(plane_at(r), kind, p).start()

        def gather(own_place, to, plan):
            def from_line(r, p, kind=0):
                move_line(r, p, kind, r).wait_recv()
                if own_place == 1 and r > 1:
                    move_line(r, p, kind, 0).start()
                if p < 2:
                    move_b(plane_at(r), False, p).start()
                pass_on(r, kind, p)

            def from_b(r, p):
                move_b(plane_at(r), True, p).wait_recv()
                if p == 2:
                    for other in to:
                        move_line(r, p, 1, other).start()
                pass_on(r, 1, p)

            def from_a(r, kind):
                zq = plane_at(r)
                idx = piece(zq, True, kind == 1)
                if (r, kind) == (3, 1):
                    for p in (0, 2, 1):
                        wait_all(pb_out.at[idx, parts[p]], pool.at[33 + p])
                        move(idx, p, pair_s, z_r, dev_c).start()
                    return
                ref = pb_out.at[idx]
                wait_all(ref, pool.at[25 + zq * 2 + kind])
                remote(ref, ref, pair_s, z_r, dev_c).start()

            for p in range(3):
                for start, size in steps[p]:
                    adam(start, size)
                for other in to:
                    move_line(own_place, p, 0, other).start()
                move_b(plane_at(own_place), False, p).start()
                pass_on(own_place, 0, p)
            pv_new, mv_new, vv_new = adam_update(gv_sum[...] * scale, vec_state[0], vec_state[1], vec_state[2], lr, 0.0)
            pv_out[...] = pv_new
            mv_out[...] = mv_new
            vv_out[...] = vv_new
            takers = {"z": from_line, "b": from_b, "a": from_a}
            for item in plan:
                takers[item[0]](*[int(digit) for digit in item[1:]])
            wait_all(pb_out.at[pl.ds(0, group // 2)], z_r)
            lines = 2 + 2 * own_place
            wait_all(pb_out.at[pl.ds(0, lines)], z_s)
            wait_all(pb_out.at[pl.ds(0, lines), parts[2]], m_s)

        @pl.when(place == 0)
        def _():
            gather(0, (1, 2), END_PLAN)

        @pl.when(place == 1)
        def _():
            gather(1, (2, 0), INNER_PLAN)

        for ref, sem in ((pb_out.at[pl.ds(0, 4), pl.ds(0, late)], b_s), (pb_out.at[0, parts[2]], mb_s),
                         (pb_out.at[pl.ds(0, 8)], a_s), (pb_out.at[pl.ds(0, group // 2)], pair_s)):
            wait_all(ref, sem)

    vmem = pl.BlockSpec(memory_space=pltpu.VMEM)
    hbm = pl.BlockSpec(memory_space=pltpu.HBM)
    sem = sems = pltpu.SemaphoreType.DMA
    return pl.pallas_call(
        body,
        name="adam_step",
        out_shape=(
            jax.ShapeDtypeStruct((group, rows, LANES), BF16),
            *[jax.ShapeDtypeStruct((rows, LANES), F32)] * 3,
            *[jax.ShapeDtypeStruct((vrows, LANES), F32)] * 3,
        ),
        in_specs=[hbm] * 8 + [pl.BlockSpec(memory_space=pltpu.SMEM)],
        out_specs=(vmem,) * 7,
        scratch_shapes=[
            pltpu.VMEM((16, rows, 1, LANES), BF16),
            pltpu.VMEM((16, rows, 1, LANES), BF16),
            *[pltpu.VMEM((8, rows, LANES), F32)] * 2,
            *[pltpu.VMEM((4, last, LANES), F32)] * 4,
            *[pltpu.VMEM((4, 2, rows - last, LANES), F32)] * 2,
            *[pltpu.VMEM((rows - last, LANES), F32)] * 2,
            pltpu.VMEM((rows, LANES), F32),
            pltpu.VMEM((group, 1, LANES), F32),
            pltpu.VMEM((3, rows, LANES), F32),
            *[pltpu.VMEM((vhalf, 1, LANES), BF16)] * 2,
            pltpu.VMEM((vhalf, LANES), F32),
            *[pltpu.VMEM((4, quarter, LANES), F32)] * 3,
            *[pltpu.VMEM((vhalf, LANES), F32)] * 2,
            pltpu.VMEM((vrows, LANES), F32),
            pltpu.VMEM((3, vrows, LANES), F32),
            sems((3,)), sems((39,)), *[sem] * 8, sems((3,)),
            *[sem] * 12,
        ],
        compiler_params=pltpu.CompilerParams(
            collective_id=0, has_side_effects=True, vmem_limit_bytes=32 * 1024 * 1024),
    )


def store_kernel(shapes):
    def body(*refs):
        n = len(shapes)
        ins, outs, sem = refs[:n], refs[n:2 * n], refs[2 * n]
        copies = [pltpu.make_async_copy(ins[i], outs[i], sem.at[i]) for i in range(n)]
        for copy in copies:
            copy.start()
        for copy in copies:
            copy.wait()

    return pl.pallas_call(
        body,
        name="store_results",
        out_shape=tuple(shapes),
        in_specs=[pl.BlockSpec(memory_space=pltpu.VMEM)] * len(shapes),
        out_specs=tuple([pl.BlockSpec(memory_space=pltpu.HBM)] * len(shapes)),
        scratch_shapes=[pltpu.SemaphoreType.DMA((len(shapes),))],
        compiler_params=pltpu.CompilerParams(vmem_limit_bytes=16 * 1024 * 1024),
    )


def solution(mesh):
    axis_name = mesh.axis_names[0]
    group = mesh.shape[axis_name]

    def local_step(g_mat, g_vec, p_mat, m_mat, v_mat, p_vec, m_vec, v_vec, learn_rate):
        rows = p_mat.shape[0] // LANES
        vrows = p_vec.shape[0] // LANES
        operands = [
            g_mat.reshape(group * rows, 1, LANES), g_vec.reshape(vrows, 1, LANES),
            *[t.reshape(rows, LANES) for t in (p_mat, m_mat, v_mat)],
            *[t.reshape(vrows, LANES) for t in (p_vec, m_vec, v_vec)]]
        operands = [pltpu.with_memory_space_constraint(t, pltpu.HBM) for t in operands]
        results = step_kernel(group, rows, vrows, axis_name)(*operands, learn_rate.reshape(1))
        results = store_kernel([jax.ShapeDtypeStruct(r.shape, r.dtype) for r in results])(*results)
        full, new_p, new_m, new_v, new_pv, new_mv, new_vv = results
        return (*[t.reshape(-1) for t in (new_p, new_m, new_v, new_pv, new_mv, new_vv)], full.reshape(-1))

    return jax.shard_map(
        local_step,
        mesh=mesh,
        in_specs=(P(axis_name, None), P(axis_name, None), P(axis_name), P(axis_name), P(axis_name), P(), P(), P(), P()),
        out_specs=(P(axis_name), P(axis_name), P(axis_name), P(), P(), P(), P()),
        check_vma=False,
    )
```

```python
import jax
import jax.numpy as jnp
from jax import lax
from jax.experimental import pallas as pl
from jax.experimental.pallas import tpu as pltpu
from jax.sharding import PartitionSpec as P

STEP = 10
ADAM_BETA1 = 0.9
ADAM_BETA2 = 0.98
ADAM_EPS = 1e-8
WEIGHT_DECAY = 0.01
MAX_NORM = 1.0
NORM_EPS = 1e-6
BIAS_ONE = 1.0 - ADAM_BETA1 ** STEP
BIAS_TWO = 1.0 - ADAM_BETA2 ** STEP

MESH = pl.DeviceIdType.MESH
F32 = jnp.float32
BF16 = jnp.bfloat16
LANES = 128
STEPS = 1


END_PLAN = [
    "b00", "z100", "z110", "b01", "b02", "b10", "z120", "z200", "z210", "a00", "b11", "z220",
    "z121", "b20", "a01", "a10", "z300", "z310", "b21", "z320", "a11", "z221", "z321", "b30",
    "b31", "a30", "a21", "a20", "a31",
]
INNER_PLAN = [
    "z200", "z000", "z210", "a10", "b11", "b12", "b10", "z010", "z220", "z020", "z300", "b20",
    "b00", "b21", "z021", "z310", "b01", "z320", "z221", "a11", "a20", "a00", "z321", "a01",
    "b30", "b31", "a31", "a30", "a21",
]


def adam_update(grad_vals, param_vals, moment_one, moment_two, learn_rate, decay_rate):
    new_one = ADAM_BETA1 * moment_one + (1.0 - ADAM_BETA1) * grad_vals
    new_two = ADAM_BETA2 * moment_two + (1.0 - ADAM_BETA2) * grad_vals * grad_vals
    direction = (new_one / BIAS_ONE) / (jnp.sqrt(new_two / BIAS_TWO) + ADAM_EPS)
    return param_vals - learn_rate * (direction + decay_rate * param_vals), new_one, new_two


def step_kernel(group, rows, vrows, axis_name):
    inv_group = 1.0 / group
    vstep = vrows // 16 * 8
    vhalf = vrows - vstep
    qstep = vhalf // 32 * 8
    quarter = vhalf - 3 * qstep
    last = rows * 47 // 75 // (8 * STEPS) * (8 * STEPS)
    early, late = 192, 352
    bounds = (0, early, late, rows)
    parts = [pl.ds(lo, hi - lo) for lo, hi in zip(bounds, bounds[1:])]
    steps = []
    for lo, hi in zip(bounds, bounds[1:]):
        half = lo + ((hi - lo) // 2 + 15) // 16 * 16
        steps.append([(lo, half - lo), (half, hi - half)])

    def body(g_ref, gv_ref, p_ref, m_ref, v_ref, pv_ref, mv_ref, vv_ref, lr_ref,
             pb_out, p_out, m_out, v_out, pv_out, mv_out, vv_out,
             own, pair, send_a, recv_a, send_b, recv_b, send_z, recv_z, mid, mid_recv, mid_b, mid_b_recv, grad, norm_rows,
             state, gv_own, gv_pair, gv_sums, gv_quarter, gv_plane, gv_line, gv_half, gv_other, gv_sum, vec_state,
             own_sem, pool, pair_s, a_s, b_s, z_s, z_r, m_s, mb_s, mb_r, load_sem,
             vc_s, vc_r, vq_s, vq_r, vp_s, vp_r, vz_s, vz_r, ve_s, ve_r, n_s, n_r):
        me = lax.axis_index(axis_name)
        core = me % 2
        x = (me // 2) % 2
        y = (me // 4) % 2
        z = me // 8
        str_a = 2 + 2 * core
        str_b = 4 - 2 * core
        a = x + core * (y - x)
        b = y + core * (x - y)
        dev_c = me + 1 - 2 * core
        dev_a = me + (1 - 2 * a) * str_a
        dev_b = me + (1 - 2 * b) * str_b
        dev_x = me + (1 - 2 * x) * 2
        dev_y = me + (1 - 2 * y) * 4
        spot = y * 2 + x
        high = z // 2
        order = [3 - 3 * high, 2 - high, 1 - z + 4 * high, z]

        place = z + high * (3 - 2 * z)

        def plane_at(r):
            return r + high * (3 - 2 * r)

        def dev_z(zq):
            return me + (zq - z) * 8

        def piece(zq, flip_a, flip_b):
            aq = 1 - a if flip_a else a
            bq = 1 - b if flip_b else b
            return zq * 8 + aq * str_a + bq * str_b + core

        def partner_piece(zq, flip_a, flip_b):
            aq = 1 - b if flip_a else b
            bq = 1 - a if flip_b else a
            return zq * 8 + aq * str_b + bq * str_a + 1 - core

        def remote(src, dst, s_sem, r_sem, dev):
            return pltpu.make_async_remote_copy(
                src_ref=src, dst_ref=dst, send_sem=s_sem, recv_sem=r_sem, device_id=(dev,), device_id_type=MESH)

        flips = [(True, True), (True, False), (False, True), (False, False)]
        own_copies = []
        for j in range(4):
            for k, (fa, fb) in enumerate(flips):
                src = g_ref.at[pl.ds(piece(order[j], fa, fb) * rows, rows)]
                group_of = 0 if j + k == 0 else 1 + k // 2
                own_copies.append(pltpu.make_async_copy(src, own.at[j * 4 + k], own_sem.at[group_of]))
        use_order = [j * 4 + k for ks in ((0, 1), (2, 3)) for j in range(4) for k in ks]
        for i in use_order[:4]:
            own_copies[i].start()
        vec_load = pltpu.make_async_copy(gv_ref.at[pl.ds(core * vstep, vhalf)], gv_own, load_sem.at[0])
        vec_load.start()

        def wait_all(ref, sem):
            remote(ref, ref, sem, sem, dev_c).wait_recv()

        barrier = pltpu.get_barrier_semaphore()
        plane = [dev_x, dev_y, dev_x + dev_y - me]
        partners = [dev_c] + plane + [dev_z(order[j]) for j in range(3)]
        for partner in partners:
            pl.semaphore_signal(barrier, inc=1, device_id=(partner,), device_id_type=MESH)
        pl.semaphore_wait(barrier, len(partners))

        pair_copies = []
        for j in range(4):
            for k, (fa, fb) in enumerate(flips):
                src = g_ref.at[pl.ds(partner_piece(order[j], fa, fb) * rows, rows)]
                arrival = pool.at[j * 2 + k if k < 2 else 8 + j // 2]
                pair_copies.append(remote(src, pair.at[j * 4 + k], pair_s, arrival, dev_c))
        vec_pair = remote(gv_ref.at[pl.ds((1 - core) * vstep, vhalf)], gv_pair, vc_s, vc_r, dev_c)
        src = g_ref.at[pl.ds(partner_piece(order[0], True, True) * rows + last, rows - last)]
        pair_head = remote(src, pair.at[0, pl.ds(last, rows - last)], pair_s, pool.at[0], dev_c)
        src = g_ref.at[pl.ds(partner_piece(order[0], True, True) * rows, last)]
        pair_rest = remote(src, pair.at[0, pl.ds(0, last)], pair_s, pool.at[38], dev_c)
        pair_head.start()
        for n, i in enumerate(use_order):
            if i > 0:
                pair_copies[i].start()
            if n == 1:
                vec_pair.start()
                pair_rest.start()
            if n >= 4:
                own_copies[i].start()
        for i, ref in enumerate((p_ref, m_ref, v_ref)):
            pltpu.make_async_copy(ref, state.at[i], load_sem.at[1]).start()
        for i, ref in enumerate((pv_ref, mv_ref, vv_ref)):
            pltpu.make_async_copy(ref, vec_state.at[i], load_sem.at[2]).start()

        def chunks(start, stop, fn):
            size = (stop - start) // STEPS

            @pl.loop(0, STEPS)
            def _(i):
                fn(pl.ds(pl.multiple_of(start + i * size, 8), size), pl.ds(pl.multiple_of(i * size, 8), size))

        def pair_sum(i, s):
            return own[i, s, 0, :].astype(F32) + pair[i, s, 0, :].astype(F32)

        def move_a_sum(i, first):
            part = pl.ds(0, last) if first else pl.ds(last, rows - last)
            return remote(send_a.at[i, part], recv_a.at[i, part], a_s, pool.at[10 + i * 2 + first], dev_a)

        loaded = set()

        def do_a(i, first):
            slot = (i // 2) * 4 + i % 2
            if slot not in loaded:
                take(slot)
            if slot == 0 and first:
                pair_rest.wait_recv()

            def add_pair(s, _):
                send_a[i, s, :] = pair_sum(slot, s)

            chunks(*((0, last) if first else (last, rows)), add_pair)
            move_a_sum(i, first).start()

        def take(slot):
            loaded.add(slot)
            if slot == 0:
                own_copies[0].wait()
                pair_head.wait_recv()
            else:
                if len(loaded) == 2:
                    wait_all(own.at[pl.ds(0, 7)], own_sem.at[1])
                pair_copies[slot].wait_recv()

        do_a(0, 0)

        vec_load.wait()
        vec_pair.wait_recv()
        gv_sums[...] = gv_own[:, 0, :].astype(F32) + gv_pair[:, 0, :].astype(F32)

        def quarter_at(zq):
            return pl.ds(pl.multiple_of(zq * qstep, 8), quarter)

        for zq in order[:3]:
            remote(gv_sums.at[quarter_at(zq)], gv_quarter.at[z], vq_s, vq_r, dev_z(zq)).start()
        gv_quarter[z] = gv_sums[quarter_at(z), :]

        def in_order(parts):
            return ((parts[0] + parts[1]) + parts[2]) + parts[3]

        for i in range(1, 6):
            do_a(i, 0)

        wait_all(gv_quarter.at[pl.ds(0, 3)], vq_r)
        gv_plane[spot] = in_order(gv_quarter)
        for dev in plane:
            remote(gv_plane.at[spot], gv_plane.at[spot], vp_s, vp_r, dev).start()

        for i, first in [(0, 1), (2, 1), (7, 0), (1, 1), (6, 0), (4, 1), (3, 1), (5, 1), (6, 1), (7, 1)]:
            do_a(i, first)

        def move_mid(j, kind, slot, r):
            at = slot * 2 + kind
            return remote(mid.at[j, kind], mid_recv.at[slot, kind], m_s, pool.at[30 + at], dev_z(plane_at(r)))

        def do_mid(j):
            for kind in (1, 0):
                slot = j * 4 + 3 - kind
                i = j * 2 + 1 - kind
                if j == 0 and kind == 1:
                    wait_all(own.at[pl.ds(0, 8)], own_sem.at[2])
                if j % 2 == 0 and kind == 1:
                    wait_all(pair.at[pl.ds(0, 4)], pool.at[8 + j // 2])
                move_a_sum(i, 0).wait_recv()

                def add_a(s, t, kind=kind, slot=slot, i=i):
                    mid[j, kind, t, :] = pair_sum(slot, s) + recv_a[i, s, :]

                chunks(last, rows, add_a)
                if j < 3:
                    @pl.when(place == 0)
                    def _(kind=kind):
                        move_mid(j, kind, (2, 3, 0)[j], 1).start()
                if j == 2:
                    @pl.when(place == 1)
                    def _(kind=kind):
                        move_mid(j, kind, 0, 0).start()

        def merge_mid(j):
            @pl.when(place == 1)
            def _():
                for kind in (1, 0):
                    move_mid(j, kind, 2 + j, 0).wait_recv()

                    def add_end(_, t, kind=kind):
                        mid[j, kind, t, :] = mid[j, kind, t, :] + mid_recv[2 + j, kind, t, :]

                    chunks(last, rows, add_end)
                    move_mid(j, kind, 1, 3 - j).start()

        def mid_total(kind, t):
            return mid[3, kind, t, :] + mid_recv[0, kind, t, :] + mid_recv[1, kind, t, :]

        def wait_mid(kind):
            for slot in range(2):
                move_mid(3, kind, slot, 2).wait_recv()

        mid_b_copy = remote(mid_b, mid_b_recv, mb_s, mb_r, dev_b)

        def mid_second():
            wait_mid(1)

            def add_mid(_, t):
                mid_b[t, :] = mid_total(1, t)

            chunks(last, rows, add_mid)
            mid_b_copy.start()

        b_copies = [remote(send_b.at[j], recv_b.at[j], b_s, pool.at[26 + j], dev_b) for j in range(4)]
        z_copies = [remote(send_z.at[j], recv_z.at[z], z_s, z_r, dev_z(order[j])) for j in range(3)]

        def do_b(j):
            move_a_sum(j * 2, 1).wait_recv()

            def add_a(s, _):
                send_b[j, s, :] = pair_sum(j * 4 + 2, s) + recv_a[j * 2, s, :]

            chunks(0, last, add_a)
            b_copies[j].start()

        def plane_total(j, s):
            return pair_sum(j * 4 + 3, s) + recv_a[j * 2 + 1, s, :] + recv_b[j, s, :]

        def do_z(j):
            move_a_sum(j * 2 + 1, 1).wait_recv()
            b_copies[j].wait_recv()

            def add_ab(s, _):
                send_z[j, s, :] = plane_total(j, s)

            if j < 3:
                chunks(0, last, add_ab)
                z_copies[j].start()

        do_mid(0)
        do_mid(1)
        do_mid(2)
        merge_mid(0)
        do_b(0)
        wait_all(gv_plane.at[pl.ds(0, 3)], vp_r)
        gv_line[z] = in_order(gv_plane) * inv_group
        for zq in order[:3]:
            remote(gv_line.at[z], gv_line.at[z], vz_s, vz_r, dev_z(zq)).start()
        merge_mid(1)
        do_b(1)
        do_mid(3)
        do_z(0)
        do_b(2)
        do_z(1)
        wait_all(gv_line.at[pl.ds(0, 3)], vz_r)
        for zq in range(4):
            gv_half[pl.ds(zq * qstep, quarter), :] = gv_line[zq]
        vec_end = remote(gv_half, gv_other, ve_s, ve_r, dev_c)
        vec_end.start()
        vec_end.wait_recv()
        gv_sum[pl.ds(pl.multiple_of(core * vstep, 8), vhalf), :] = gv_half[...]
        gv_sum[pl.ds(pl.multiple_of((1 - core) * vstep, 8), vhalf), :] = gv_other[...]
        vec_sq = jnp.sum(gv_sum[...] * gv_sum[...])
        mid_second()
        do_z(2)
        do_b(3)

        def squares(size, total):
            def add(i, acc):
                g = total(pl.ds(pl.multiple_of(i * size, 8), size), i)
                return acc + jnp.sum((g * g).reshape(size // 8, 8, LANES), axis=0)

            return add

        mid_step = (rows - last) // STEPS
        last_step = last // STEPS

        def final_mid(t, i):
            g = (mid_total(0, t) + mid_b_recv[t, :]) * inv_group
            grad[pl.ds(pl.multiple_of(last + i * mid_step, 8), mid_step), :] = g
            return g

        def last_plane(s, _):
            send_z[3, s, :] = plane_total(3, s)

        def final_last(s, i):
            g = send_z[3, s, :]
            for j in range(3):
                g = g + recv_z[order[j], s, :]
            g = g * inv_group
            grad[s, :] = g
            return g

        do_z(3)
        chunks(0, last, last_plane)
        wait_mid(0)
        mid_b_copy.wait_recv()
        sq = lax.fori_loop(0, STEPS, squares(mid_step, final_mid), jnp.zeros((8, LANES), F32))
        wait_all(recv_z.at[pl.ds(0, 3)], z_r)
        sq = lax.fori_loop(0, STEPS, squares(last_step, final_last), sq)
        norm_rows[me] = jnp.sum(sq, axis=0, keepdims=True)

        for d in range(1, group):
            to = (me + d) % group
            remote(norm_rows.at[me], norm_rows.at[me], n_s, n_r, to).start()
        wait_all(state, load_sem.at[1])
        wait_all(vec_state, load_sem.at[2])
        for ref, sem in ((pair, pair_s), (gv_pair, vc_s), (gv_quarter.at[pl.ds(0, 3)], vq_s), (gv_plane.at[pl.ds(0, 3)], vp_s),
                         (gv_line.at[pl.ds(0, 3)], vz_s), (gv_half, ve_s), (send_a, a_s), (send_b, b_s),
                         (send_z.at[pl.ds(0, 3)], z_s), (mid.at[pl.ds(0, 3)], m_s), (mid_b, mb_s),
                         (norm_rows.at[pl.ds(0, group - 1)], n_s)):
            wait_all(ref, sem)
        wait_all(norm_rows.at[pl.ds(0, group - 1)], n_r)
        norm_sq = jnp.sum(norm_rows[...]) + vec_sq
        norm = jnp.sqrt(jnp.full((8, LANES), norm_sq, F32))
        scale = jnp.minimum(1.0, MAX_NORM / (norm + NORM_EPS))[0:1, :]
        lr = lr_ref[0]

        def adam(start, size):
            s = pl.ds(start, size)
            new_p, new_m, new_v = adam_update(grad[s, :] * scale, state[0, s, :], state[1, s, :], state[2, s, :], lr, WEIGHT_DECAY)
            p_out[s, :] = new_p
            m_out[s, :] = new_m
            v_out[s, :] = new_v
            pb_out[me, s, :] = new_p.astype(BF16)

        def move(idx, p, s_sem, r_sem, dev):
            ref = pb_out.at[idx, parts[p]]
            return remote(ref, ref, s_sem, r_sem, dev)

        def move_line(r, p, kind, to):
            zq = plane_at(r)
            return move(piece(zq, False, kind == 1), p, (m_s if kind else z_s), pool.at[zq * 4 + p + kind], dev_z(plane_at(to)))

        def move_b(zq, flip, p):
            return move(piece(zq, False, flip), p, (mb_s if p == 2 else b_s), pool.at[24 if p == 2 else 16 + zq * 2 + p], dev_b)

        def move_a(r, kind, p):
            zq = plane_at(r)
            arrival = 33 + p if (r, kind) == (3, 1) else 25 + zq * 2 + kind
            return move(piece(zq, False, kind == 1), p, a_s, pool.at[arrival], dev_a)

        def move_c(zq, kind, p):
            return move(piece(zq, False, kind == 1), p, pair_s, z_r, dev_c)

        def pass_on(r, kind, p):
            move_a(r, kind, p).start()
            move_c(plane_at(r), kind, p).start()

        def gather(own_place, to, plan):
            def from_line(r, p, kind=0):
                move_line(r, p, kind, r).wait_recv()
                if own_place == 1 and r > 1:
                    move_line(r, p, kind, 0).start()
                if p < 2:
                    move_b(plane_at(r), False, p).start()
                pass_on(r, kind, p)

            def from_b(r, p):
                move_b(plane_at(r), True, p).wait_recv()
                if p == 2:
                    for other in to:
                        move_line(r, p, 1, other).start()
                pass_on(r, 1, p)

            def from_a(r, kind):
                zq = plane_at(r)
                idx = piece(zq, True, kind == 1)
                if (r, kind) == (3, 1):
                    for p in (0, 2, 1):
                        wait_all(pb_out.at[idx, parts[p]], pool.at[33 + p])
                        move(idx, p, pair_s, z_r, dev_c).start()
                    return
                ref = pb_out.at[idx]
                wait_all(ref, pool.at[25 + zq * 2 + kind])
                remote(ref, ref, pair_s, z_r, dev_c).start()

            for p in range(3):
                for start, size in steps[p]:
                    adam(start, size)
                for other in to:
                    move_line(own_place, p, 0, other).start()
                move_b(plane_at(own_place), False, p).start()
                pass_on(own_place, 0, p)
            pv_new, mv_new, vv_new = adam_update(gv_sum[...] * scale, vec_state[0], vec_state[1], vec_state[2], lr, 0.0)
            pv_out[...] = pv_new
            mv_out[...] = mv_new
            vv_out[...] = vv_new
            takers = {"z": from_line, "b": from_b, "a": from_a}
            for item in plan:
                takers[item[0]](*[int(digit) for digit in item[1:]])
            wait_all(pb_out.at[pl.ds(0, group // 2)], z_r)
            lines = 2 + 2 * own_place
            wait_all(pb_out.at[pl.ds(0, lines)], z_s)
            wait_all(pb_out.at[pl.ds(0, lines), parts[2]], m_s)

        @pl.when(place == 0)
        def _():
            gather(0, (1, 2), END_PLAN)

        @pl.when(place == 1)
        def _():
            gather(1, (2, 0), INNER_PLAN)

        for ref, sem in ((pb_out.at[pl.ds(0, 4), pl.ds(0, late)], b_s), (pb_out.at[0, parts[2]], mb_s),
                         (pb_out.at[pl.ds(0, 8)], a_s), (pb_out.at[pl.ds(0, group // 2)], pair_s)):
            wait_all(ref, sem)

    vmem = pl.BlockSpec(memory_space=pltpu.VMEM)
    hbm = pl.BlockSpec(memory_space=pltpu.HBM)
    sem = sems = pltpu.SemaphoreType.DMA
    return pl.pallas_call(
        body,
        name="adam_step",
        out_shape=(
            jax.ShapeDtypeStruct((group, rows, LANES), BF16),
            *[jax.ShapeDtypeStruct((rows, LANES), F32)] * 3,
            *[jax.ShapeDtypeStruct((vrows, LANES), F32)] * 3,
        ),
        in_specs=[hbm] * 8 + [pl.BlockSpec(memory_space=pltpu.SMEM)],
        out_specs=(vmem,) * 7,
        scratch_shapes=[
            pltpu.VMEM((16, rows, 1, LANES), BF16),
            pltpu.VMEM((16, rows, 1, LANES), BF16),
            *[pltpu.VMEM((8, rows, LANES), F32)] * 2,
            *[pltpu.VMEM((4, last, LANES), F32)] * 4,
            *[pltpu.VMEM((4, 2, rows - last, LANES), F32)] * 2,
            *[pltpu.VMEM((rows - last, LANES), F32)] * 2,
            pltpu.VMEM((rows, LANES), F32),
            pltpu.VMEM((group, 1, LANES), F32),
            pltpu.VMEM((3, rows, LANES), F32),
            *[pltpu.VMEM((vhalf, 1, LANES), BF16)] * 2,
            pltpu.VMEM((vhalf, LANES), F32),
            *[pltpu.VMEM((4, quarter, LANES), F32)] * 3,
            *[pltpu.VMEM((vhalf, LANES), F32)] * 2,
            pltpu.VMEM((vrows, LANES), F32),
            pltpu.VMEM((3, vrows, LANES), F32),
            sems((3,)), sems((39,)), *[sem] * 8, sems((3,)),
            *[sem] * 12,
        ],
        compiler_params=pltpu.CompilerParams(
            collective_id=0, has_side_effects=True, vmem_limit_bytes=32 * 1024 * 1024),
    )


def store_kernel(shapes):
    def body(*refs):
        n = len(shapes)
        ins, outs, sem = refs[:n], refs[n:2 * n], refs[2 * n]
        copies = [pltpu.make_async_copy(ins[i], outs[i], sem.at[i]) for i in range(n)]
        for copy in copies:
            copy.start()
        for copy in copies:
            copy.wait()

    return pl.pallas_call(
        body,
        name="store_results",
        out_shape=tuple(shapes),
        in_specs=[pl.BlockSpec(memory_space=pltpu.VMEM)] * len(shapes),
        out_specs=tuple([pl.BlockSpec(memory_space=pltpu.HBM)] * len(shapes)),
        scratch_shapes=[pltpu.SemaphoreType.DMA((len(shapes),))],
        compiler_params=pltpu.CompilerParams(vmem_limit_bytes=16 * 1024 * 1024),
    )


def solution(mesh):
    axis_name = mesh.axis_names[0]
    group = mesh.shape[axis_name]

    def local_step(g_mat, g_vec, p_mat, m_mat, v_mat, p_vec, m_vec, v_vec, learn_rate):
        rows = p_mat.shape[0] // LANES
        vrows = p_vec.shape[0] // LANES
        operands = [
            g_mat.reshape(group * rows, 1, LANES), g_vec.reshape(vrows, 1, LANES),
            *[t.reshape(rows, LANES) for t in (p_mat, m_mat, v_mat)],
            *[t.reshape(vrows, LANES) for t in (p_vec, m_vec, v_vec)]]
        operands = [pltpu.with_memory_space_constraint(t, pltpu.HBM) for t in operands]
        results = step_kernel(group, rows, vrows, axis_name)(*operands, learn_rate.reshape(1))
        results = store_kernel([jax.ShapeDtypeStruct(r.shape, r.dtype) for r in results])(*results)
        full, new_p, new_m, new_v, new_pv, new_mv, new_vv = results
        return (*[t.reshape(-1) for t in (new_p, new_m, new_v, new_pv, new_mv, new_vv)], full.reshape(-1))

    return jax.shard_map(
        local_step,
        mesh=mesh,
        in_specs=(P(axis_name, None), P(axis_name, None), P(axis_name), P(axis_name), P(axis_name), P(), P(), P(), P()),
        out_specs=(P(axis_name), P(axis_name), P(axis_name), P(), P(), P(), P()),
        check_vma=False,
    )
```
